32 devices in a mesh: dp: 2 (over y), seq: 4 (over x, core), tp: 4 (over z).
Axes of the slice: x: 2, y: 2, z: 4, core: 2. Of those that a mesh axis runs over, the one named last changes fastest.
Arguments:
- tokens: bfloat16 [2048, 4096], P(('dp', 'seq', 'tp')), parts along dimension 0, may hold values from -6 to 6
- pre_gain: float32 [4096], replicated, may hold values from 0.25 to 1.75
- proj_inner: bfloat16 [4096, 4096], P(None, 'tp'), may hold values from -0.09375 to 0.09375
- proj_gate: bfloat16 [4096, 4096], P(None, 'tp'), may hold values from -0.09375 to 0.09375
- proj_states: bfloat16 [4096, 1024], P(None, 'tp'), may hold values from -0.09375 to 0.09375
- proj_step: bfloat16 [4096, 64], P(None, 'tp'), may hold values from -0.09375 to 0.09375
- step_bias: float32 [64], P('tp'), may hold values from -5 to -3
- log_rate: float32 [64], P('tp'), as said below
- conv_inner: float32 [4, 4096], P(None, 'tp'), may hold values from -3 to 3
- conv_states: float32 [4, 1024], P(None, 'tp'), may hold values from -3 to 3
- skip_gain: float32 [64], P('tp'), may hold values from 1 to 4
- norm_gain: float32 [4096], P('tp'), may hold values from 0.25 to 1.75
- proj_output: bfloat16 [4096, 4096], P('tp'), may hold values from -0.09375 to 0.09375
Outputs:
- layer_out: bfloat16 [2048, 4096], P(('dp', 'seq', 'tp')), parts along dimension 0
The draws below stay inside these ranges and needn't reach their ends.
There are 2 independent parts, one for each index of `dp`. The reference program is written for one: setup_inputs(seed, part) draws one part's arguments, and reference() takes and returns one part's arrays. A program takes and returns all parts, laid end to end along the dimension named above; an argument that names none is the same for every part. Nothing has to cross between parts.
Inputs may be any that keep to these rules, and one draw needn't show every extreme that they name: exp(log_rate) lies between 0.1 / (0.035 * 1024) and 1 / (25 * 0.035).
All inputs are finite; a program needn't handle non-finite values.
Results may differ from the reference program's by a relative error of at most 0.017.
Values may be sent and summed in bfloat16 or wider, within the bound.
A program may use at most 64 MiB of HBM per device.

```python
from functools import partial
import jax
import jax.numpy as jnp
from jax import lax

D = 4096
HEADS = 64
HEAD_DIM = 64
STATE = 128
KERNEL = 4
BLOCK = 128
INNER = 4096
GROUPS = 4
SEQ_LEN = 1024


def draw_log_rate(key, part):
    picked = jax.random.fold_in(key, 11)
    kind_key, slow_key, fast_key = jax.random.split(picked, 3)
    shares = jax.random.uniform(kind_key, (HEADS,), jnp.float32)
    slow_rate = jax.random.uniform(slow_key, (HEADS,), jnp.float32, jnp.log(0.1), jnp.log(1.0)) - jnp.log(0.035 * SEQ_LEN)
    fast_rate = jax.random.uniform(fast_key, (HEADS,), jnp.float32, jnp.log(1.0 / 40.0), jnp.log(1.0 / 25.0)) - jnp.log(0.035)
    limit = 0.5
    return jnp.where(shares < limit, slow_rate, fast_rate)


def steps_of(stream_key, dims, shards, low, high):
    def one(dim, shards_of):
        steps = jax.random.uniform(jax.random.fold_in(jax.random.fold_in(stream_key, 6), dim), (shards_of,), jnp.float32, low / len(shards), high / len(shards))
        return jnp.repeat(jnp.exp(steps), dims[dim] // shards_of).reshape((-1,) + (1,) * (len(dims) - dim - 1))

    gain = one(*shards[0])
    for cut in shards[1:]:
        gain = gain * one(*cut)
    return gain


def bell_draw(rng, dims, deviation, most, cuts=(), held_as=jnp.bfloat16):
    gain = steps_of(rng, dims, cuts, -0.22, 0.18) if cuts else 1.0
    array = jax.random.normal(rng, dims, jnp.float32) * deviation * gain
    return jnp.minimum(jnp.maximum(array, -most), most).astype(held_as)


def setup_inputs(seed: int = 0, part: int = 0) -> dict:
    key_list = jax.random.split(jax.random.key(seed), 14)
    part_keys = jax.random.split(jax.random.fold_in(key_list[13], part), 14)
    return {
        "tokens": bell_draw(part_keys[0], (SEQ_LEN, D), 1.0, 6.0, ((0, 16),)),
        "pre_gain": jnp.clip(1.0 + 0.15 * jax.random.normal(key_list[1], (D,), jnp.float32), 0.25, 1.75),
        "proj_inner": bell_draw(key_list[2], (D, INNER), D ** -0.5, 0.09375, ((1, 4),)),
        "proj_gate": bell_draw(key_list[3], (D, INNER), D ** -0.5, 0.09375, ((1, 4),)),
        "proj_states": bell_draw(key_list[4], (D, 2 * GROUPS * STATE), D ** -0.5, 0.09375, ((1, 4),)),
        "proj_step": bell_draw(key_list[5], (D, HEADS), D ** -0.5, 0.09375, ((1, 4),)),
        "step_bias": jnp.clip(-5.0 + 2.0 * jax.random.uniform(key_list[6], (HEADS,), jnp.float32) ** steps_of(key_list[6], (HEADS,), ((0, 4),), -0.2, 0.2), -5.0, -3.0),
        "log_rate": draw_log_rate(jax.random.fold_in(key_list[13], 71), part),
        "conv_inner": bell_draw(key_list[8], (KERNEL, INNER), KERNEL ** -0.5, 3.0, ((1, 4),), jnp.float32),
        "conv_states": bell_draw(key_list[9], (KERNEL, 2 * GROUPS * STATE), KERNEL ** -0.5, 3.0, ((1, 4),), jnp.float32),
        "skip_gain": jnp.clip(1.0 + 3.0 * jax.random.uniform(key_list[10], (HEADS,), jnp.float32) ** steps_of(key_list[10], (HEADS,), ((0, 4),), -0.2, 0.2), 1.0, 4.0),
        "norm_gain": jnp.clip(1.0 + 0.15 * jax.random.normal(key_list[11], (INNER,), jnp.float32), 0.25, 1.75),
        "proj_output": bell_draw(key_list[12], (INNER, D), INNER ** -0.5, 0.09375, ((0, 4),)),
    }


epsilon = 1e-05
highest = lax.Precision.HIGHEST

def causal_conv(values, kernel_taps, before):
    length = values.shape[0]
    padded = jnp.concatenate((before, values), axis=0)
    running_sum = jnp.zeros(values.shape, jnp.float32)
    for offset in range(kernel_taps.shape[0]):
        running_sum = running_sum + kernel_taps[offset] * padded[offset:offset + length]
    return running_sum

def block_step(carry_state, inputs, copies):
    values, step_size, log_decay, in_states, out_states = inputs
    block_len = values.shape[0]
    running = jnp.cumsum(log_decay, axis=0)
    scores = jnp.einsum('tgn,sgn->gts', out_states, in_states, precision=highest)
    scores = jnp.tile(scores, (copies, 1, 1))
    places = jnp.arange(block_len)
    lower_mask = (places[:, None] >= places[None, :])[None]
    spread = running.T[:, :, None] - running.T[:, None, :]
    decay_table = jnp.where(lower_mask, jnp.exp(jnp.where(lower_mask, spread, 0.0)), 0.0)
    weights = scores * decay_table * step_size.T[:, None, :]
    within = jnp.einsum('hts,shp->thp', weights, values, precision=highest)
    out_heads = jnp.tile(out_states, (1, copies, 1))
    in_heads = jnp.tile(in_states, (1, copies, 1))
    carried = jnp.einsum('thn,hpn->thp', out_heads, carry_state, precision=highest) * jnp.exp(running)[:, :, None]
    tail_decay = jnp.exp(running[-1][None, :] - running) * step_size
    scaled = values * tail_decay[:, :, None]
    new_state = jnp.exp(running[-1])[:, None, None] * carry_state + jnp.einsum('shp,shn->hpn', scaled, in_heads, precision=highest)
    return (new_state, within + carried)

def scan_blocks(values, step_size, log_decay, in_states, out_states, carry_state, block_len, copies):
    row_count, head_count, head_dim = values.shape
    block_count = row_count // block_len

    def split_blocks(source):
        return source.reshape((block_count, block_len) + source.shape[1:])
    final_state, outputs = lax.scan(partial(block_step, copies=copies), carry_state, (split_blocks(values), split_blocks(step_size), split_blocks(log_decay), split_blocks(in_states), split_blocks(out_states)))
    return (final_state, outputs.reshape(row_count, head_count, head_dim))

def reference(tokens, pre_gain, proj_inner, proj_gate, proj_states, proj_step, step_bias, log_rate, conv_inner, conv_states, skip_gain, norm_gain, proj_output):
    tokens_wide = tokens.astype(jnp.float32)
    normed = (tokens_wide * lax.rsqrt(lax.optimization_barrier(jnp.mean(tokens_wide * tokens_wide, axis=1, keepdims=True)) + epsilon) * pre_gain).astype(jnp.bfloat16)
    inner_proj = jnp.dot(normed, proj_inner, preferred_element_type=jnp.float32).astype(jnp.bfloat16)
    gate_proj = jnp.dot(normed, proj_gate, preferred_element_type=jnp.float32).astype(jnp.bfloat16)
    state_proj = jnp.dot(normed, proj_states, preferred_element_type=jnp.float32).astype(jnp.bfloat16)
    step_size = jax.nn.softplus(jnp.dot(normed, proj_step, preferred_element_type=jnp.float32) + step_bias)
    log_decay = -jnp.exp(log_rate) * step_size
    before_inner = jnp.zeros((KERNEL - 1, INNER), jnp.float32)
    before_states = jnp.zeros((KERNEL - 1, 2 * GROUPS * STATE), jnp.float32)
    mixed_inner = jax.nn.silu(causal_conv(inner_proj.astype(jnp.float32), conv_inner, before_inner)).astype(jnp.bfloat16)
    mixed_states = jax.nn.silu(causal_conv(state_proj.astype(jnp.float32), conv_states, before_states)).astype(jnp.bfloat16)
    values = mixed_inner.astype(jnp.float32).reshape(SEQ_LEN, HEADS, HEAD_DIM)
    paired = mixed_states.astype(jnp.float32).reshape(SEQ_LEN, GROUPS, 2, STATE)
    zero_state = jnp.zeros((HEADS, HEAD_DIM, STATE), jnp.float32)
    final_state, scanned = scan_blocks(values, step_size, log_decay, paired[:, :, 0], paired[:, :, 1], zero_state, BLOCK, HEADS // GROUPS)
    ssd_out = scanned + skip_gain[None, :, None] * values
    gated_out = ssd_out * jax.nn.silu(gate_proj.astype(jnp.float32)).reshape(SEQ_LEN, HEADS, HEAD_DIM)
    grouped = gated_out.reshape(SEQ_LEN, HEADS // GROUPS, GROUPS, HEAD_DIM)
    mean_square = lax.optimization_barrier(jnp.mean(grouped * grouped, axis=(1, 3), keepdims=True))
    normal_out = grouped * lax.rsqrt(mean_square + epsilon)
    mixed_out = (normal_out.reshape(SEQ_LEN, INNER) * norm_gain).astype(jnp.bfloat16)
    return (tokens_wide + jnp.dot(mixed_out, proj_output, preferred_element_type=jnp.float32)).astype(jnp.bfloat16)
```

```python
from functools import partial

import jax
import jax.numpy as jnp
from jax import lax
from jax.sharding import PartitionSpec as P
from jax.experimental import pallas as pl
from jax.experimental.pallas import tpu as pltpu

HEAD_DIM = 64
STATE = 128
GROUP_HEADS = 16
BLOCK = 128
GROUPS = 4


epsilon = 1e-05
highest = lax.Precision.HIGHEST


def from_behind(value, axis, steps):
    count = lax.axis_size(axis)
    initial, last = (max(0, -steps), min(count, count - steps))
    return lax.ppermute(value, axis, [(source, source + steps) for source in range(initial, last)])


def causal_conv(values, kernel_taps, before):
    length = values.shape[0]
    padded = jnp.concatenate((before, values), axis=0)
    running_sum = jnp.zeros(values.shape, jnp.float32)
    for offset in range(kernel_taps.shape[0]):
        running_sum = running_sum + kernel_taps[offset] * padded[offset : offset + length]
    return running_sum


def block_step(carry_state, inputs, copies):
    values, step_size, log_decay, in_states, out_states = inputs
    block_len = values.shape[0]
    running = jnp.cumsum(log_decay, axis=0)
    scores = jnp.einsum("tgn,sgn->gts", out_states, in_states, precision=highest)
    scores = jnp.tile(scores, (copies, 1, 1))
    places = jnp.arange(block_len)
    lower_mask = (places[:, None] >= places[None, :])[None]
    spread = running.T[:, :, None] - running.T[:, None, :]
    decay_table = jnp.where(lower_mask, jnp.exp(jnp.where(lower_mask, spread, 0.0)), 0.0)
    weights = scores * decay_table * step_size.T[:, None, :]
    within = jnp.einsum("hts,shp->thp", weights, values, precision=highest)
    out_heads = jnp.tile(out_states, (1, copies, 1))
    in_heads = jnp.tile(in_states, (1, copies, 1))
    carried = (
        jnp.einsum("thn,hpn->thp", out_heads, carry_state, precision=highest)
        * jnp.exp(running)[:, :, None]
    )
    tail_decay = jnp.exp(running[-1][None, :] - running) * step_size
    scaled = values * tail_decay[:, :, None]
    new_state = jnp.exp(running[-1])[:, None, None] * carry_state + jnp.einsum(
        "shp,shn->hpn", scaled, in_heads, precision=highest
    )
    return (new_state, within + carried)


def scan_blocks(
    values, step_size, log_decay, in_states, out_states, carry_state, block_len, copies
):
    row_count, head_count, head_dim = values.shape
    block_count = row_count // block_len

    def split_blocks(source):
        return source.reshape((block_count, block_len) + source.shape[1:])

    final_state, outputs = lax.scan(
        partial(block_step, copies=copies),
        carry_state,
        (
            split_blocks(values),
            split_blocks(step_size),
            split_blocks(log_decay),
            split_blocks(in_states),
            split_blocks(out_states),
        ),
    )
    return (final_state, outputs.reshape(row_count, head_count, head_dim))


def plain_body(
    tokens,
    pre_gain,
    proj_inner,
    proj_gate,
    proj_states,
    proj_step,
    step_bias,
    log_rate,
    conv_inner,
    conv_states,
    skip_gain,
    norm_gain,
    proj_output,
):
    tokens_wide = tokens.astype(jnp.float32)
    normed = (
        tokens_wide
        * lax.rsqrt(jnp.mean(tokens_wide * tokens_wide, axis=1, keepdims=True) + epsilon)
        * pre_gain
    ).astype(jnp.bfloat16)
    inner_width = proj_inner.shape[1]
    state_width = proj_states.shape[1]
    heads_local = proj_step.shape[1]
    copies = heads_local // GROUPS
    row_piece = lax.all_gather(normed, "tp", axis=0, tiled=True)
    projected = jnp.concatenate(
        (
            jnp.dot(row_piece, proj_inner, preferred_element_type=jnp.float32),
            jnp.dot(row_piece, proj_gate, preferred_element_type=jnp.float32),
            jnp.dot(row_piece, proj_states, preferred_element_type=jnp.float32),
            jnp.dot(row_piece, proj_step, preferred_element_type=jnp.float32),
        ),
        axis=1,
    )
    row_count = projected.shape[0]
    inner_proj = projected[:, :inner_width].astype(jnp.bfloat16)
    gate_proj = projected[:, inner_width : 2 * inner_width].astype(jnp.bfloat16)
    state_proj = projected[:, 2 * inner_width : 2 * inner_width + state_width].astype(jnp.bfloat16)
    step_size = jax.nn.softplus(projected[:, 2 * inner_width + state_width :] + step_bias)
    log_decay = -jnp.exp(log_rate) * step_size
    margin = conv_inner.shape[0] - 1
    before_inner, before_states = from_behind(
        (inner_proj[row_count - margin :], state_proj[row_count - margin :]), "seq", 1
    )
    mixed_inner = jax.nn.silu(
        causal_conv(inner_proj.astype(jnp.float32), conv_inner, before_inner.astype(jnp.float32))
    ).astype(jnp.bfloat16)
    mixed_local = jax.nn.silu(
        causal_conv(state_proj.astype(jnp.float32), conv_states, before_states.astype(jnp.float32))
    ).astype(jnp.bfloat16)
    mixed_all = lax.all_gather(mixed_local, "tp", axis=1, tiled=True)
    values = mixed_inner.astype(jnp.float32).reshape(row_count, heads_local, HEAD_DIM)
    paired = mixed_all.astype(jnp.float32).reshape(row_count, GROUPS, 2, STATE)
    in_states = paired[:, :, 0]
    out_states = paired[:, :, 1]
    zero_state = jnp.zeros((heads_local, HEAD_DIM, STATE), jnp.float32)
    final_state, scanned = scan_blocks(
        values, step_size, log_decay, in_states, out_states, zero_state, BLOCK, copies
    )
    decay_sum = jnp.sum(log_decay, axis=0)
    decay_sums, summaries = (
        lax.all_gather(decay_sum[None].astype(jnp.bfloat16), "seq", axis=0, tiled=True).astype(
            jnp.float32
        ),
        lax.all_gather(final_state[None].astype(jnp.bfloat16), "seq", axis=0, tiled=True).astype(
            jnp.float32
        ),
    )
    position = lax.axis_index("seq")
    device_ids = jnp.arange(decay_sums.shape[0])
    earlier_mask = (device_ids < position)[:, None]
    before_me = jnp.sum(jnp.where(earlier_mask, decay_sums, 0.0), axis=0)
    reach_end = jnp.cumsum(decay_sums, axis=0)
    weights = jnp.where(
        earlier_mask, jnp.exp(jnp.where(earlier_mask, before_me[None] - reach_end, 0.0)), 0.0
    )
    incoming = jnp.einsum("jh,jhpn->hpn", weights, summaries, precision=highest)
    running = jnp.cumsum(log_decay, axis=0)
    out_heads = jnp.tile(out_states, (1, copies, 1))
    carried = (
        jnp.einsum("thn,hpn->thp", out_heads, incoming, precision=highest)
        * jnp.exp(running)[:, :, None]
    )
    ssd_out = scanned + carried + skip_gain[None, :, None] * values
    gated_out = ssd_out * jax.nn.silu(gate_proj.astype(jnp.float32)).reshape(
        row_count, heads_local, HEAD_DIM
    )
    head_squares = jnp.sum(gated_out * gated_out, axis=2)
    every_square = lax.all_gather(head_squares, "tp", axis=1, tiled=True)
    group_totals = jnp.sum(
        every_square.reshape(row_count, every_square.shape[1] // GROUPS, GROUPS), axis=1
    )
    mean_square = (group_totals / (GROUP_HEADS * HEAD_DIM))[:, None, :, None]
    grouped = gated_out.reshape(row_count, copies, GROUPS, HEAD_DIM)
    normal_out = grouped * lax.rsqrt(mean_square + epsilon)
    mixed_out = (normal_out.reshape(row_count, inner_width) * norm_gain).astype(jnp.bfloat16)
    summed = lax.psum_scatter(
        jnp.dot(mixed_out, proj_output, preferred_element_type=jnp.float32).astype(jnp.bfloat16),
        "tp",
        scatter_dimension=0,
        tiled=True,
    ).astype(jnp.float32)
    return (tokens_wide + summed).astype(jnp.bfloat16)


def plain_solution(mesh):
    placed = (
        P(("dp", "seq", "tp"), None),
        P(),
        P(None, "tp"),
        P(None, "tp"),
        P(None, "tp"),
        P(None, "tp"),
        P("tp"),
        P("tp"),
        P(None, "tp"),
        P(None, "tp"),
        P("tp"),
        P("tp"),
        P("tp", None),
    )
    return jax.shard_map(
        plain_body, mesh=mesh, in_specs=placed, out_specs=P(("dp", "seq", "tp"), None), check_vma=False
    )


LANES = 128
PAD = 16
MESH = pl.DeviceIdType.MESH
NT = (((1,), (1,)), ((), ()))


def remote(source, target, send, receive, device):
    return pltpu.make_async_remote_copy(
        src_ref=source,
        dst_ref=target,
        send_sem=send,
        recv_sem=receive,
        device_id=device,
        device_id_type=MESH,
    )


def bdot(a, b):
    return jnp.dot(a, b, preferred_element_type=jnp.float32)


def fused_kernel(
    n,
    shards,
    tokens_far,
    pre_gain,
    w_inner,
    w_gate,
    w_states,
    w_step,
    step_bias,
    log_rate,
    taps_inner,
    taps_states,
    skip_gain,
    norm_gain,
    w_out,
    out,
    tokens,
    wide,
    step_w,
    wout,
    rows_all,
    proj,
    states,
    taps_all,
    raw_step,
    run_ref,
    x_mix,
    s_mix,
    acc,
    ends,
    state_out,
    state_in,
    squares,
    mixed,
    stage,
    from_right,
    from_left,
    own_sum,
    load_sem,
    line,
    ahead,
    g_send,
    g_recv,
    t_send,
    t_recv,
    s_send,
    s_recv,
    c_send,
    c_recv,
    ti_send,
    ti_recv,
    ts_send,
    ts_recv,
    e_send,
    e_recv,
    q_send,
    q_recv,
    r_send,
    rl_recv,
    rr_recv,
):
    z = lax.axis_index("tp")
    s = lax.axis_index("seq")
    rows, width = tokens.shape
    total = n * rows
    inner = w_inner.shape[1]
    state_w = w_states.shape[1]
    heads = w_step.shape[0]
    half = rows // 2

    token_load = pltpu.make_async_copy(tokens_far, tokens, load_sem.at[5])
    token_load.start()
    barrier = pltpu.get_barrier_semaphore()
    neighbours = (
        (z > 0, {"tp": z - 1}),
        (z < n - 1, {"tp": z + 1}),
        (s > 0, {"seq": s - 1}),
        (s < shards - 1, {"seq": s + 1}),
    )
    met = jnp.int32(0)
    for there, device in neighbours:
        met = met + there.astype(jnp.int32)

        @pl.when(there)
        def _():
            pl.semaphore_signal(barrier, inc=1, device_id=device, device_id_type=MESH)

    loads = [
        pltpu.make_async_copy(w_states, wide.at[:, pl.ds(2 * inner, state_w)], load_sem.at[0]),
        pltpu.make_async_copy(w_step, step_w, load_sem.at[1]),
        pltpu.make_async_copy(w_inner, wide.at[:, pl.ds(0, inner)], load_sem.at[2]),
        pltpu.make_async_copy(w_gate, wide.at[:, pl.ds(inner, inner)], load_sem.at[3]),
        pltpu.make_async_copy(w_out, wout, load_sem.at[4]),
    ]
    token_load.wait()
    for load in loads[:4]:
        load.start()

    def own_rows(i, _):
        piece = pl.ds(pl.multiple_of(i * 16, 16), 16)
        value = tokens[piece, :].astype(jnp.float32)
        scale = lax.rsqrt(jnp.mean(value * value, axis=1, keepdims=True) + epsilon)
        place = pl.ds(pl.multiple_of(z * rows + i * 16, 16), 16)
        rows_all[place, :] = (value * scale * pre_gain[...]).astype(jnp.bfloat16)
        return 0

    lax.fori_loop(0, half // 16, own_rows, 0)
    taps_all[z] = taps_states[...]

    @pl.when(s == 0)
    def _():
        proj[0:PAD, 0:inner] = jnp.zeros((PAD, inner), jnp.bfloat16)
        states[0:PAD, :] = jnp.zeros((PAD, states.shape[1]), jnp.bfloat16)
        state_in[...] = jnp.zeros(state_in.shape, jnp.bfloat16)

    pl.semaphore_wait(barrier, met)

    def row_copy(source, part, side):
        block = rows_all.at[pl.ds(pl.multiple_of(source * rows + part * half, 16), half), :]
        step = 1 if side == 0 else -1
        return remote(
            block, block, g_send.at[side, source, part], g_recv.at[source, part], {"tp": z + step}
        )

    def send_on(source, part):
        @pl.when(jnp.logical_and(source <= z, z < n - 1))
        def _():
            row_copy(source, part, 0).start()

        @pl.when(jnp.logical_and(source >= z, z > 0))
        def _():
            row_copy(source, part, 1).start()

    send_on(z, 0)
    lax.fori_loop(half // 16, rows // 16, own_rows, 0)
    send_on(z, 1)

    def greet_line(side, condition):
        @pl.when(condition)
        def _():
            pl.semaphore_signal(
                line.at[side],
                inc=1,
                device_id={"tp": z + 1 if side == 0 else z - 1},
                device_id_type=MESH,
            )

    greet_line(0, z == 0)
    greet_line(1, z == n - 1)
    for side in range(2):
        edge = 0 if side == 0 else n - 1

        @pl.when(z != edge)
        def _():
            pl.semaphore_wait(line.at[side], 1)

        greet_line(side, jnp.logical_and(z != edge, z != n - 1 - edge))

    @pl.when(s > 0)
    def _():
        pl.semaphore_signal(ahead, inc=1, device_id={"seq": s - 1}, device_id_type=MESH)


    def tap_copy(source, other):
        return remote(
            taps_all.at[source], taps_all.at[source], t_send.at[other], t_recv.at[source], {"tp": other}
        )

    def in_copy(source, chunk, other):
        block = states.at[
            pl.ds(pl.multiple_of(PAD + chunk * rows, 16), rows),
            pl.ds(pl.multiple_of(source * state_w, LANES), STATE),
        ]
        return remote(
            block, block, s_send.at[chunk, other], s_recv.at[source, chunk], {"tp": other}
        )

    def out_copy(source, other):
        block = states.at[
            pl.ds(PAD, total), pl.ds(pl.multiple_of(source * state_w + STATE, LANES), STATE)
        ]
        return remote(block, block, c_send.at[other], c_recv.at[source], {"tp": other})

    def square_copy(source, other):
        return remote(
            squares.at[source], squares.at[source], q_send.at[other], q_recv.at[source], {"tp": other}
        )

    def each_other(action):
        def one(i, _):
            @pl.when(i != z)
            def _():
                action(i)

            return 0

        lax.fori_loop(0, n, one, 0)

    each_other(lambda i: tap_copy(z, i).start())

    def inner_tail():
        return remote(
            proj.at[pl.ds(total, PAD), pl.ds(0, inner)],
            proj.at[pl.ds(0, PAD), pl.ds(0, inner)],
            ti_send,
            ti_recv,
            {"seq": s + 1, "tp": z},
        )

    def state_tail(source, other):
        columns = pl.ds(pl.multiple_of(source * state_w, LANES), state_w)
        return remote(
            states.at[pl.ds(total, PAD), columns],
            states.at[pl.ds(0, PAD), columns],
            ts_send.at[other],
            ts_recv.at[source],
            {"seq": s + 1, "tp": other},
        )

    for load in loads[:4]:
        load.wait()
    loads[4].start()

    def project_tiles(chunk, first, end):
        piece = pl.ds(pl.multiple_of(chunk * rows, rows), rows)
        place = pl.ds(pl.multiple_of(PAD + chunk * rows, 16), rows)

        def tile(i, _):
            columns = pl.ds(pl.multiple_of(i * 256, 256), 256)
            proj[place, columns] = bdot(rows_all[piece, :], wide[:, columns]).astype(jnp.bfloat16)
            return 0

        lax.fori_loop(first, end, tile, 0)

    def project(chunk, tiles):
        piece = pl.ds(pl.multiple_of(chunk * rows, rows), rows)
        place = pl.ds(pl.multiple_of(PAD + chunk * rows, 16), rows)
        own = pl.ds(pl.multiple_of(z * state_w, LANES), state_w)
        states[place, own] = bdot(
            rows_all[piece, :], wide[:, 2 * inner : 2 * inner + state_w]
        ).astype(jnp.bfloat16)
        each_other(lambda i: in_copy(z, chunk, i).start())

        @pl.when(jnp.logical_and(chunk == n - 1, s < shards - 1))
        def _():
            pl.semaphore_wait(ahead, 1)
            for other in range(n):
                state_tail(z, other).start()

        raw_step[piece, :] = lax.dot_general(
            rows_all[piece, :], step_w[...], NT, preferred_element_type=jnp.float32
        )

        project_tiles(chunk, 0, tiles)

        @pl.when(jnp.logical_and(chunk == n - 1, s < shards - 1))
        def _():
            inner_tail().start()

    gate_tile = inner // 256
    farthest = jnp.maximum(z, n - 1 - z)

    def arrive(distance, _):
        for side in range(2):
            source = z - distance if side == 0 else z + distance
            inside = jnp.logical_and(source >= 0, source < n)

            @pl.when(jnp.logical_and(inside, distance > 0))
            def _():
                for part in range(2):
                    row_copy(source, part, side).wait_recv()
                    send_on(source, part)

        def one(side, _):
            source = z - distance + 2 * distance * side
            inside = jnp.logical_and(source >= 0, source < n)

            @pl.when(jnp.logical_and(inside, jnp.logical_or(distance > 0, side == 0)))
            def _():
                project(source, jnp.where(distance == farthest, gate_tile, 2 * gate_tile))

            return 0

        lax.fori_loop(0, 2, one, 0)
        return 0

    lax.fori_loop(0, n, arrive, 0)

    def late_gate(side, _):
        source = z - farthest + 2 * farthest * side

        @pl.when(jnp.logical_and(source >= 0, source < n))
        def _():
            project_tiles(source, gate_tile, 2 * gate_tile)

        return 0

    each_other(lambda i: out_copy(z, i).start())

    step = raw_step[...] + step_bias[...]
    step = jnp.maximum(step, 0.0) + jnp.log1p(jnp.exp(-jnp.abs(step)))
    decay = -jnp.exp(log_rate[...]) * step
    place_t = lax.broadcasted_iota(jnp.int32, (total, total), 0)
    place_s = lax.broadcasted_iota(jnp.int32, (total, total), 1)
    tri = (place_t >= place_s).astype(jnp.float32)
    run = jnp.dot(tri, decay, precision=highest, preferred_element_type=jnp.float32)
    run_ref[...] = jnp.zeros(run_ref.shape, jnp.float32)
    run_ref[:, 0:heads] = run
    run_t = run_ref[...].T
    last = run[total - 1 : total, :]
    reach = jnp.exp(last - run) * step
    grown = jnp.exp(run)
    whole = jnp.exp(last)
    lane = lax.broadcasted_iota(jnp.int32, (1, LANES), 1)
    low = lane < HEAD_DIM

    def conv(buffer, columns, taps):
        value = buffer[:, columns].astype(jnp.float32)
        kernel_len = taps.shape[0]
        out_value = jnp.zeros((total, value.shape[1]), jnp.float32)
        for k in range(kernel_len):
            first = PAD - (kernel_len - 1) + k
            out_value = out_value + taps[k : k + 1, :] * value[first : first + total, :]
        return jax.nn.silu(out_value).astype(jnp.bfloat16)

    @pl.when(s > 0)
    def _():
        inner_tail().wait_recv()

    def conv_tile(i, _):
        columns = pl.ds(pl.multiple_of(i * 256, 256), 256)
        x_mix[:, columns] = conv(proj, columns, taps_inner[:, columns])
        return 0

    lax.fori_loop(0, inner // 256, conv_tile, 0)

    def take_states(part, i):
        columns = pl.ds(pl.multiple_of(i * state_w + part * STATE, LANES), STATE)
        taps = taps_all[i][:, part * STATE : (part + 1) * STATE]
        s_mix[:, columns] = conv(states, columns, taps)

    def take_in(i, _):
        @pl.when(i != z)
        def _():
            tap_copy(i, z).wait_recv()
            for chunk in range(n):
                in_copy(i, chunk, z).wait_recv()

        @pl.when(s > 0)
        def _():
            state_tail(i, z).wait_recv()

        take_states(0, i)
        return 0

    def take_out(i, _):
        @pl.when(i != z)
        def _():
            out_copy(i, z).wait_recv()

        take_states(1, i)
        return 0

    lax.fori_loop(0, n, take_in, 0)

    def group_in(g):
        return s_mix[:, g * 2 * STATE : g * 2 * STATE + STATE]

    def group_out(g):
        return s_mix[:, g * 2 * STATE + STATE : (g + 1) * 2 * STATE]

    def pair_of(value, h):
        return jnp.where(low, value[:, h : h + 1], value[:, h + 1 : h + 2])

    pairs = heads // 2
    per_quad = GROUPS // 2
    quads = pairs // per_quad
    quad_w = GROUPS * HEAD_DIM

    def end_copy(c):
        columns = pl.ds(c * quad_w, quad_w)
        return remote(
            state_out.at[:, columns],
            state_in.at[:, columns],
            e_send.at[c],
            e_recv.at[c],
            {"seq": s + 1, "tp": z},
        )

    turned = [group_in(g).T for g in range(GROUPS)]
    for q in range(pairs):
        columns = slice(q * LANES, (q + 1) * LANES)
        h = 2 * q
        scaled = (x_mix[:, columns].astype(jnp.float32) * pair_of(reach, h)).astype(jnp.bfloat16)
        ends[:, columns] = jnp.where(
            low, bdot(turned[h % GROUPS], scaled), bdot(turned[(h + 1) % GROUPS], scaled)
        )
        if q % per_quad == per_quad - 1:
            c = q // per_quad

            @pl.when(jnp.logical_and(s == 0, shards > 1))
            def _():
                columns = slice(c * quad_w, (c + 1) * quad_w)
                state_out[:, columns] = ends[:, columns].astype(jnp.bfloat16)
                end_copy(c).start()

    def hand_on(c, here):
        @pl.when(here)
        def _():
            end_copy(c).wait_recv()

            @pl.when(s < shards - 1)
            def _():
                for q in range(c * per_quad, (c + 1) * per_quad):
                    columns = slice(q * LANES, (q + 1) * LANES)
                    state_out[:, columns] = (
                        ends[:, columns]
                        + pair_of(whole, 2 * q) * state_in[:, columns].astype(jnp.float32)
                    ).astype(jnp.bfloat16)
                end_copy(c).start()

    lax.fori_loop(0, 2, late_gate, 0)
    for c in range(quads):
        hand_on(c, s == 1)
    lax.fori_loop(0, n, take_out, 0)

    scores = [
        lax.dot_general(group_out(g), group_in(g), NT, preferred_element_type=jnp.float32)
        for g in range(GROUPS)
    ]
    for q in range(pairs):
        columns = slice(q * LANES, (q + 1) * LANES)
        h = 2 * q
        value = x_mix[:, columns].astype(jnp.float32)
        stepped = (value * pair_of(step, h)).astype(jnp.bfloat16)
        direct = value * pair_of(skip_gain[...], h)
        for low_t in range(0, total, BLOCK):
            high_t = low_t + BLOCK
            causal = place_t[low_t:high_t, :high_t] >= place_s[low_t:high_t, :high_t]
            both = []
            for k in (h, h + 1):
                spread = run[low_t:high_t, k : k + 1] - run_t[k : k + 1, :high_t]
                table = jnp.where(causal, jnp.exp(jnp.where(causal, spread, 0.0)), 0.0)
                weights = (scores[k % GROUPS][low_t:high_t, :high_t] * table).astype(jnp.bfloat16)
                both.append(bdot(weights, stepped[:high_t, :]))
            acc[low_t:high_t, columns] = jnp.where(low, both[0], both[1]) + direct[low_t:high_t, :]
    sums = [jnp.zeros((total, LANES), jnp.float32) for _ in range(per_quad)]
    for q in range(pairs):
        columns = slice(q * LANES, (q + 1) * LANES)
        h = 2 * q
        if q % per_quad == 0:
            hand_on(q // per_quad, s > 1)
        came = state_in[:, columns]
        carried = jnp.where(
            low, bdot(group_out(h % GROUPS), came), bdot(group_out((h + 1) % GROUPS), came)
        )
        gate = proj[PAD:, inner + q * LANES : inner + (q + 1) * LANES].astype(jnp.float32)
        gated = (acc[:, columns] + carried * pair_of(grown, h)) * jax.nn.silu(gate)
        acc[:, columns] = gated
        sums[q % per_quad] = sums[q % per_quad] + gated * gated
    pick = lax.broadcasted_iota(jnp.int32, (8, LANES), 0)
    where_lane = lax.broadcasted_iota(jnp.int32, (8, LANES), 1)
    local = jnp.zeros((8, total), jnp.float32)
    for k in range(per_quad):
        chosen = (where_lane // HEAD_DIM + 2 * k == pick).astype(jnp.float32)
        local = local + lax.dot_general(
            chosen, sums[k], NT, precision=highest, preferred_element_type=jnp.float32
        )
    squares[z] = local
    each_other(lambda i: square_copy(z, i).start())
    loads[4].wait()
    each_other(lambda i: square_copy(i, z).wait_recv())
    sum_all = squares[0]
    for i in range(1, n):
        sum_all = sum_all + squares[i]
    inverse = lax.rsqrt(sum_all / (n * heads // GROUPS * HEAD_DIM) + epsilon)
    inverse = jnp.concatenate([inverse] * (LANES // 8), axis=0).T
    for q in range(pairs):
        columns = slice(q * LANES, (q + 1) * LANES)
        g = (2 * q) % GROUPS
        mixed[:, columns] = (
            acc[:, columns] * pair_of(inverse, g) * norm_gain[:, columns]
        ).astype(jnp.bfloat16)

    pieces = r_send.shape[1]
    piece_w = width // pieces

    def partial_of(target, p):
        return bdot(mixed[pl.ds(pl.multiple_of(target * rows, rows), rows), :], wout[:, p])

    def columns_of(p):
        return pl.ds(pl.multiple_of(p * piece_w, LANES), piece_w)

    def sum_copy(target, p, side):
        landing, receive, way = (from_right, rl_recv, -1) if side == 0 else (from_left, rr_recv, 1)
        return remote(
            stage.at[target, :, columns_of(p)],
            landing.at[target, :, columns_of(p)],
            r_send.at[target, p],
            receive.at[target, p],
            {"tp": z + way},
        )

    items = (n - 1) * pieces
    lag = 3

    def one_sum(t, _):
        for side in range(2):
            i = t - lag * (n - 1 - z) if side == 0 else t - lag * z
            k, p = jnp.maximum(i, 0) // pieces, lax.rem(jnp.maximum(i, 0), pieces)
            target = k if side == 0 else n - 1 - k
            landing = from_right if side == 0 else from_left
            active = target < z if side == 0 else target > z
            more = z < n - 1 if side == 0 else z > 0
            active = jnp.logical_and(active, jnp.logical_and(i >= 0, i < items))

            @pl.when(active)
            def _():
                value = partial_of(target, columns_of(p))

                @pl.when(more)
                def _():
                    sum_copy(target, p, side).wait_recv()
                    stage[target, :, columns_of(p)] = (
                        value + landing[target, :, columns_of(p)].astype(jnp.float32)
                    ).astype(jnp.bfloat16)

                @pl.when(jnp.logical_not(more))
                def _():
                    stage[target, :, columns_of(p)] = value.astype(jnp.bfloat16)

                sum_copy(target, p, side).start()

        @pl.when(jnp.logical_and(t >= items, t < items + pieces))
        def _():
            columns = columns_of(t - items)
            own_sum[:, columns] = tokens[:, columns].astype(jnp.float32) + partial_of(z, columns)

        return 0

    lax.fori_loop(0, items + max(lag * (n - 1), pieces), one_sum, 0)

    def finish(p, _):
        columns = columns_of(p)
        @pl.when(z < n - 1)
        def _():
            sum_copy(z, p, 0).wait_recv()

        @pl.when(z > 0)
        def _():
            sum_copy(z, p, 1).wait_recv()

        none = jnp.zeros((rows, piece_w), jnp.float32)
        right = jnp.where(z < n - 1, from_right[z, :, columns].astype(jnp.float32), none)
        left = jnp.where(z > 0, from_left[z, :, columns].astype(jnp.float32), none)
        out[:, columns] = (own_sum[:, columns] + right + left).astype(jnp.bfloat16)
        return 0

    lax.fori_loop(0, pieces, finish, 0)

    def sent_rows(source, _):
        for part in range(2):

            @pl.when(jnp.logical_and(source <= z, z < n - 1))
            def _():
                row_copy(source, part, 0).wait_send()

            @pl.when(jnp.logical_and(source >= z, z > 0))
            def _():
                row_copy(source, part, 1).wait_send()

        return 0

    lax.fori_loop(0, n, sent_rows, 0)

    def sent_small(i):
        tap_copy(z, i).wait_send()
        square_copy(z, i).wait_send()
        out_copy(z, i).wait_send()
        for chunk in range(n):
            in_copy(z, chunk, i).wait_send()

        def sent_sum(p, _):
            sum_copy(i, p, 0).wait_send()
            return 0

        lax.fori_loop(0, pieces, sent_sum, 0)

    each_other(sent_small)

    @pl.when(s < shards - 1)
    def _():
        inner_tail().wait_send()
        for other in range(n):
            state_tail(z, other).wait_send()
        for c in range(quads):
            end_copy(c).wait_send()


def body(
    n,
    shards,
    tokens,
    pre_gain,
    proj_inner,
    proj_gate,
    proj_states,
    proj_step,
    step_bias,
    log_rate,
    conv_inner,
    conv_states,
    skip_gain,
    norm_gain,
    proj_output,
):
    rows, width = tokens.shape
    inner, state_w, heads = proj_inner.shape[1], proj_states.shape[1], proj_step.shape[1]
    total = n * rows
    all_states = n * state_w
    quads = heads // GROUPS
    pieces = 8
    bf16, f32 = jnp.bfloat16, jnp.float32
    vmem = pl.BlockSpec(memory_space=pltpu.VMEM)
    far = pl.BlockSpec(memory_space=pl.ANY)
    dma = pltpu.SemaphoreType.DMA
    return pl.pallas_call(
        partial(fused_kernel, n, shards),
        out_shape=jax.ShapeDtypeStruct((rows, width), bf16),
        in_specs=[far, vmem, far, far, far, far, vmem, vmem, vmem, vmem, vmem, vmem, far],
        out_specs=vmem,
        scratch_shapes=[
            pltpu.VMEM((rows, width), bf16),
            pltpu.VMEM((width, 2 * inner + state_w), bf16),
            pltpu.VMEM((heads, width), bf16),
            pltpu.VMEM((inner, width), bf16),
            pltpu.VMEM((total, width), bf16),
            pltpu.VMEM((PAD + total, 2 * inner), bf16),
            pltpu.VMEM((PAD + total, all_states), bf16),
            pltpu.VMEM((n,) + conv_states.shape, f32),
            pltpu.VMEM((total, heads), f32),
            pltpu.VMEM((total, LANES), f32),
            pltpu.VMEM((total, inner), bf16),
            pltpu.VMEM((total, all_states), bf16),
            pltpu.VMEM((total, inner), f32),
            pltpu.VMEM((STATE, inner), f32),
            pltpu.VMEM((STATE, inner), bf16),
            pltpu.VMEM((STATE, inner), bf16),
            pltpu.VMEM((n, 8, total), f32),
            pltpu.VMEM((total, inner), bf16),
            pltpu.VMEM((n, rows, width), bf16),
            pltpu.VMEM((n, rows, width), bf16),
            pltpu.VMEM((n, rows, width), bf16),
            pltpu.VMEM((rows, width), f32),
            dma((6,)),
            pltpu.SemaphoreType.REGULAR((2,)),
            pltpu.SemaphoreType.REGULAR,
            dma((2, n, 2)),
            dma((n, 2)),
            dma((n,)),
            dma((n,)),
            dma((n, n)),
            dma((n, n)),
            dma((n,)),
            dma((n,)),
            dma,
            dma,
            dma((n,)),
            dma((n,)),
            dma((quads,)),
            dma((quads,)),
            dma((n,)),
            dma((n,)),
            dma((n, pieces)),
            dma((n, pieces)),
            dma((n, pieces)),
        ],
        compiler_params=pltpu.CompilerParams(
            collective_id=0, has_side_effects=True, vmem_limit_bytes=62 * 1024 * 1024
        ),
    )(
        tokens,
        pre_gain[None],
        proj_inner,
        proj_gate,
        proj_states,
        proj_step.T,
        step_bias[None],
        log_rate[None],
        conv_inner,
        conv_states,
        skip_gain[None],
        norm_gain[None],
        proj_output,
    )


def solution(mesh):
    n, shards = mesh.shape["tp"], mesh.shape["seq"]
    plain = plain_solution(mesh)

    def run(*arrays):
        tokens, proj_inner, proj_states, proj_step = arrays[0], arrays[2], arrays[4], arrays[5]
        rows = tokens.shape[0] // (mesh.shape["dp"] * shards * n)
        heads, state_w = proj_step.shape[1] // n, proj_states.shape[1] // n
        fits = (
            rows % 32 == 0
            and (rows * n) % BLOCK == 0
            and state_w == 2 * STATE
            and heads % GROUPS == 0
            and (proj_inner.shape[1] // n) % 256 == 0
        )
        if not fits:
            return plain(*arrays)
        line = P(("dp", "seq", "tp"), None)
        columns = P(None, "tp")
        placed = (
            (line, P()) + (columns,) * 4 + (P("tp"), P("tp"), columns, columns)
            + (P("tp"), P("tp"), P("tp", None))
        )
        return jax.shard_map(
            partial(body, n, shards), mesh=mesh, in_specs=placed, out_specs=line, check_vma=False
        )(*arrays)

    return run
```

```python
from functools import partial

import jax
import jax.numpy as jnp
from jax import lax
from jax.sharding import PartitionSpec as P
from jax.experimental import pallas as pl
from jax.experimental.pallas import tpu as pltpu

HEAD_DIM = 64
STATE = 128
GROUP_HEADS = 16
BLOCK = 128
GROUPS = 4


epsilon = 1e-05
highest = lax.Precision.HIGHEST


def from_behind(value, axis, steps):
    count = lax.axis_size(axis)
    initial, last = (max(0, -steps), min(count, count - steps))
    return lax.ppermute(value, axis, [(source, source + steps) for source in range(initial, last)])


def causal_conv(values, kernel_taps, before):
    length = values.shape[0]
    padded = jnp.concatenate((before, values), axis=0)
    running_sum = jnp.zeros(values.shape, jnp.float32)
    for offset in range(kernel_taps.shape[0]):
        running_sum = running_sum + kernel_taps[offset] * padded[offset : offset + length]
    return running_sum


def block_step(carry_state, inputs, copies):
    values, step_size, log_decay, in_states, out_states = inputs
    block_len = values.shape[0]
    running = jnp.cumsum(log_decay, axis=0)
    scores = jnp.einsum("tgn,sgn->gts", out_states, in_states, precision=highest)
    scores = jnp.tile(scores, (copies, 1, 1))
    places = jnp.arange(block_len)
    lower_mask = (places[:, None] >= places[None, :])[None]
    spread = running.T[:, :, None] - running.T[:, None, :]
    decay_table = jnp.where(lower_mask, jnp.exp(jnp.where(lower_mask, spread, 0.0)), 0.0)
    weights = scores * decay_table * step_size.T[:, None, :]
    within = jnp.einsum("hts,shp->thp", weights, values, precision=highest)
    out_heads = jnp.tile(out_states, (1, copies, 1))
    in_heads = jnp.tile(in_states, (1, copies, 1))
    carried = (
        jnp.einsum("thn,hpn->thp", out_heads, carry_state, precision=highest)
        * jnp.exp(running)[:, :, None]
    )
    tail_decay = jnp.exp(running[-1][None, :] - running) * step_size
    scaled = values * tail_decay[:, :, None]
    new_state = jnp.exp(running[-1])[:, None, None] * carry_state + jnp.einsum(
        "shp,shn->hpn", scaled, in_heads, precision=highest
    )
    return (new_state, within + carried)


def scan_blocks(
    values, step_size, log_decay, in_states, out_states, carry_state, block_len, copies
):
    row_count, head_count, head_dim = values.shape
    block_count = row_count // block_len

    def split_blocks(source):
        return source.reshape((block_count, block_len) + source.shape[1:])

    final_state, outputs = lax.scan(
        partial(block_step, copies=copies),
        carry_state,
        (
            split_blocks(values),
            split_blocks(step_size),
            split_blocks(log_decay),
            split_blocks(in_states),
            split_blocks(out_states),
        ),
    )
    return (final_state, outputs.reshape(row_count, head_count, head_dim))


def plain_body(
    tokens,
    pre_gain,
    proj_inner,
    proj_gate,
    proj_states,
    proj_step,
    step_bias,
    log_rate,
    conv_inner,
    conv_states,
    skip_gain,
    norm_gain,
    proj_output,
):
    tokens_wide = tokens.astype(jnp.float32)
    normed = (
        tokens_wide
        * lax.rsqrt(jnp.mean(tokens_wide * tokens_wide, axis=1, keepdims=True) + epsilon)
        * pre_gain
    ).astype(jnp.bfloat16)
    inner_width = proj_inner.shape[1]
    state_width = proj_states.shape[1]
    heads_local = proj_step.shape[1]
    copies = heads_local // GROUPS
    row_piece = lax.all_gather(normed, "tp", axis=0, tiled=True)
    projected = jnp.concatenate(
        (
            jnp.dot(row_piece, proj_inner, preferred_element_type=jnp.float32),
            jnp.dot(row_piece, proj_gate, preferred_element_type=jnp.float32),
            jnp.dot(row_piece, proj_states, preferred_element_type=jnp.float32),
            jnp.dot(row_piece, proj_step, preferred_element_type=jnp.float32),
        ),
        axis=1,
    )
    row_count = projected.shape[0]
    inner_proj = projected[:, :inner_width].astype(jnp.bfloat16)
    gate_proj = projected[:, inner_width : 2 * inner_width].astype(jnp.bfloat16)
    state_proj = projected[:, 2 * inner_width : 2 * inner_width + state_width].astype(jnp.bfloat16)
    step_size = jax.nn.softplus(projected[:, 2 * inner_width + state_width :] + step_bias)
    log_decay = -jnp.exp(log_rate) * step_size
    margin = conv_inner.shape[0] - 1
    before_inner, before_states = from_behind(
        (inner_proj[row_count - margin :], state_proj[row_count - margin :]), "seq", 1
    )
    mixed_inner = jax.nn.silu(
        causal_conv(inner_proj.astype(jnp.float32), conv_inner, before_inner.astype(jnp.float32))
    ).astype(jnp.bfloat16)
    mixed_local = jax.nn.silu(
        causal_conv(state_proj.astype(jnp.float32), conv_states, before_states.astype(jnp.float32))
    ).astype(jnp.bfloat16)
    mixed_all = lax.all_gather(mixed_local, "tp", axis=1, tiled=True)
    values = mixed_inner.astype(jnp.float32).reshape(row_count, heads_local, HEAD_DIM)
    paired = mixed_all.astype(jnp.float32).reshape(row_count, GROUPS, 2, STATE)
    in_states = paired[:, :, 0]
    out_states = paired[:, :, 1]
    zero_state = jnp.zeros((heads_local, HEAD_DIM, STATE), jnp.float32)
    final_state, scanned = scan_blocks(
        values, step_size, log_decay, in_states, out_states, zero_state, BLOCK, copies
    )
    decay_sum = jnp.sum(log_decay, axis=0)
    decay_sums, summaries = (
        lax.all_gather(decay_sum[None].astype(jnp.bfloat16), "seq", axis=0, tiled=True).astype(
            jnp.float32
        ),
        lax.all_gather(final_state[None].astype(jnp.bfloat16), "seq", axis=0, tiled=True).astype(
            jnp.float32
        ),
    )
    position = lax.axis_index("seq")
    device_ids = jnp.arange(decay_sums.shape[0])
    earlier_mask = (device_ids < position)[:, None]
    before_me = jnp.sum(jnp.where(earlier_mask, decay_sums, 0.0), axis=0)
    reach_end = jnp.cumsum(decay_sums, axis=0)
    weights = jnp.where(
        earlier_mask, jnp.exp(jnp.where(earlier_mask, before_me[None] - reach_end, 0.0)), 0.0
    )
    incoming = jnp.einsum("jh,jhpn->hpn", weights, summaries, precision=highest)
    running = jnp.cumsum(log_decay, axis=0)
    out_heads = jnp.tile(out_states, (1, copies, 1))
    carried = (
        jnp.einsum("thn,hpn->thp", out_heads, incoming, precision=highest)
        * jnp.exp(running)[:, :, None]
    )
    ssd_out = scanned + carried + skip_gain[None, :, None] * values
    gated_out = ssd_out * jax.nn.silu(gate_proj.astype(jnp.float32)).reshape(
        row_count, heads_local, HEAD_DIM
    )
    head_squares = jnp.sum(gated_out * gated_out, axis=2)
    every_square = lax.all_gather(head_squares, "tp", axis=1, tiled=True)
    group_totals = jnp.sum(
        every_square.reshape(row_count, every_square.shape[1] // GROUPS, GROUPS), axis=1
    )
    mean_square = (group_totals / (GROUP_HEADS * HEAD_DIM))[:, None, :, None]
    grouped = gated_out.reshape(row_count, copies, GROUPS, HEAD_DIM)
    normal_out = grouped * lax.rsqrt(mean_square + epsilon)
    mixed_out = (normal_out.reshape(row_count, inner_width) * norm_gain).astype(jnp.bfloat16)
    summed = lax.psum_scatter(
        jnp.dot(mixed_out, proj_output, preferred_element_type=jnp.float32).astype(jnp.bfloat16),
        "tp",
        scatter_dimension=0,
        tiled=True,
    ).astype(jnp.float32)
    return (tokens_wide + summed).astype(jnp.bfloat16)


def plain_solution(mesh):
    placed = (
        P(("dp", "seq", "tp"), None),
        P(),
        P(None, "tp"),
        P(None, "tp"),
        P(None, "tp"),
        P(None, "tp"),
        P("tp"),
        P("tp"),
        P(None, "tp"),
        P(None, "tp"),
        P("tp"),
        P("tp"),
        P("tp", None),
    )
    return jax.shard_map(
        plain_body, mesh=mesh, in_specs=placed, out_specs=P(("dp", "seq", "tp"), None), check_vma=False
    )


LANES = 128
PAD = 16
MESH = pl.DeviceIdType.MESH
NT = (((1,), (1,)), ((), ()))


def remote(source, target, send, receive, device):
    return pltpu.make_async_remote_copy(
        src_ref=source,
        dst_ref=target,
        send_sem=send,
        recv_sem=receive,
        device_id=device,
        device_id_type=MESH,
    )


def bdot(a, b):
    return jnp.dot(a, b, preferred_element_type=jnp.float32)


def fused_kernel(
    n,
    shards,
    shared,
    tokens_far,
    pre_gain,
    w_inner,
    w_gate,
    w_states,
    w_step,
    step_bias,
    log_rate,
    taps_inner,
    taps_states,
    skip_gain,
    norm_gain,
    w_out,
    out,
    tokens,
    wide,
    step_w,
    wout,
    rows_all,
    proj,
    states,
    taps_all,
    raw_step,
    run_ref,
    x_mix,
    s_mix,
    acc,
    ends,
    state_out,
    state_in,
    squares,
    mixed,
    stage,
    from_right,
    from_left,
    own_sum,
    spare,
    pre,
    far,
    load_sem,
    line,
    ahead,
    g_send,
    g_recv,
    t_send,
    t_recv,
    s_send,
    s_recv,
    c_send,
    c_recv,
    ti_send,
    ti_recv,
    ts_send,
    ts_recv,
    e_send,
    e_recv,
    q_send,
    q_recv,
    r_send,
    rl_recv,
    rr_recv,
    wz_send,
    wz_recv,
    wy_send,
    wy_recv,
    wx_send,
    wx_recv,
    wd_send,
    wd_recv,
    m_send,
    m_recv,
):
    z = lax.axis_index("tp")
    s = lax.axis_index("seq")
    part_id = lax.axis_index("dp")
    rows, width = tokens.shape
    total = n * rows
    inner = w_inner.shape[1]
    state_w = w_states.shape[1]
    heads = w_step.shape[0]
    half = rows // 2
    at_end = jnp.logical_or(z == 0, z == n - 1)
    beside = jnp.logical_or(z == 1, z == n - 2)
    across = lax.rem(s + shards // 2, shards)
    sibling = s + 1 - 2 * lax.rem(s, 2)

    token_load = pltpu.make_async_copy(tokens_far, tokens, load_sem.at[5])
    token_load.start()
    barrier = pltpu.get_barrier_semaphore()
    neighbours = (
        (z > 0, {"tp": z - 1}),
        (z < n - 1, {"tp": z + 1}),
        (s > 0, {"seq": s - 1}),
        (s < shards - 1, {"seq": s + 1}),
        (z >= 0, {"seq": across}),
        (z >= 0, {"dp": 1 - part_id}),
    )
    met = jnp.int32(0)
    for there, device in neighbours:
        met = met + there.astype(jnp.int32)

        @pl.when(there)
        def _():
            pl.semaphore_signal(barrier, inc=1, device_id=device, device_id_type=MESH)

    loads = [
        pltpu.make_async_copy(w_states, wide.at[:, pl.ds(2 * inner, state_w)], load_sem.at[0]),
        pltpu.make_async_copy(w_step, step_w, load_sem.at[1]),
        pltpu.make_async_copy(w_inner, wide.at[:, pl.ds(0, inner)], load_sem.at[2]),
        pltpu.make_async_copy(w_gate, wide.at[:, pl.ds(inner, inner)], load_sem.at[3]),
        pltpu.make_async_copy(w_out, wout, load_sem.at[4]),
    ]
    token_load.wait()
    for load in loads[:4]:
        load.start()

    def own_rows(i, _):
        piece = pl.ds(pl.multiple_of(i * 16, 16), 16)
        value = tokens[piece, :].astype(jnp.float32)
        scale = lax.rsqrt(jnp.mean(value * value, axis=1, keepdims=True) + epsilon)
        place = pl.ds(pl.multiple_of(z * rows + i * 16, 16), 16)
        rows_all[place, :] = (value * scale * pre_gain[...]).astype(jnp.bfloat16)
        return 0

    lax.fori_loop(0, half // 16, own_rows, 0)
    taps_all[z] = taps_states[...]

    @pl.when(s == 0)
    def _():
        proj[0:PAD, 0:inner] = jnp.zeros((PAD, inner), jnp.bfloat16)
        states[0:PAD, :] = jnp.zeros((PAD, states.shape[1]), jnp.bfloat16)
        state_in[...] = jnp.zeros(state_in.shape, jnp.bfloat16)

    pl.semaphore_wait(barrier, met)

    def row_copy(source, part, side):
        block = rows_all.at[pl.ds(pl.multiple_of(source * rows + part * half, 16), half), :]
        step = 1 if side == 0 else -1
        return remote(
            block, block, g_send.at[side, source, part], g_recv.at[source, part], {"tp": z + step}
        )

    def send_on(source, part):
        @pl.when(jnp.logical_and(source <= z, z < n - 1))
        def _():
            row_copy(source, part, 0).start()

        @pl.when(jnp.logical_and(source >= z, z > 0))
        def _():
            row_copy(source, part, 1).start()

    slice_rows = inner // (2 * shards)
    chunk_rows = slice_rows // 2
    shared_w = spare.shape[1]

    def slice_of(d, q, c):
        first = (d * shards + q) * slice_rows + c * chunk_rows
        return pl.ds(pl.multiple_of(first, chunk_rows), chunk_rows)

    def down_copy(c):
        block = slice_of(part_id, s, c)
        return remote(
            w_out.at[block, pl.ds(0, shared_w)],
            spare.at[block, :],
            wz_send.at[c],
            wz_recv.at[c],
            {"tp": jnp.where(z == 0, 1, n - 2)},
        )

    def y_copy(c):
        block = spare.at[slice_of(part_id, s, c), :]
        return remote(block, block, wy_send.at[c], wy_recv.at[c], {"dp": 1 - part_id})

    def y_taken(c):
        block = spare.at[slice_of(1 - part_id, s, c), :]
        return remote(block, block, wy_send.at[c], wy_recv.at[c], {"dp": 1 - part_id})

    def x_copy(k, c, to):
        d = part_id if k == 0 else 1 - part_id
        block = spare.at[slice_of(d, s if to else across, c), :]
        return remote(block, block, wx_send.at[k, c], wx_recv.at[k, c], {"seq": across})

    def core_copy(j, to):
        d = part_id if j % 2 == 0 else 1 - part_id
        q = s if j < 2 else across
        q = q if to else q + 1 - 2 * lax.rem(q, 2)
        first = (d * shards + q) * slice_rows
        block = spare.at[pl.ds(pl.multiple_of(first, slice_rows), slice_rows), :]
        return remote(block, block, wd_send.at[j], wd_recv.at[j], {"seq": sibling})

    def send_down(c):
        @pl.when(at_end)
        def _():
            down_copy(c).start()

    send_on(z, 0)
    send_down(0)
    lax.fori_loop(half // 16, rows // 16, own_rows, 0)
    send_on(z, 1)
    send_down(1)

    def greet_line(side, condition):
        @pl.when(condition)
        def _():
            pl.semaphore_signal(
                line.at[side],
                inc=1,
                device_id={"tp": z + 1 if side == 0 else z - 1},
                device_id_type=MESH,
            )

    greet_line(0, z == 0)
    greet_line(1, z == n - 1)
    for side in range(2):
        edge = 0 if side == 0 else n - 1

        @pl.when(z != edge)
        def _():
            pl.semaphore_wait(line.at[side], 1)

        greet_line(side, jnp.logical_and(z != edge, z != n - 1 - edge))

    @pl.when(s > 0)
    def _():
        pl.semaphore_signal(ahead, inc=1, device_id={"seq": s - 1}, device_id_type=MESH)


    def tap_copy(source, other):
        return remote(
            taps_all.at[source], taps_all.at[source], t_send.at[other], t_recv.at[source], {"tp": other}
        )

    def in_copy(source, chunk, other):
        block = states.at[
            pl.ds(pl.multiple_of(PAD + chunk * rows, 16), rows),
            pl.ds(pl.multiple_of(source * state_w, LANES), STATE),
        ]
        return remote(
            block, block, s_send.at[chunk, other], s_recv.at[source, chunk], {"tp": other}
        )

    def out_copy(source, other):
        block = states.at[
            pl.ds(PAD, total), pl.ds(pl.multiple_of(source * state_w + STATE, LANES), STATE)
        ]
        return remote(block, block, c_send.at[other], c_recv.at[source], {"tp": other})

    def square_copy(source, other):
        return remote(
            squares.at[source], squares.at[source], q_send.at[other], q_recv.at[source], {"tp": other}
        )

    def each_other(action):
        def one(i, _):
            @pl.when(i != z)
            def _():
                action(i)

            return 0

        lax.fori_loop(0, n, one, 0)

    each_other(lambda i: tap_copy(z, i).start())

    def inner_tail():
        return remote(
            proj.at[pl.ds(total, PAD), pl.ds(0, inner)],
            proj.at[pl.ds(0, PAD), pl.ds(0, inner)],
            ti_send,
            ti_recv,
            {"seq": s + 1, "tp": z},
        )

    def state_tail(source, other):
        columns = pl.ds(pl.multiple_of(source * state_w, LANES), state_w)
        return remote(
            states.at[pl.ds(total, PAD), columns],
            states.at[pl.ds(0, PAD), columns],
            ts_send.at[other],
            ts_recv.at[source],
            {"seq": s + 1, "tp": other},
        )

    for load in loads[:4]:
        load.wait()
    loads[4].start()

    gate_tile = inner // 256

    def project_tiles(chunk, first, end):
        piece = pl.ds(pl.multiple_of(chunk * rows, rows), rows)
        place = pl.ds(pl.multiple_of(PAD + chunk * rows, 16), rows)

        def tile(i, _):
            columns = pl.ds(pl.multiple_of(i * 256, 256), 256)
            proj[place, columns] = bdot(rows_all[piece, :], wide[:, columns]).astype(jnp.bfloat16)
            return 0

        lax.fori_loop(first, end, tile, 0)

    def project(chunk):
        piece = pl.ds(pl.multiple_of(chunk * rows, rows), rows)
        place = pl.ds(pl.multiple_of(PAD + chunk * rows, 16), rows)
        own = pl.ds(pl.multiple_of(z * state_w, LANES), state_w)
        states[place, own] = bdot(
            rows_all[piece, :], wide[:, 2 * inner : 2 * inner + state_w]
        ).astype(jnp.bfloat16)
        each_other(lambda i: in_copy(z, chunk, i).start())

        @pl.when(jnp.logical_and(chunk == n - 1, s < shards - 1))
        def _():
            pl.semaphore_wait(ahead, 1)
            for other in range(n):
                state_tail(z, other).start()

        raw_step[piece, :] = lax.dot_general(
            rows_all[piece, :], step_w[...], NT, preferred_element_type=jnp.float32
        )

        project_tiles(chunk, 0, gate_tile)

        @pl.when(jnp.logical_and(chunk == n - 1, s < shards - 1))
        def _():
            inner_tail().start()


    def arrive(distance, _):
        for part in range(2):
            for side in range(2):
                source = z - distance if side == 0 else z + distance
                inside = jnp.logical_and(source >= 0, source < n)

                @pl.when(jnp.logical_and(inside, distance > 0))
                def _():
                    row_copy(source, part, side).wait_recv()
                    send_on(source, part)

        @pl.when(jnp.logical_and(beside, distance == 1))
        def _():
            down_copy(0).wait_recv()
            y_copy(0).start()
            x_copy(0, 0, True).start()

        @pl.when(jnp.logical_and(beside, distance == 2))
        def _():
            y_taken(0).wait_recv()
            x_copy(1, 0, True).start()
            down_copy(1).wait_recv()
            y_copy(1).start()
            x_copy(0, 1, True).start()

        @pl.when(jnp.logical_and(beside, distance == 3))
        def _():
            y_taken(1).wait_recv()
            x_copy(1, 1, True).start()
            for j in range(2):
                core_copy(j, True).start()

        def one(side, _):
            source = z - distance + 2 * distance * side
            inside = jnp.logical_and(source >= 0, source < n)

            @pl.when(jnp.logical_and(inside, jnp.logical_or(distance > 0, side == 0)))
            def _():
                project(source)

            return 0

        lax.fori_loop(0, 2, one, 0)
        return 0

    lax.fori_loop(0, n, arrive, 0)

    def gate_tiles(i, _):
        columns = pl.ds(pl.multiple_of(inner + i * 256, 256), 256)
        proj[pl.ds(PAD, total), columns] = bdot(rows_all[...], wide[:, columns]).astype(jnp.bfloat16)
        return 0

    each_other(lambda i: out_copy(z, i).start())

    step = raw_step[...] + step_bias[...]
    step = jnp.maximum(step, 0.0) + jnp.log1p(jnp.exp(-jnp.abs(step)))
    decay = -jnp.exp(log_rate[...]) * step
    place_t = lax.broadcasted_iota(jnp.int32, (total, total), 0)
    place_s = lax.broadcasted_iota(jnp.int32, (total, total), 1)
    tri = (place_t >= place_s).astype(jnp.float32)
    run = jnp.dot(tri, decay, precision=highest, preferred_element_type=jnp.float32)
    run_ref[...] = jnp.zeros(run_ref.shape, jnp.float32)
    run_ref[:, 0:heads] = run
    run_t = run_ref[...].T
    last = run[total - 1 : total, :]
    reach = jnp.exp(last - run) * step
    grown = jnp.exp(run)
    whole = jnp.exp(last)
    lane = lax.broadcasted_iota(jnp.int32, (1, LANES), 1)
    low = lane < HEAD_DIM

    def conv(buffer, columns, taps):
        value = buffer[:, columns].astype(jnp.float32)
        kernel_len = taps.shape[0]
        out_value = jnp.zeros((total, value.shape[1]), jnp.float32)
        for k in range(kernel_len):
            first = PAD - (kernel_len - 1) + k
            out_value = out_value + taps[k : k + 1, :] * value[first : first + total, :]
        return jax.nn.silu(out_value).astype(jnp.bfloat16)

    @pl.when(s > 0)
    def _():
        inner_tail().wait_recv()

    def conv_tile(i, _):
        columns = pl.ds(pl.multiple_of(i * 256, 256), 256)
        x_mix[:, columns] = conv(proj, columns, taps_inner[:, columns])
        return 0

    lax.fori_loop(0, inner // 256, conv_tile, 0)

    def take_states(part, i):
        columns = pl.ds(pl.multiple_of(i * state_w + part * STATE, LANES), STATE)
        taps = taps_all[i][:, part * STATE : (part + 1) * STATE]
        s_mix[:, columns] = conv(states, columns, taps)

    def take_in(i, _):
        @pl.when(i != z)
        def _():
            tap_copy(i, z).wait_recv()
            for chunk in range(n):
                in_copy(i, chunk, z).wait_recv()

        @pl.when(s > 0)
        def _():
            state_tail(i, z).wait_recv()

        take_states(0, i)
        return 0

    def take_out(i, _):
        @pl.when(i != z)
        def _():
            out_copy(i, z).wait_recv()

        take_states(1, i)
        return 0

    lax.fori_loop(0, n, take_in, 0)

    def group_in(g):
        return s_mix[:, g * 2 * STATE : g * 2 * STATE + STATE]

    def group_out(g):
        return s_mix[:, g * 2 * STATE + STATE : (g + 1) * 2 * STATE]

    def pair_of(value, h):
        return jnp.where(low, value[:, h : h + 1], value[:, h + 1 : h + 2])

    pairs = heads // 2
    per_quad = GROUPS // 2
    quads = pairs // per_quad
    quad_w = GROUPS * HEAD_DIM

    def end_copy(c):
        columns = pl.ds(c * quad_w, quad_w)
        return remote(
            state_out.at[:, columns],
            state_in.at[:, columns],
            e_send.at[c],
            e_recv.at[c],
            {"seq": s + 1, "tp": z},
        )

    turned = [group_in(g).T for g in range(GROUPS)]
    for q in range(pairs):
        columns = slice(q * LANES, (q + 1) * LANES)
        h = 2 * q
        scaled = (x_mix[:, columns].astype(jnp.float32) * pair_of(reach, h)).astype(jnp.bfloat16)
        ends[:, columns] = jnp.where(
            low, bdot(turned[h % GROUPS], scaled), bdot(turned[(h + 1) % GROUPS], scaled)
        )
        if q % per_quad == per_quad - 1:
            c = q // per_quad

            @pl.when(jnp.logical_and(s == 0, shards > 1))
            def _():
                columns = slice(c * quad_w, (c + 1) * quad_w)
                state_out[:, columns] = ends[:, columns].astype(jnp.bfloat16)
                end_copy(c).start()

    def hand_on(c, here):
        @pl.when(here)
        def _():
            end_copy(c).wait_recv()

            @pl.when(s < shards - 1)
            def _():
                for q in range(c * per_quad, (c + 1) * per_quad):
                    columns = slice(q * LANES, (q + 1) * LANES)
                    state_out[:, columns] = (
                        ends[:, columns]
                        + pair_of(whole, 2 * q) * state_in[:, columns].astype(jnp.float32)
                    ).astype(jnp.bfloat16)
                end_copy(c).start()

    lax.fori_loop(0, gate_tile // 2, gate_tiles, 0)
    for c in range(quads):
        hand_on(c, s == 1)
    lax.fori_loop(gate_tile // 2, gate_tile, gate_tiles, 0)

    @pl.when(beside)
    def _():
        for k in range(2):
            for c in range(2):
                x_copy(k, c, False).wait_recv()
            core_copy(2 + k, True).start()

    lax.fori_loop(0, n, take_out, 0)

    scores = [
        lax.dot_general(group_out(g), group_in(g), NT, preferred_element_type=jnp.float32)
        for g in range(GROUPS)
    ]
    for q in range(pairs):
        columns = slice(q * LANES, (q + 1) * LANES)
        h = 2 * q
        value = x_mix[:, columns].astype(jnp.float32)
        stepped = (value * pair_of(step, h)).astype(jnp.bfloat16)
        direct = value * pair_of(skip_gain[...], h)
        for low_t in range(0, total, BLOCK):
            high_t = low_t + BLOCK
            causal = place_t[low_t:high_t, :high_t] >= place_s[low_t:high_t, :high_t]
            both = []
            for k in (h, h + 1):
                spread = run[low_t:high_t, k : k + 1] - run_t[k : k + 1, :high_t]
                table = jnp.where(causal, jnp.exp(jnp.where(causal, spread, 0.0)), 0.0)
                weights = (scores[k % GROUPS][low_t:high_t, :high_t] * table).astype(jnp.bfloat16)
                both.append(bdot(weights, stepped[:high_t, :]))
            acc[low_t:high_t, columns] = jnp.where(low, both[0], both[1]) + direct[low_t:high_t, :]
    sums = [jnp.zeros((total, LANES), jnp.float32) for _ in range(per_quad)]
    for q in range(pairs):
        columns = slice(q * LANES, (q + 1) * LANES)
        h = 2 * q
        if q % per_quad == 0:
            hand_on(q // per_quad, s > 1)
        came = state_in[:, columns]
        carried = jnp.where(
            low, bdot(group_out(h % GROUPS), came), bdot(group_out((h + 1) % GROUPS), came)
        )
        gate = proj[PAD:, inner + q * LANES : inner + (q + 1) * LANES].astype(jnp.float32)
        gated = (acc[:, columns] + carried * pair_of(grown, h)) * jax.nn.silu(gate)
        acc[:, columns] = gated
        sums[q % per_quad] = sums[q % per_quad] + gated * gated
    pick = lax.broadcasted_iota(jnp.int32, (8, LANES), 0)
    where_lane = lax.broadcasted_iota(jnp.int32, (8, LANES), 1)
    local = jnp.zeros((8, total), jnp.float32)
    for k in range(per_quad):
        chosen = (where_lane // HEAD_DIM + 2 * k == pick).astype(jnp.float32)
        local = local + lax.dot_general(
            chosen, sums[k], NT, precision=highest, preferred_element_type=jnp.float32
        )
    squares[z] = local
    each_other(lambda i: square_copy(z, i).start())

    def mix_copy(target):
        place = pl.ds(pl.multiple_of(target * rows, rows), rows)
        return remote(
            pre.at[place, :],
            far.at[place, :],
            m_send.at[target],
            m_recv.at[target],
            {"tp": jnp.where(z == 0, 1, n - 2)},
        )

    @pl.when(at_end)
    def _():
        for q in range(pairs):
            columns = slice(q * LANES, (q + 1) * LANES)
            pre[:, columns] = (acc[:, columns] * norm_gain[:, columns]).astype(jnp.bfloat16)
        for i in range(n - 1):
            mix_copy(jnp.where(z == 0, n - 1 - i, i)).start()

    loads[4].wait()
    each_other(lambda i: square_copy(i, z).wait_recv())
    sum_all = squares[0]
    for i in range(1, n):
        sum_all = sum_all + squares[i]
    inverse = lax.rsqrt(sum_all / (n * heads // GROUPS * HEAD_DIM) + epsilon)
    inverse = jnp.concatenate([inverse] * (LANES // 8), axis=0).T
    run_ref[...] = inverse
    for q in range(pairs):
        columns = slice(q * LANES, (q + 1) * LANES)
        g = (2 * q) % GROUPS
        mixed[:, columns] = (
            acc[:, columns] * pair_of(inverse, g) * norm_gain[:, columns]
        ).astype(jnp.bfloat16)

    pieces = r_send.shape[1]
    piece_w = width // pieces

    def partial_of(target, p):
        return bdot(mixed[pl.ds(pl.multiple_of(target * rows, rows), rows), :], wout[:, p])

    def columns_of(p):
        return pl.ds(pl.multiple_of(p * piece_w, LANES), piece_w)

    def sum_copy(target, p, side):
        landing, receive, way = (from_right, rl_recv, -1) if side == 0 else (from_left, rr_recv, 1)
        return remote(
            stage.at[target, :, columns_of(p)],
            landing.at[target, :, columns_of(p)],
            r_send.at[target, p],
            receive.at[target, p],
            {"tp": z + way},
        )

    def far_partial(target, p):
        place = pl.ds(pl.multiple_of(target * rows, rows), rows)
        return bdot(far[place, :], spare[:, p])

    def take_far(target):
        place = pl.ds(pl.multiple_of(target * rows, rows), rows)
        mix_copy(target).wait_recv()
        scale = run_ref[place, :]
        for q in range(pairs):
            columns = slice(q * LANES, (q + 1) * LANES)
            far[place, columns] = (
                far[place, columns].astype(jnp.float32) * pair_of(scale, (2 * q) % GROUPS)
            ).astype(jnp.bfloat16)

    @pl.when(beside)
    def _():
        for j in range(4):
            core_copy(j, False).wait_recv()

    items = (n - 1) * pieces
    lag = 3

    def one_sum(t, _):
        for side in range(2):
            i = t - lag * (n - 1 - z) if side == 0 else t - lag * z
            k, p = jnp.maximum(i, 0) // pieces, lax.rem(jnp.maximum(i, 0), pieces)
            target = k if side == 0 else n - 1 - k
            landing = from_right if side == 0 else from_left
            active = target < z if side == 0 else target > z
            more = z < n - 1 if side == 0 else z > 0
            active = jnp.logical_and(active, jnp.logical_and(i >= 0, i < items))

            has_far = z == n - 2 if side == 0 else z == 1
            is_end = z == n - 1 if side == 0 else z == 0
            use_far = jnp.logical_and(has_far, p < shared)
            active = jnp.logical_and(active, jnp.logical_or(p >= shared, jnp.logical_not(is_end)))

            @pl.when(jnp.logical_and(active, jnp.logical_and(has_far, p == 0)))
            def _():
                take_far(target)

            @pl.when(active)
            def _():
                value = partial_of(target, columns_of(p))

                @pl.when(use_far)
                def _():
                    stage[target, :, columns_of(p)] = (
                        value + far_partial(target, columns_of(p))
                    ).astype(jnp.bfloat16)

                @pl.when(jnp.logical_and(more, jnp.logical_not(use_far)))
                def _():
                    sum_copy(target, p, side).wait_recv()
                    stage[target, :, columns_of(p)] = (
                        value + landing[target, :, columns_of(p)].astype(jnp.float32)
                    ).astype(jnp.bfloat16)

                @pl.when(jnp.logical_not(more))
                def _():
                    stage[target, :, columns_of(p)] = value.astype(jnp.bfloat16)

                sum_copy(target, p, side).start()

        @pl.when(jnp.logical_and(beside, t == items))
        def _():
            take_far(z)

        @pl.when(jnp.logical_and(t >= items, t < items + pieces))
        def _():
            columns = columns_of(t - items)
            own = tokens[:, columns].astype(jnp.float32) + partial_of(z, columns)
            own_sum[:, columns] = own

            @pl.when(jnp.logical_and(beside, t - items < shared))
            def _():
                own_sum[:, columns] = own + far_partial(z, columns)

        return 0

    lax.fori_loop(0, items + max(lag * (n - 1), pieces), one_sum, 0)

    def finish(p, _):
        columns = columns_of(p)
        lands = (
            jnp.logical_and(z < n - 1, jnp.logical_or(z != n - 2, p >= shared)),
            jnp.logical_and(z > 0, jnp.logical_or(z != 1, p >= shared)),
        )
        for side in range(2):

            @pl.when(lands[side])
            def _():
                sum_copy(z, p, side).wait_recv()

        none = jnp.zeros((rows, piece_w), jnp.float32)
        right = jnp.where(lands[0], from_right[z, :, columns].astype(jnp.float32), none)
        left = jnp.where(lands[1], from_left[z, :, columns].astype(jnp.float32), none)
        out[:, columns] = (own_sum[:, columns] + right + left).astype(jnp.bfloat16)
        return 0

    lax.fori_loop(0, pieces, finish, 0)

    def sent_rows(source, _):
        for part in range(2):

            @pl.when(jnp.logical_and(source <= z, z < n - 1))
            def _():
                row_copy(source, part, 0).wait_send()

            @pl.when(jnp.logical_and(source >= z, z > 0))
            def _():
                row_copy(source, part, 1).wait_send()

        return 0

    lax.fori_loop(0, n, sent_rows, 0)

    def sent_small(i):
        tap_copy(z, i).wait_send()
        square_copy(z, i).wait_send()
        out_copy(z, i).wait_send()
        for chunk in range(n):
            in_copy(z, chunk, i).wait_send()

        def sent_sum(p, _):
            sum_copy(i, p, 0).wait_send()
            return 0

        lax.fori_loop(jnp.where(at_end, shared, 0), pieces, sent_sum, 0)

    each_other(sent_small)

    @pl.when(s < shards - 1)
    def _():
        inner_tail().wait_send()
        for other in range(n):
            state_tail(z, other).wait_send()
        for c in range(quads):
            end_copy(c).wait_send()

    @pl.when(at_end)
    def _():
        for c in range(2):
            down_copy(c).wait_send()
        for i in range(n - 1):
            mix_copy(jnp.where(z == 0, n - 1 - i, i)).wait_send()

    @pl.when(beside)
    def _():
        for c in range(2):
            y_copy(c).wait_send()
            for k in range(2):
                x_copy(k, c, True).wait_send()
        for j in range(4):
            core_copy(j, True).wait_send()


def body(
    n,
    shards,
    tokens,
    pre_gain,
    proj_inner,
    proj_gate,
    proj_states,
    proj_step,
    step_bias,
    log_rate,
    conv_inner,
    conv_states,
    skip_gain,
    norm_gain,
    proj_output,
):
    rows, width = tokens.shape
    inner, state_w, heads = proj_inner.shape[1], proj_states.shape[1], proj_step.shape[1]
    total = n * rows
    all_states = n * state_w
    quads = heads // GROUPS
    pieces, shared = 8, 4
    bf16, f32 = jnp.bfloat16, jnp.float32
    vmem = pl.BlockSpec(memory_space=pltpu.VMEM)
    far = pl.BlockSpec(memory_space=pl.ANY)
    dma = pltpu.SemaphoreType.DMA
    return pl.pallas_call(
        partial(fused_kernel, n, shards, shared),
        out_shape=jax.ShapeDtypeStruct((rows, width), bf16),
        in_specs=[far, vmem, far, far, far, far, vmem, vmem, vmem, vmem, vmem, vmem, far],
        out_specs=vmem,
        scratch_shapes=[
            pltpu.VMEM((rows, width), bf16),
            pltpu.VMEM((width, 2 * inner + state_w), bf16),
            pltpu.VMEM((heads, width), bf16),
            pltpu.VMEM((inner, width), bf16),
            pltpu.VMEM((total, width), bf16),
            pltpu.VMEM((PAD + total, 2 * inner), bf16),
            pltpu.VMEM((PAD + total, all_states), bf16),
            pltpu.VMEM((n,) + conv_states.shape, f32),
            pltpu.VMEM((total, heads), f32),
            pltpu.VMEM((total, LANES), f32),
            pltpu.VMEM((total, inner), bf16),
            pltpu.VMEM((total, all_states), bf16),
            pltpu.VMEM((total, inner), f32),
            pltpu.VMEM((STATE, inner), f32),
            pltpu.VMEM((STATE, inner), bf16),
            pltpu.VMEM((STATE, inner), bf16),
            pltpu.VMEM((n, 8, total), f32),
            pltpu.VMEM((total, inner), bf16),
            pltpu.VMEM((n, rows, width), bf16),
            pltpu.VMEM((n, rows, width), bf16),
            pltpu.VMEM((n, rows, width), bf16),
            pltpu.VMEM((rows, width), f32),
            pltpu.VMEM((inner, width // pieces * shared), bf16),
            pltpu.VMEM((total, inner), bf16),
            pltpu.VMEM((total, inner), bf16),
            dma((6,)),
            pltpu.SemaphoreType.REGULAR((2,)),
            pltpu.SemaphoreType.REGULAR,
            dma((2, n, 2)),
            dma((n, 2)),
            dma((n,)),
            dma((n,)),
            dma((n, n)),
            dma((n, n)),
            dma((n,)),
            dma((n,)),
            dma,
            dma,
            dma((n,)),
            dma((n,)),
            dma((quads,)),
            dma((quads,)),
            dma((n,)),
            dma((n,)),
            dma((n, pieces)),
            dma((n, pieces)),
            dma((n, pieces)),
            dma((2,)),
            dma((2,)),
            dma((2,)),
            dma((2,)),
            dma((2, 2)),
            dma((2, 2)),
            dma((4,)),
            dma((4,)),
            dma((n,)),
            dma((n,)),
        ],
        compiler_params=pltpu.CompilerParams(
            collective_id=0, has_side_effects=True, vmem_limit_bytes=62 * 1024 * 1024
        ),
    )(
        tokens,
        pre_gain[None],
        proj_inner,
        proj_gate,
        proj_states,
        proj_step.T,
        step_bias[None],
        log_rate[None],
        conv_inner,
        conv_states,
        skip_gain[None],
        norm_gain[None],
        proj_output,
    )


def solution(mesh):
    n, shards = mesh.shape["tp"], mesh.shape["seq"]
    plain = plain_solution(mesh)

    def run(*arrays):
        tokens, proj_inner, proj_states, proj_step = arrays[0], arrays[2], arrays[4], arrays[5]
        rows = tokens.shape[0] // (mesh.shape["dp"] * shards * n)
        heads, state_w = proj_step.shape[1] // n, proj_states.shape[1] // n
        fits = (
            n == 4
            and shards == 4
            and mesh.shape["dp"] == 2
            and rows % 32 == 0
            and (rows * n) % BLOCK == 0
            and state_w == 2 * STATE
            and heads % GROUPS == 0
            and (proj_inner.shape[1] // n) % 256 == 0
        )
        if not fits:
            return plain(*arrays)
        line = P(("dp", "seq", "tp"), None)
        columns = P(None, "tp")
        placed = (
            (line, P()) + (columns,) * 4 + (P("tp"), P("tp"), columns, columns)
            + (P("tp"), P("tp"), P("tp", None))
        )
        return jax.shard_map(
            partial(body, n, shards), mesh=mesh, in_specs=placed, out_specs=line, check_vma=False
        )(*arrays)

    return run
```

```python
from functools import partial

import jax
import jax.numpy as jnp
from jax import lax
from jax.sharding import PartitionSpec as P
from jax.experimental import pallas as pl
from jax.experimental.pallas import tpu as pltpu

HEAD_DIM = 64
STATE = 128
GROUP_HEADS = 16
BLOCK = 128
GROUPS = 4


epsilon = 1e-05
highest = lax.Precision.HIGHEST


def from_behind(value, axis, steps):
    count = lax.axis_size(axis)
    initial, last = (max(0, -steps), min(count, count - steps))
    return lax.ppermute(value, axis, [(source, source + steps) for source in range(initial, last)])


def causal_conv(values, kernel_taps, before):
    length = values.shape[0]
    padded = jnp.concatenate((before, values), axis=0)
    running_sum = jnp.zeros(values.shape, jnp.float32)
    for offset in range(kernel_taps.shape[0]):
        running_sum = running_sum + kernel_taps[offset] * padded[offset : offset + length]
    return running_sum


def block_step(carry_state, inputs, copies):
    values, step_size, log_decay, in_states, out_states = inputs
    block_len = values.shape[0]
    running = jnp.cumsum(log_decay, axis=0)
    scores = jnp.einsum("tgn,sgn->gts", out_states, in_states, precision=highest)
    scores = jnp.tile(scores, (copies, 1, 1))
    places = jnp.arange(block_len)
    lower_mask = (places[:, None] >= places[None, :])[None]
    spread = running.T[:, :, None] - running.T[:, None, :]
    decay_table = jnp.where(lower_mask, jnp.exp(jnp.where(lower_mask, spread, 0.0)), 0.0)
    weights = scores * decay_table * step_size.T[:, None, :]
    within = jnp.einsum("hts,shp->thp", weights, values, precision=highest)
    out_heads = jnp.tile(out_states, (1, copies, 1))
    in_heads = jnp.tile(in_states, (1, copies, 1))
    carried = (
        jnp.einsum("thn,hpn->thp", out_heads, carry_state, precision=highest)
        * jnp.exp(running)[:, :, None]
    )
    tail_decay = jnp.exp(running[-1][None, :] - running) * step_size
    scaled = values * tail_decay[:, :, None]
    new_state = jnp.exp(running[-1])[:, None, None] * carry_state + jnp.einsum(
        "shp,shn->hpn", scaled, in_heads, precision=highest
    )
    return (new_state, within + carried)


def scan_blocks(
    values, step_size, log_decay, in_states, out_states, carry_state, block_len, copies
):
    row_count, head_count, head_dim = values.shape
    block_count = row_count // block_len

    def split_blocks(source):
        return source.reshape((block_count, block_len) + source.shape[1:])

    final_state, outputs = lax.scan(
        partial(block_step, copies=copies),
        carry_state,
        (
            split_blocks(values),
            split_blocks(step_size),
            split_blocks(log_decay),
            split_blocks(in_states),
            split_blocks(out_states),
        ),
    )
    return (final_state, outputs.reshape(row_count, head_count, head_dim))


def plain_body(
    tokens,
    pre_gain,
    proj_inner,
    proj_gate,
    proj_states,
    proj_step,
    step_bias,
    log_rate,
    conv_inner,
    conv_states,
    skip_gain,
    norm_gain,
    proj_output,
):
    tokens_wide = tokens.astype(jnp.float32)
    normed = (
        tokens_wide
        * lax.rsqrt(jnp.mean(tokens_wide * tokens_wide, axis=1, keepdims=True) + epsilon)
        * pre_gain
    ).astype(jnp.bfloat16)
    inner_width = proj_inner.shape[1]
    state_width = proj_states.shape[1]
    heads_local = proj_step.shape[1]
    copies = heads_local // GROUPS
    row_piece = lax.all_gather(normed, "tp", axis=0, tiled=True)
    projected = jnp.concatenate(
        (
            jnp.dot(row_piece, proj_inner, preferred_element_type=jnp.float32),
            jnp.dot(row_piece, proj_gate, preferred_element_type=jnp.float32),
            jnp.dot(row_piece, proj_states, preferred_element_type=jnp.float32),
            jnp.dot(row_piece, proj_step, preferred_element_type=jnp.float32),
        ),
        axis=1,
    )
    row_count = projected.shape[0]
    inner_proj = projected[:, :inner_width].astype(jnp.bfloat16)
    gate_proj = projected[:, inner_width : 2 * inner_width].astype(jnp.bfloat16)
    state_proj = projected[:, 2 * inner_width : 2 * inner_width + state_width].astype(jnp.bfloat16)
    step_size = jax.nn.softplus(projected[:, 2 * inner_width + state_width :] + step_bias)
    log_decay = -jnp.exp(log_rate) * step_size
    margin = conv_inner.shape[0] - 1
    before_inner, before_states = from_behind(
        (inner_proj[row_count - margin :], state_proj[row_count - margin :]), "seq", 1
    )
    mixed_inner = jax.nn.silu(
        causal_conv(inner_proj.astype(jnp.float32), conv_inner, before_inner.astype(jnp.float32))
    ).astype(jnp.bfloat16)
    mixed_local = jax.nn.silu(
        causal_conv(state_proj.astype(jnp.float32), conv_states, before_states.astype(jnp.float32))
    ).astype(jnp.bfloat16)
    mixed_all = lax.all_gather(mixed_local, "tp", axis=1, tiled=True)
    values = mixed_inner.astype(jnp.float32).reshape(row_count, heads_local, HEAD_DIM)
    paired = mixed_all.astype(jnp.float32).reshape(row_count, GROUPS, 2, STATE)
    in_states = paired[:, :, 0]
    out_states = paired[:, :, 1]
    zero_state = jnp.zeros((heads_local, HEAD_DIM, STATE), jnp.float32)
    final_state, scanned = scan_blocks(
        values, step_size, log_decay, in_states, out_states, zero_state, BLOCK, copies
    )
    decay_sum = jnp.sum(log_decay, axis=0)
    decay_sums, summaries = (
        lax.all_gather(decay_sum[None].astype(jnp.bfloat16), "seq", axis=0, tiled=True).astype(
            jnp.float32
        ),
        lax.all_gather(final_state[None].astype(jnp.bfloat16), "seq", axis=0, tiled=True).astype(
            jnp.float32
        ),
    )
    position = lax.axis_index("seq")
    device_ids = jnp.arange(decay_sums.shape[0])
    earlier_mask = (device_ids < position)[:, None]
    before_me = jnp.sum(jnp.where(earlier_mask, decay_sums, 0.0), axis=0)
    reach_end = jnp.cumsum(decay_sums, axis=0)
    weights = jnp.where(
        earlier_mask, jnp.exp(jnp.where(earlier_mask, before_me[None] - reach_end, 0.0)), 0.0
    )
    incoming = jnp.einsum("jh,jhpn->hpn", weights, summaries, precision=highest)
    running = jnp.cumsum(log_decay, axis=0)
    out_heads = jnp.tile(out_states, (1, copies, 1))
    carried = (
        jnp.einsum("thn,hpn->thp", out_heads, incoming, precision=highest)
        * jnp.exp(running)[:, :, None]
    )
    ssd_out = scanned + carried + skip_gain[None, :, None] * values
    gated_out = ssd_out * jax.nn.silu(gate_proj.astype(jnp.float32)).reshape(
        row_count, heads_local, HEAD_DIM
    )
    head_squares = jnp.sum(gated_out * gated_out, axis=2)
    every_square = lax.all_gather(head_squares, "tp", axis=1, tiled=True)
    group_totals = jnp.sum(
        every_square.reshape(row_count, every_square.shape[1] // GROUPS, GROUPS), axis=1
    )
    mean_square = (group_totals / (GROUP_HEADS * HEAD_DIM))[:, None, :, None]
    grouped = gated_out.reshape(row_count, copies, GROUPS, HEAD_DIM)
    normal_out = grouped * lax.rsqrt(mean_square + epsilon)
    mixed_out = (normal_out.reshape(row_count, inner_width) * norm_gain).astype(jnp.bfloat16)
    summed = lax.psum_scatter(
        jnp.dot(mixed_out, proj_output, preferred_element_type=jnp.float32).astype(jnp.bfloat16),
        "tp",
        scatter_dimension=0,
        tiled=True,
    ).astype(jnp.float32)
    return (tokens_wide + summed).astype(jnp.bfloat16)


def plain_solution(mesh):
    placed = (
        P(("dp", "seq", "tp"), None),
        P(),
        P(None, "tp"),
        P(None, "tp"),
        P(None, "tp"),
        P(None, "tp"),
        P("tp"),
        P("tp"),
        P(None, "tp"),
        P(None, "tp"),
        P("tp"),
        P("tp"),
        P("tp", None),
    )
    return jax.shard_map(
        plain_body, mesh=mesh, in_specs=placed, out_specs=P(("dp", "seq", "tp"), None), check_vma=False
    )


LANES = 128
PAD = 16
MESH = pl.DeviceIdType.MESH
NT = (((1,), (1,)), ((), ()))


def remote(source, target, send, receive, device):
    return pltpu.make_async_remote_copy(
        src_ref=source,
        dst_ref=target,
        send_sem=send,
        recv_sem=receive,
        device_id=device,
        device_id_type=MESH,
    )


def bdot(a, b):
    return jnp.dot(a, b, preferred_element_type=jnp.float32)


def fused_kernel(
    n,
    shards,
    shared,
    tokens_far,
    pre_gain_far,
    w_inner,
    w_gate,
    w_states,
    w_step,
    step_bias_far,
    log_rate_far,
    taps_inner_far,
    taps_states,
    skip_gain_far,
    norm_gain_far,
    w_out,
    out,
    tokens,
    pre_gain,
    step_bias,
    log_rate,
    taps_inner,
    skip_gain,
    norm_gain,
    wide,
    step_w,
    wout,
    rows_all,
    proj,
    states,
    taps_all,
    raw_step,
    run_ref,
    x_mix,
    s_mix,
    acc,
    ends,
    state_out,
    state_in,
    squares,
    mixed,
    stage,
    from_right,
    from_left,
    own_sum,
    spare,
    pre,
    far,
    done,
    load_sem,
    o_sem,
    line,
    ahead,
    g_send,
    g_recv,
    t_send,
    t_recv,
    s_send,
    s_recv,
    c_send,
    c_recv,
    ti_send,
    ti_recv,
    ts_send,
    ts_recv,
    e_send,
    e_recv,
    q_send,
    q_recv,
    r_send,
    rl_recv,
    rr_recv,
    wz_send,
    wz_recv,
    wy_send,
    wy_recv,
    wx_send,
    wx_recv,
    wd_send,
    wd_recv,
    m_send,
    m_recv,
):
    z = lax.axis_index("tp")
    s = lax.axis_index("seq")
    part_id = lax.axis_index("dp")
    rows, width = tokens.shape
    total = n * rows
    inner = w_inner.shape[1]
    state_w = w_states.shape[1]
    heads = w_step.shape[0]
    half = rows // 2
    at_end = jnp.logical_or(z == 0, z == n - 1)
    beside = jnp.logical_or(z == 1, z == n - 2)
    across = lax.rem(s + shards // 2, shards)
    sibling = s + 1 - 2 * lax.rem(s, 2)

    early = [
        pltpu.make_async_copy(source, target, load_sem.at[5 + i])
        for i, (source, target) in enumerate(
            (
                (tokens_far, tokens),
                (pre_gain_far, pre_gain),
                (taps_states, taps_all.at[z]),
                (step_bias_far, step_bias),
                (log_rate_far, log_rate),
                (taps_inner_far, taps_inner),
                (skip_gain_far, skip_gain),
                (norm_gain_far, norm_gain),
            )
        )
    ]
    for load in early:
        load.start()
    barrier = pltpu.get_barrier_semaphore()
    neighbours = (
        (z > 0, {"tp": z - 1}),
        (z < n - 1, {"tp": z + 1}),
        (s > 0, {"seq": s - 1}),
        (s < shards - 1, {"seq": s + 1}),
        (z >= 0, {"seq": across}),
        (z >= 0, {"dp": 1 - part_id}),
    )
    met = jnp.int32(0)
    for there, device in neighbours:
        met = met + there.astype(jnp.int32)

        @pl.when(there)
        def _():
            pl.semaphore_signal(barrier, inc=1, device_id=device, device_id_type=MESH)

    loads = [
        pltpu.make_async_copy(w_states, wide.at[:, pl.ds(2 * inner, state_w)], load_sem.at[0]),
        pltpu.make_async_copy(w_step, step_w, load_sem.at[1]),
        pltpu.make_async_copy(w_inner, wide.at[:, pl.ds(0, inner)], load_sem.at[2]),
        pltpu.make_async_copy(w_gate, wide.at[:, pl.ds(inner, inner)], load_sem.at[3]),
        pltpu.make_async_copy(w_out, wout, load_sem.at[4]),
    ]
    for load in early[:2]:
        load.wait()
    for load in loads[:4]:
        load.start()

    def own_rows(i, _):
        piece = pl.ds(pl.multiple_of(i * 16, 16), 16)
        value = tokens[piece, :].astype(jnp.float32)
        scale = lax.rsqrt(jnp.mean(value * value, axis=1, keepdims=True) + epsilon)
        place = pl.ds(pl.multiple_of(z * rows + i * 16, 16), 16)
        rows_all[place, :] = (value * scale * pre_gain[...]).astype(jnp.bfloat16)
        return 0

    lax.fori_loop(half // 16, rows // 16, own_rows, 0)

    @pl.when(s == 0)
    def _():
        proj[0:PAD, 0:inner] = jnp.zeros((PAD, inner), jnp.bfloat16)
        states[0:PAD, :] = jnp.zeros((PAD, states.shape[1]), jnp.bfloat16)
        state_in[...] = jnp.zeros(state_in.shape, jnp.bfloat16)

    pl.semaphore_wait(barrier, met)

    def row_copy(source, part, side):
        block = rows_all.at[pl.ds(pl.multiple_of(source * rows + part * half, 16), half), :]
        step = 1 if side == 0 else -1
        return remote(
            block, block, g_send.at[side, source, part], g_recv.at[source, part], {"tp": z + step}
        )

    def send_on(source, part):
        @pl.when(jnp.logical_and(source <= z, z < n - 1))
        def _():
            row_copy(source, part, 0).start()

        @pl.when(jnp.logical_and(source >= z, z > 0))
        def _():
            row_copy(source, part, 1).start()

    slice_rows = inner // (2 * shards)
    chunk_rows = slice_rows // 2
    shared_w = spare.shape[1]

    def slice_of(d, q, c):
        first = (d * shards + q) * slice_rows + c * chunk_rows
        return pl.ds(pl.multiple_of(first, chunk_rows), chunk_rows)

    def down_copy(c):
        block = slice_of(part_id, s, c)
        return remote(
            w_out.at[block, pl.ds(0, shared_w)],
            spare.at[block, :],
            wz_send.at[c],
            wz_recv.at[c],
            {"tp": jnp.where(z == 0, 1, n - 2)},
        )

    def y_copy(c):
        block = spare.at[slice_of(part_id, s, c), :]
        return remote(block, block, wy_send.at[c], wy_recv.at[c], {"dp": 1 - part_id})

    def y_taken(c):
        block = spare.at[slice_of(1 - part_id, s, c), :]
        return remote(block, block, wy_send.at[c], wy_recv.at[c], {"dp": 1 - part_id})

    def x_copy(k, c, to):
        d = part_id if k == 0 else 1 - part_id
        block = spare.at[slice_of(d, s if to else across, c), :]
        return remote(block, block, wx_send.at[k, c], wx_recv.at[k, c], {"seq": across})

    def core_copy(j, to):
        d = part_id if j % 2 == 0 else 1 - part_id
        q = s if j < 2 else across
        q = q if to else q + 1 - 2 * lax.rem(q, 2)
        first = (d * shards + q) * slice_rows
        block = spare.at[pl.ds(pl.multiple_of(first, slice_rows), slice_rows), :]
        return remote(block, block, wd_send.at[j], wd_recv.at[j], {"seq": sibling})

    def send_down(c):
        @pl.when(at_end)
        def _():
            down_copy(c).start()

    send_on(z, 1)
    send_down(0)
    lax.fori_loop(0, half // 16, own_rows, 0)
    send_on(z, 0)
    send_down(1)

    def greet_line(side, condition):
        @pl.when(condition)
        def _():
            pl.semaphore_signal(
                line.at[side],
                inc=1,
                device_id={"tp": z + 1 if side == 0 else z - 1},
                device_id_type=MESH,
            )

    greet_line(0, z == 0)
    greet_line(1, z == n - 1)
    for side in range(2):
        edge = 0 if side == 0 else n - 1

        @pl.when(z != edge)
        def _():
            pl.semaphore_wait(line.at[side], 1)

        greet_line(side, jnp.logical_and(z != edge, z != n - 1 - edge))

    @pl.when(s > 0)
    def _():
        pl.semaphore_signal(ahead, inc=1, device_id={"seq": s - 1}, device_id_type=MESH)


    def tap_copy(source, other):
        return remote(
            taps_all.at[source], taps_all.at[source], t_send.at[other], t_recv.at[source], {"tp": other}
        )

    def in_copy(source, chunk, other):
        block = states.at[
            pl.ds(pl.multiple_of(PAD + chunk * rows, 16), rows),
            pl.ds(pl.multiple_of(source * state_w, LANES), STATE),
        ]
        return remote(
            block, block, s_send.at[chunk, other], s_recv.at[source, chunk], {"tp": other}
        )

    def is_edge(i):
        return jnp.logical_or(i == 0, i == n - 1)

    def out_copy(source, other):
        block = states.at[
            pl.ds(PAD, total), pl.ds(pl.multiple_of(source * state_w + STATE, LANES), STATE)
        ]
        return remote(block, block, c_send.at[other], c_recv.at[source], {"tp": other})

    def square_copy(source, other):
        return remote(
            squares.at[source], squares.at[source], q_send.at[other], q_recv.at[source], {"tp": other}
        )

    def each_other(action):
        def one(i, _):
            @pl.when(i != z)
            def _():
                action(i)

            return 0

        lax.fori_loop(0, n, one, 0)

    for load in early[2:]:
        load.wait()
    each_other(lambda i: tap_copy(z, i).start())

    def inner_tail():
        return remote(
            proj.at[pl.ds(total, PAD), pl.ds(0, inner)],
            proj.at[pl.ds(0, PAD), pl.ds(0, inner)],
            ti_send,
            ti_recv,
            {"seq": s + 1, "tp": z},
        )

    def state_tail(source, other):
        columns = pl.ds(pl.multiple_of(source * state_w, LANES), state_w)
        return remote(
            states.at[pl.ds(total, PAD), columns],
            states.at[pl.ds(0, PAD), columns],
            ts_send.at[other],
            ts_recv.at[source],
            {"seq": s + 1, "tp": other},
        )

    for load in loads[:4]:
        load.wait()
    loads[4].start()

    gate_tile = inner // 256

    def project(start, size):
        piece = pl.ds(pl.multiple_of(start, size), size)
        place = pl.ds(pl.multiple_of(PAD + start, 16), size)
        own = pl.ds(pl.multiple_of(z * state_w, LANES), state_w)
        tail = jnp.logical_and(start + size == total, s < shards - 1)
        states[place, own] = bdot(
            rows_all[piece, :], wide[:, 2 * inner : 2 * inner + state_w]
        ).astype(jnp.bfloat16)

        @pl.when(tail)
        def _():
            pl.semaphore_wait(ahead, 1)
            for other in range(n):
                state_tail(z, other).start()

        if size == rows:
            send_in(start // rows)
        else:

            @pl.when(lax.rem(start, rows) == 0)
            def _():
                send_in(start // rows)
                each_other(lambda i: out_copy(z, i).start())

        raw_step[piece, :] = lax.dot_general(
            rows_all[piece, :], step_w[...], NT, preferred_element_type=jnp.float32
        )

        def tile(i, _):
            columns = pl.ds(pl.multiple_of(i * 256, 256), 256)
            proj[place, columns] = bdot(rows_all[piece, :], wide[:, columns]).astype(jnp.bfloat16)
            return 0

        lax.fori_loop(0, gate_tile, tile, 0)

        @pl.when(tail)
        def _():
            inner_tail().start()

    def gate_rows(start, size):
        piece = pl.ds(pl.multiple_of(start, rows), size)
        place = pl.ds(pl.multiple_of(PAD + start, 16), size)

        def tile(i, _):
            columns = pl.ds(pl.multiple_of(inner + i * 256, 256), 256)
            proj[place, columns] = bdot(rows_all[piece, :], wide[:, columns]).astype(jnp.bfloat16)
            return 0

        lax.fori_loop(0, gate_tile, tile, 0)

    def send_in(chunk):
        each_other(lambda i: in_copy(z, chunk, i).start())

    def arrive(distance, _):
        for part in (1, 0):
            for side in range(2):
                source = z - distance if side == 0 else z + distance
                inside = jnp.logical_and(source >= 0, source < n)

                @pl.when(jnp.logical_and(inside, distance > 0))
                def _():
                    row_copy(source, part, side).wait_recv()
                    send_on(source, part)

        @pl.when(jnp.logical_and(beside, distance == 1))
        def _():
            down_copy(0).wait_recv()
            y_copy(0).start()
            x_copy(0, 0, True).start()

        @pl.when(jnp.logical_and(beside, distance == 2))
        def _():
            y_taken(0).wait_recv()
            x_copy(1, 0, True).start()
            down_copy(1).wait_recv()
            y_copy(1).start()
            x_copy(0, 1, True).start()

        def one(side, _):
            source = z - distance + 2 * distance * side
            inside = jnp.logical_and(source >= 0, source < n)

            @pl.when(jnp.logical_and(inside, jnp.logical_or(distance > 0, side == 0)))
            def _():
                project(source * rows, rows)

            return 0

        lax.fori_loop(0, 2, one, 0)
        return 0

    lax.fori_loop(0, n - 1, arrive, 0)

    @pl.when(beside)
    def _():
        y_taken(1).wait_recv()
        x_copy(1, 1, True).start()
        for j in range(2):
            core_copy(j, True).start()

    @pl.when(jnp.logical_not(at_end))
    def _():
        each_other(lambda i: out_copy(z, i).start())
        gate_rows(0, total)

    @pl.when(at_end)
    def _():
        gate_rows(jnp.where(z == 0, 0, rows), total - rows)

        def last_half(i, _):
            part = 1 - i
            for side in range(2):

                @pl.when(z == (n - 1 if side == 0 else 0))
                def _():
                    row_copy(n - 1 - z, part, side).wait_recv()

            project((n - 1 - z) * rows + part * half, half)
            return 0

        lax.fori_loop(0, 2, last_half, 0)

    step = raw_step[...] + step_bias[...]
    step = jnp.maximum(step, 0.0) + jnp.log1p(jnp.exp(-jnp.abs(step)))
    decay = -jnp.exp(log_rate[...]) * step
    place_t = lax.broadcasted_iota(jnp.int32, (total, total), 0)
    place_s = lax.broadcasted_iota(jnp.int32, (total, total), 1)
    tri = (place_t >= place_s).astype(jnp.float32)
    run = jnp.dot(tri, decay, precision=highest, preferred_element_type=jnp.float32)
    run_ref[...] = jnp.zeros(run_ref.shape, jnp.float32)
    run_ref[:, 0:heads] = run
    run_t = run_ref[...].T
    last = run[total - 1 : total, :]
    reach = jnp.exp(last - run) * step
    grown = jnp.exp(run)
    whole = jnp.exp(last)
    lane = lax.broadcasted_iota(jnp.int32, (1, LANES), 1)
    low = lane < HEAD_DIM

    def conv(buffer, columns, taps):
        value = buffer[:, columns].astype(jnp.float32)
        kernel_len = taps.shape[0]
        out_value = jnp.zeros((total, value.shape[1]), jnp.float32)
        for k in range(kernel_len):
            first = PAD - (kernel_len - 1) + k
            out_value = out_value + taps[k : k + 1, :] * value[first : first + total, :]
        return jax.nn.silu(out_value).astype(jnp.bfloat16)

    @pl.when(s > 0)
    def _():
        inner_tail().wait_recv()

    def conv_tile(i, _):
        columns = pl.ds(pl.multiple_of(i * 256, 256), 256)
        x_mix[:, columns] = conv(proj, columns, taps_inner[:, columns])
        return 0

    lax.fori_loop(0, inner // 256, conv_tile, 0)

    def take_states(part, i):
        columns = pl.ds(pl.multiple_of(i * state_w + part * STATE, LANES), STATE)
        taps = taps_all[i][:, part * STATE : (part + 1) * STATE]
        s_mix[:, columns] = conv(states, columns, taps)

    def take_in(i, _):
        @pl.when(i != z)
        def _():
            tap_copy(i, z).wait_recv()
            for chunk in range(n):
                in_copy(i, chunk, z).wait_recv()

        @pl.when(s > 0)
        def _():
            state_tail(i, z).wait_recv()

        take_states(0, i)
        return 0

    def take_out(i, _):
        @pl.when(i != z)
        def _():
            out_copy(i, z).wait_recv()

        take_states(1, i)
        return 0

    lax.fori_loop(0, n, take_in, 0)

    def group_in(g):
        return s_mix[:, g * 2 * STATE : g * 2 * STATE + STATE]

    def group_out(g):
        return s_mix[:, g * 2 * STATE + STATE : (g + 1) * 2 * STATE]

    def pair_of(value, h):
        return jnp.where(low, value[:, h : h + 1], value[:, h + 1 : h + 2])

    pairs = heads // 2
    per_quad = GROUPS // 2
    quads = pairs // per_quad
    quad_w = GROUPS * HEAD_DIM

    def end_copy(c):
        columns = pl.ds(c * quad_w, quad_w)
        return remote(
            state_out.at[:, columns],
            state_in.at[:, columns],
            e_send.at[c],
            e_recv.at[c],
            {"seq": s + 1, "tp": z},
        )

    turned = [group_in(g).T for g in range(GROUPS)]
    for q in range(pairs):
        columns = slice(q * LANES, (q + 1) * LANES)
        h = 2 * q
        scaled = (x_mix[:, columns].astype(jnp.float32) * pair_of(reach, h)).astype(jnp.bfloat16)
        ends[:, columns] = jnp.where(
            low, bdot(turned[h % GROUPS], scaled), bdot(turned[(h + 1) % GROUPS], scaled)
        )
        if q % per_quad == per_quad - 1:
            c = q // per_quad

            @pl.when(jnp.logical_and(s == 0, shards > 1))
            def _():
                columns = slice(c * quad_w, (c + 1) * quad_w)
                state_out[:, columns] = ends[:, columns].astype(jnp.bfloat16)
                end_copy(c).start()

    def hand_on(c, here):
        @pl.when(here)
        def _():
            end_copy(c).wait_recv()

            @pl.when(s < shards - 1)
            def _():
                for q in range(c * per_quad, (c + 1) * per_quad):
                    columns = slice(q * LANES, (q + 1) * LANES)
                    state_out[:, columns] = (
                        ends[:, columns]
                        + pair_of(whole, 2 * q) * state_in[:, columns].astype(jnp.float32)
                    ).astype(jnp.bfloat16)
                end_copy(c).start()

    for c in range(quads):
        hand_on(c, s == 1)

    @pl.when(at_end)
    def _():
        gate_rows((n - 1 - z) * rows, rows)


    @pl.when(beside)
    def _():
        for k in range(2):
            for c in range(2):
                x_copy(k, c, False).wait_recv()
            core_copy(2 + k, True).start()

    lax.fori_loop(0, n, take_out, 0)

    scores = [
        lax.dot_general(group_out(g), group_in(g), NT, preferred_element_type=jnp.float32)
        for g in range(GROUPS)
    ]
    for q in range(pairs):
        columns = slice(q * LANES, (q + 1) * LANES)
        h = 2 * q
        value = x_mix[:, columns].astype(jnp.float32)
        stepped = (value * pair_of(step, h)).astype(jnp.bfloat16)
        direct = value * pair_of(skip_gain[...], h)
        for low_t in range(0, total, BLOCK):
            high_t = low_t + BLOCK
            causal = place_t[low_t:high_t, :high_t] >= place_s[low_t:high_t, :high_t]
            both = []
            for k in (h, h + 1):
                spread = run[low_t:high_t, k : k + 1] - run_t[k : k + 1, :high_t]
                table = jnp.where(causal, jnp.exp(jnp.where(causal, spread, 0.0)), 0.0)
                weights = (scores[k % GROUPS][low_t:high_t, :high_t] * table).astype(jnp.bfloat16)
                both.append(bdot(weights, stepped[:high_t, :]))
            acc[low_t:high_t, columns] = jnp.where(low, both[0], both[1]) + direct[low_t:high_t, :]
        if q % per_quad == per_quad - 1:
            hand_on(q // per_quad, s == 2)
    sums = [jnp.zeros((total, LANES), jnp.float32) for _ in range(per_quad)]
    for q in range(pairs):
        columns = slice(q * LANES, (q + 1) * LANES)
        h = 2 * q
        if q % per_quad == 0:
            hand_on(q // per_quad, s > 2)
        came = state_in[:, columns]
        carried = jnp.where(
            low, bdot(group_out(h % GROUPS), came), bdot(group_out((h + 1) % GROUPS), came)
        )
        gate = proj[PAD:, inner + q * LANES : inner + (q + 1) * LANES].astype(jnp.float32)
        gated = (acc[:, columns] + carried * pair_of(grown, h)) * jax.nn.silu(gate)
        acc[:, columns] = gated
        sums[q % per_quad] = sums[q % per_quad] + gated * gated
    pick = lax.broadcasted_iota(jnp.int32, (8, LANES), 0)
    where_lane = lax.broadcasted_iota(jnp.int32, (8, LANES), 1)
    local = jnp.zeros((8, total), jnp.float32)
    for k in range(per_quad):
        chosen = (where_lane // HEAD_DIM + 2 * k == pick).astype(jnp.float32)
        local = local + lax.dot_general(
            chosen, sums[k], NT, precision=highest, preferred_element_type=jnp.float32
        )
    squares[z] = local
    each_other(lambda i: square_copy(z, i).start())

    def mix_copy(target):
        place = pl.ds(pl.multiple_of(target * rows, rows), rows)
        return remote(
            pre.at[place, :],
            far.at[place, :],
            m_send.at[target],
            m_recv.at[target],
            {"tp": jnp.where(z == 0, 1, n - 2)},
        )

    @pl.when(at_end)
    def _():
        for q in range(pairs):
            columns = slice(q * LANES, (q + 1) * LANES)
            pre[:, columns] = (acc[:, columns] * norm_gain[:, columns]).astype(jnp.bfloat16)
        for i in range(n - 1):
            mix_copy(jnp.where(z == 0, n - 1 - i, i)).start()

    loads[4].wait()
    each_other(lambda i: square_copy(i, z).wait_recv())
    sum_all = squares[0]
    for i in range(1, n):
        sum_all = sum_all + squares[i]
    inverse = lax.rsqrt(sum_all / (n * heads // GROUPS * HEAD_DIM) + epsilon)
    inverse = jnp.concatenate([inverse] * (LANES // 8), axis=0).T
    run_ref[...] = inverse
    def mix(target):
        place = pl.ds(pl.multiple_of(target * rows, rows), rows)
        scale = run_ref[place, :]
        for q in range(pairs):
            columns = slice(q * LANES, (q + 1) * LANES)
            mixed[place, columns] = (
                acc[place, columns] * pair_of(scale, (2 * q) % GROUPS) * norm_gain[:, columns]
            ).astype(jnp.bfloat16)

    pieces = r_send.shape[1]
    piece_w = width // pieces

    def partial_of(target, p):
        return bdot(mixed[pl.ds(pl.multiple_of(target * rows, rows), rows), :], wout[:, p])

    def columns_of(p):
        return pl.ds(pl.multiple_of(p * piece_w, LANES), piece_w)

    def sum_copy(target, p, side):
        landing, receive, way = (from_right, rl_recv, -1) if side == 0 else (from_left, rr_recv, 1)
        return remote(
            stage.at[target, p],
            landing.at[target, p],
            r_send.at[target, p],
            receive.at[target, p],
            {"tp": z + way},
        )

    def far_partial(target, p):
        place = pl.ds(pl.multiple_of(target * rows, rows), rows)
        return bdot(far[place, :], spare[:, p])

    def take_far(target):
        place = pl.ds(pl.multiple_of(target * rows, rows), rows)
        mix_copy(target).wait_recv()
        scale = run_ref[place, :]
        for q in range(pairs):
            columns = slice(q * LANES, (q + 1) * LANES)
            far[place, columns] = (
                far[place, columns].astype(jnp.float32) * pair_of(scale, (2 * q) % GROUPS)
            ).astype(jnp.bfloat16)

    @pl.when(beside)
    def _():
        for j in range(4):
            core_copy(j, False).wait_recv()

    items = (n - 1) * pieces
    lag = 3

    def one_sum(t, _):
        for side in range(2):
            i = t - lag * (n - 1 - z) if side == 0 else t - lag * z
            k, p = jnp.maximum(i, 0) // pieces, lax.rem(jnp.maximum(i, 0), pieces)
            target = k if side == 0 else n - 1 - k
            landing = from_right if side == 0 else from_left
            active = target < z if side == 0 else target > z
            more = z < n - 1 if side == 0 else z > 0
            active = jnp.logical_and(active, jnp.logical_and(i >= 0, i < items))

            has_far = z == n - 2 if side == 0 else z == 1
            is_end = z == n - 1 if side == 0 else z == 0
            use_far = jnp.logical_and(has_far, p < shared)
            active = jnp.logical_and(active, jnp.logical_or(p >= shared, jnp.logical_not(is_end)))

            @pl.when(jnp.logical_and(active, p == jnp.where(is_end, shared, 0)))
            def _():
                mix(target)

                @pl.when(has_far)
                def _():
                    take_far(target)

            @pl.when(active)
            def _():
                value = partial_of(target, columns_of(p))

                @pl.when(use_far)
                def _():
                    stage[target, p] = (
                        value + far_partial(target, columns_of(p))
                    ).astype(jnp.bfloat16)

                @pl.when(jnp.logical_and(more, jnp.logical_not(use_far)))
                def _():
                    sum_copy(target, p, side).wait_recv()
                    stage[target, p] = (
                        value + landing[target, p].astype(jnp.float32)
                    ).astype(jnp.bfloat16)

                @pl.when(jnp.logical_not(more))
                def _():
                    stage[target, p] = value.astype(jnp.bfloat16)

                sum_copy(target, p, side).start()

        @pl.when(t == items)
        def _():
            mix(z)

            @pl.when(beside)
            def _():
                take_far(z)

        @pl.when(jnp.logical_and(t >= items, t < items + pieces))
        def _():
            columns = columns_of(t - items)
            own = tokens[:, columns].astype(jnp.float32) + partial_of(z, columns)
            own_sum[:, columns] = own

            @pl.when(jnp.logical_and(beside, t - items < shared))
            def _():
                own_sum[:, columns] = own + far_partial(z, columns)

        return 0

    lax.fori_loop(0, items + max(lag * (n - 1), pieces), one_sum, 0)

    def finish(p, _):
        columns = columns_of(p)
        lands = (
            jnp.logical_and(z < n - 1, jnp.logical_or(z != n - 2, p >= shared)),
            jnp.logical_and(z > 0, jnp.logical_or(z != 1, p >= shared)),
        )
        for side in range(2):

            @pl.when(lands[side])
            def _():
                sum_copy(z, p, side).wait_recv()

        none = jnp.zeros((rows, piece_w), jnp.float32)
        right = jnp.where(lands[0], from_right[z, p].astype(jnp.float32), none)
        left = jnp.where(lands[1], from_left[z, p].astype(jnp.float32), none)
        done[:, columns] = (own_sum[:, columns] + right + left).astype(jnp.bfloat16)
        out_store(p).start()
        return 0

    def out_store(p):
        columns = columns_of(p)
        return pltpu.make_async_copy(done.at[:, columns], out.at[:, columns], o_sem.at[p])

    lax.fori_loop(0, pieces, finish, 0)

    def sent_rows(source, _):
        for part in range(2):

            @pl.when(jnp.logical_and(source <= z, z < n - 1))
            def _():
                row_copy(source, part, 0).wait_send()

            @pl.when(jnp.logical_and(source >= z, z > 0))
            def _():
                row_copy(source, part, 1).wait_send()

        return 0

    lax.fori_loop(0, n, sent_rows, 0)

    def sent_small(i):
        tap_copy(z, i).wait_send()
        square_copy(z, i).wait_send()
        out_copy(z, i).wait_send()
        for chunk in range(n):
            in_copy(z, chunk, i).wait_send()

        def sent_sum(p, _):
            sum_copy(i, p, 0).wait_send()
            return 0

        lax.fori_loop(jnp.where(at_end, shared, 0), pieces, sent_sum, 0)

    each_other(sent_small)

    def stored(p, _):
        out_store(p).wait()
        return 0

    lax.fori_loop(0, pieces, stored, 0)

    @pl.when(s < shards - 1)
    def _():
        inner_tail().wait_send()
        for other in range(n):
            state_tail(z, other).wait_send()
        for c in range(quads):
            end_copy(c).wait_send()

    @pl.when(at_end)
    def _():
        for c in range(2):
            down_copy(c).wait_send()
        for i in range(n - 1):
            mix_copy(jnp.where(z == 0, n - 1 - i, i)).wait_send()

    @pl.when(beside)
    def _():
        for c in range(2):
            y_copy(c).wait_send()
            for k in range(2):
                x_copy(k, c, True).wait_send()
        for j in range(4):
            core_copy(j, True).wait_send()


def body(
    n,
    shards,
    tokens,
    pre_gain,
    proj_inner,
    proj_gate,
    proj_states,
    proj_step,
    step_bias,
    log_rate,
    conv_inner,
    conv_states,
    skip_gain,
    norm_gain,
    proj_output,
):
    rows, width = tokens.shape
    inner, state_w, heads = proj_inner.shape[1], proj_states.shape[1], proj_step.shape[1]
    total = n * rows
    all_states = n * state_w
    quads = heads // GROUPS
    pieces, shared = 8, 4
    bf16, f32 = jnp.bfloat16, jnp.float32
    far = pl.BlockSpec(memory_space=pl.ANY)
    dma = pltpu.SemaphoreType.DMA
    return pl.pallas_call(
        partial(fused_kernel, n, shards, shared),
        out_shape=jax.ShapeDtypeStruct((rows, width), bf16),
        in_specs=[far] * 13,
        out_specs=far,
        scratch_shapes=[
            pltpu.VMEM((rows, width), bf16),
            pltpu.VMEM((1, width), f32),
            pltpu.VMEM((1, heads), f32),
            pltpu.VMEM((1, heads), f32),
            pltpu.VMEM(conv_inner.shape, f32),
            pltpu.VMEM((1, heads), f32),
            pltpu.VMEM((1, inner), f32),
            pltpu.VMEM((width, 2 * inner + state_w), bf16),
            pltpu.VMEM((heads, width), bf16),
            pltpu.VMEM((inner, width), bf16),
            pltpu.VMEM((total, width), bf16),
            pltpu.VMEM((PAD + total, 2 * inner), bf16),
            pltpu.VMEM((PAD + total, all_states), bf16),
            pltpu.VMEM((n,) + conv_states.shape, f32),
            pltpu.VMEM((total, heads), f32),
            pltpu.VMEM((total, LANES), f32),
            pltpu.VMEM((total, inner), bf16),
            pltpu.VMEM((total, all_states), bf16),
            pltpu.VMEM((total, inner), f32),
            pltpu.VMEM((STATE, inner), f32),
            pltpu.VMEM((STATE, inner), bf16),
            pltpu.VMEM((STATE, inner), bf16),
            pltpu.VMEM((n, 8, total), f32),
            pltpu.VMEM((total, inner), bf16),
            pltpu.VMEM((n, pieces, rows, width // pieces), bf16),
            pltpu.VMEM((n, pieces, rows, width // pieces), bf16),
            pltpu.VMEM((n, pieces, rows, width // pieces), bf16),
            pltpu.VMEM((rows, width), f32),
            pltpu.VMEM((inner, width // pieces * shared), bf16),
            pltpu.VMEM((total, inner), bf16),
            pltpu.VMEM((total, inner), bf16),
            pltpu.VMEM((rows, width), bf16),
            dma((13,)),
            dma((pieces,)),
            pltpu.SemaphoreType.REGULAR((2,)),
            pltpu.SemaphoreType.REGULAR,
            dma((2, n, 2)),
            dma((n, 2)),
            dma((n,)),
            dma((n,)),
            dma((n, n)),
            dma((n, n)),
            dma((n,)),
            dma((n,)),
            dma,
            dma,
            dma((n,)),
            dma((n,)),
            dma((quads,)),
            dma((quads,)),
            dma((n,)),
            dma((n,)),
            dma((n, pieces)),
            dma((n, pieces)),
            dma((n, pieces)),
            dma((2,)),
            dma((2,)),
            dma((2,)),
            dma((2,)),
            dma((2, 2)),
            dma((2, 2)),
            dma((4,)),
            dma((4,)),
            dma((n,)),
            dma((n,)),
        ],
        compiler_params=pltpu.CompilerParams(
            collective_id=0, has_side_effects=True, vmem_limit_bytes=62 * 1024 * 1024
        ),
    )(
        tokens,
        pre_gain[None],
        proj_inner,
        proj_gate,
        proj_states,
        proj_step.T,
        step_bias[None],
        log_rate[None],
        conv_inner,
        conv_states,
        skip_gain[None],
        norm_gain[None],
        proj_output,
    )


def solution(mesh):
    n, shards = mesh.shape["tp"], mesh.shape["seq"]
    plain = plain_solution(mesh)

    def run(*arrays):
        tokens, proj_inner, proj_states, proj_step = arrays[0], arrays[2], arrays[4], arrays[5]
        rows = tokens.shape[0] // (mesh.shape["dp"] * shards * n)
        heads, state_w = proj_step.shape[1] // n, proj_states.shape[1] // n
        fits = (
            n == 4
            and shards == 4
            and mesh.shape["dp"] == 2
            and rows % 32 == 0
            and (rows * n) % BLOCK == 0
            and state_w == 2 * STATE
            and heads % GROUPS == 0
            and (proj_inner.shape[1] // n) % 256 == 0
        )
        if not fits:
            return plain(*arrays)
        line = P(("dp", "seq", "tp"), None)
        columns = P(None, "tp")
        placed = (
            (line, P()) + (columns,) * 4 + (P("tp"), P("tp"), columns, columns)
            + (P("tp"), P("tp"), P("tp", None))
        )
        return jax.shard_map(
            partial(body, n, shards), mesh=mesh, in_specs=placed, out_specs=line, check_vma=False
        )(*arrays)

    return run
```

```python
from functools import partial

import jax
import jax.numpy as jnp
from jax import lax
from jax.sharding import PartitionSpec as P
from jax.experimental import pallas as pl
from jax.experimental.pallas import tpu as pltpu

HEAD_DIM = 64
STATE = 128
GROUP_HEADS = 16
BLOCK = 128
GROUPS = 4


epsilon = 1e-05
highest = lax.Precision.HIGHEST


def from_behind(value, axis, steps):
    count = lax.axis_size(axis)
    initial, last = (max(0, -steps), min(count, count - steps))
    return lax.ppermute(value, axis, [(source, source + steps) for source in range(initial, last)])


def causal_conv(values, kernel_taps, before):
    length = values.shape[0]
    padded = jnp.concatenate((before, values), axis=0)
    running_sum = jnp.zeros(values.shape, jnp.float32)
    for offset in range(kernel_taps.shape[0]):
        running_sum = running_sum + kernel_taps[offset] * padded[offset : offset + length]
    return running_sum


def block_step(carry_state, inputs, copies):
    values, step_size, log_decay, in_states, out_states = inputs
    block_len = values.shape[0]
    running = jnp.cumsum(log_decay, axis=0)
    scores = jnp.einsum("tgn,sgn->gts", out_states, in_states, precision=highest)
    scores = jnp.tile(scores, (copies, 1, 1))
    places = jnp.arange(block_len)
    lower_mask = (places[:, None] >= places[None, :])[None]
    spread = running.T[:, :, None] - running.T[:, None, :]
    decay_table = jnp.where(lower_mask, jnp.exp(jnp.where(lower_mask, spread, 0.0)), 0.0)
    weights = scores * decay_table * step_size.T[:, None, :]
    within = jnp.einsum("hts,shp->thp", weights, values, precision=highest)
    out_heads = jnp.tile(out_states, (1, copies, 1))
    in_heads = jnp.tile(in_states, (1, copies, 1))
    carried = (
        jnp.einsum("thn,hpn->thp", out_heads, carry_state, precision=highest)
        * jnp.exp(running)[:, :, None]
    )
    tail_decay = jnp.exp(running[-1][None, :] - running) * step_size
    scaled = values * tail_decay[:, :, None]
    new_state = jnp.exp(running[-1])[:, None, None] * carry_state + jnp.einsum(
        "shp,shn->hpn", scaled, in_heads, precision=highest
    )
    return (new_state, within + carried)


def scan_blocks(
    values, step_size, log_decay, in_states, out_states, carry_state, block_len, copies
):
    row_count, head_count, head_dim = values.shape
    block_count = row_count // block_len

    def split_blocks(source):
        return source.reshape((block_count, block_len) + source.shape[1:])

    final_state, outputs = lax.scan(
        partial(block_step, copies=copies),
        carry_state,
        (
            split_blocks(values),
            split_blocks(step_size),
            split_blocks(log_decay),
            split_blocks(in_states),
            split_blocks(out_states),
        ),
    )
    return (final_state, outputs.reshape(row_count, head_count, head_dim))


def plain_body(
    tokens,
    pre_gain,
    proj_inner,
    proj_gate,
    proj_states,
    proj_step,
    step_bias,
    log_rate,
    conv_inner,
    conv_states,
    skip_gain,
    norm_gain,
    proj_output,
):
    tokens_wide = tokens.astype(jnp.float32)
    normed = (
        tokens_wide
        * lax.rsqrt(jnp.mean(tokens_wide * tokens_wide, axis=1, keepdims=True) + epsilon)
        * pre_gain
    ).astype(jnp.bfloat16)
    inner_width = proj_inner.shape[1]
    state_width = proj_states.shape[1]
    heads_local = proj_step.shape[1]
    copies = heads_local // GROUPS
    row_piece = lax.all_gather(normed, "tp", axis=0, tiled=True)
    projected = jnp.concatenate(
        (
            jnp.dot(row_piece, proj_inner, preferred_element_type=jnp.float32),
            jnp.dot(row_piece, proj_gate, preferred_element_type=jnp.float32),
            jnp.dot(row_piece, proj_states, preferred_element_type=jnp.float32),
            jnp.dot(row_piece, proj_step, preferred_element_type=jnp.float32),
        ),
        axis=1,
    )
    row_count = projected.shape[0]
    inner_proj = projected[:, :inner_width].astype(jnp.bfloat16)
    gate_proj = projected[:, inner_width : 2 * inner_width].astype(jnp.bfloat16)
    state_proj = projected[:, 2 * inner_width : 2 * inner_width + state_width].astype(jnp.bfloat16)
    step_size = jax.nn.softplus(projected[:, 2 * inner_width + state_width :] + step_bias)
    log_decay = -jnp.exp(log_rate) * step_size
    margin = conv_inner.shape[0] - 1
    before_inner, before_states = from_behind(
        (inner_proj[row_count - margin :], state_proj[row_count - margin :]), "seq", 1
    )
    mixed_inner = jax.nn.silu(
        causal_conv(inner_proj.astype(jnp.float32), conv_inner, before_inner.astype(jnp.float32))
    ).astype(jnp.bfloat16)
    mixed_local = jax.nn.silu(
        causal_conv(state_proj.astype(jnp.float32), conv_states, before_states.astype(jnp.float32))
    ).astype(jnp.bfloat16)
    mixed_all = lax.all_gather(mixed_local, "tp", axis=1, tiled=True)
    values = mixed_inner.astype(jnp.float32).reshape(row_count, heads_local, HEAD_DIM)
    paired = mixed_all.astype(jnp.float32).reshape(row_count, GROUPS, 2, STATE)
    in_states = paired[:, :, 0]
    out_states = paired[:, :, 1]
    zero_state = jnp.zeros((heads_local, HEAD_DIM, STATE), jnp.float32)
    final_state, scanned = scan_blocks(
        values, step_size, log_decay, in_states, out_states, zero_state, BLOCK, copies
    )
    decay_sum = jnp.sum(log_decay, axis=0)
    decay_sums, summaries = (
        lax.all_gather(decay_sum[None].astype(jnp.bfloat16), "seq", axis=0, tiled=True).astype(
            jnp.float32
        ),
        lax.all_gather(final_state[None].astype(jnp.bfloat16), "seq", axis=0, tiled=True).astype(
            jnp.float32
        ),
    )
    position = lax.axis_index("seq")
    device_ids = jnp.arange(decay_sums.shape[0])
    earlier_mask = (device_ids < position)[:, None]
    before_me = jnp.sum(jnp.where(earlier_mask, decay_sums, 0.0), axis=0)
    reach_end = jnp.cumsum(decay_sums, axis=0)
    weights = jnp.where(
        earlier_mask, jnp.exp(jnp.where(earlier_mask, before_me[None] - reach_end, 0.0)), 0.0
    )
    incoming = jnp.einsum("jh,jhpn->hpn", weights, summaries, precision=highest)
    running = jnp.cumsum(log_decay, axis=0)
    out_heads = jnp.tile(out_states, (1, copies, 1))
    carried = (
        jnp.einsum("thn,hpn->thp", out_heads, incoming, precision=highest)
        * jnp.exp(running)[:, :, None]
    )
    ssd_out = scanned + carried + skip_gain[None, :, None] * values
    gated_out = ssd_out * jax.nn.silu(gate_proj.astype(jnp.float32)).reshape(
        row_count, heads_local, HEAD_DIM
    )
    head_squares = jnp.sum(gated_out * gated_out, axis=2)
    every_square = lax.all_gather(head_squares, "tp", axis=1, tiled=True)
    group_totals = jnp.sum(
        every_square.reshape(row_count, every_square.shape[1] // GROUPS, GROUPS), axis=1
    )
    mean_square = (group_totals / (GROUP_HEADS * HEAD_DIM))[:, None, :, None]
    grouped = gated_out.reshape(row_count, copies, GROUPS, HEAD_DIM)
    normal_out = grouped * lax.rsqrt(mean_square + epsilon)
    mixed_out = (normal_out.reshape(row_count, inner_width) * norm_gain).astype(jnp.bfloat16)
    summed = lax.psum_scatter(
        jnp.dot(mixed_out, proj_output, preferred_element_type=jnp.float32).astype(jnp.bfloat16),
        "tp",
        scatter_dimension=0,
        tiled=True,
    ).astype(jnp.float32)
    return (tokens_wide + summed).astype(jnp.bfloat16)


def plain_solution(mesh):
    placed = (
        P(("dp", "seq", "tp"), None),
        P(),
        P(None, "tp"),
        P(None, "tp"),
        P(None, "tp"),
        P(None, "tp"),
        P("tp"),
        P("tp"),
        P(None, "tp"),
        P(None, "tp"),
        P("tp"),
        P("tp"),
        P("tp", None),
    )
    return jax.shard_map(
        plain_body, mesh=mesh, in_specs=placed, out_specs=P(("dp", "seq", "tp"), None), check_vma=False
    )


LANES = 128
PAD = 16
MESH = pl.DeviceIdType.MESH
NT = (((1,), (1,)), ((), ()))


def remote(source, target, send, receive, device):
    return pltpu.make_async_remote_copy(
        src_ref=source,
        dst_ref=target,
        send_sem=send,
        recv_sem=receive,
        device_id=device,
        device_id_type=MESH,
    )


def bdot(a, b):
    return jnp.dot(a, b, preferred_element_type=jnp.float32)


def fused_kernel(
    n,
    shards,
    shared,
    tokens_far,
    pre_gain_far,
    w_inner,
    w_gate,
    w_states,
    w_step,
    step_bias_far,
    log_rate_far,
    taps_inner_far,
    taps_states,
    skip_gain_far,
    norm_gain_far,
    w_out,
    out,
    tokens,
    pre_gain,
    step_bias,
    log_rate,
    taps_inner,
    skip_gain,
    norm_gain,
    wide,
    step_w,
    wout,
    rows_all,
    proj,
    states,
    taps_all,
    raw_step,
    run_ref,
    x_mix,
    s_mix,
    acc,
    ends,
    state_out,
    state_in,
    squares,
    mixed,
    stage,
    from_right,
    from_left,
    own_sum,
    spare,
    pre,
    far,
    done,
    load_sem,
    o_sem,
    line,
    ahead,
    g_send,
    g_recv,
    t_send,
    t_recv,
    s_send,
    s_recv,
    c_send,
    c_recv,
    ti_send,
    ti_recv,
    ts_send,
    ts_recv,
    e_send,
    e_recv,
    q_send,
    q_recv,
    r_send,
    rl_recv,
    rr_recv,
    wz_send,
    wz_recv,
    wy_send,
    wy_recv,
    wx_send,
    wx_recv,
    wd_send,
    wd_recv,
    m_send,
    m_recv,
):
    z = lax.axis_index("tp")
    s = lax.axis_index("seq")
    part_id = lax.axis_index("dp")
    rows, width = tokens.shape
    total = n * rows
    inner = w_inner.shape[1]
    state_w = w_states.shape[1]
    heads = w_step.shape[0]
    half = rows // 2
    at_end = jnp.logical_or(z == 0, z == n - 1)
    beside = jnp.logical_or(z == 1, z == n - 2)
    across = lax.rem(s + shards // 2, shards)
    sibling = s + 1 - 2 * lax.rem(s, 2)

    early = [
        pltpu.make_async_copy(source, target, load_sem.at[5 + i])
        for i, (source, target) in enumerate(
            (
                (tokens_far, tokens),
                (pre_gain_far, pre_gain),
                (taps_states, taps_all.at[z]),
                (step_bias_far, step_bias),
                (log_rate_far, log_rate),
                (taps_inner_far, taps_inner),
                (skip_gain_far, skip_gain),
                (norm_gain_far, norm_gain),
            )
        )
    ]
    for load in early:
        load.start()
    barrier = pltpu.get_barrier_semaphore()
    neighbours = (
        (z > 0, {"tp": z - 1}),
        (z < n - 1, {"tp": z + 1}),
        (s > 0, {"seq": s - 1}),
        (s < shards - 1, {"seq": s + 1}),
        (z >= 0, {"seq": across}),
        (z >= 0, {"dp": 1 - part_id}),
    )
    met = jnp.int32(0)
    for there, device in neighbours:
        met = met + there.astype(jnp.int32)

        @pl.when(there)
        def _():
            pl.semaphore_signal(barrier, inc=1, device_id=device, device_id_type=MESH)

    loads = [
        pltpu.make_async_copy(w_states, wide.at[:, pl.ds(2 * inner, state_w)], load_sem.at[0]),
        pltpu.make_async_copy(w_step, step_w, load_sem.at[1]),
        pltpu.make_async_copy(w_inner, wide.at[:, pl.ds(0, inner)], load_sem.at[2]),
        pltpu.make_async_copy(w_gate, wide.at[:, pl.ds(inner, inner)], load_sem.at[3]),
        pltpu.make_async_copy(w_out, wout, load_sem.at[4]),
    ]
    for load in early[:2]:
        load.wait()
    for load in loads[:4]:
        load.start()

    def own_rows(i, _):
        piece = pl.ds(pl.multiple_of(i * 16, 16), 16)
        value = tokens[piece, :].astype(jnp.float32)
        scale = lax.rsqrt(jnp.mean(value * value, axis=1, keepdims=True) + epsilon)
        place = pl.ds(pl.multiple_of(z * rows + i * 16, 16), 16)
        rows_all[place, :] = (value * scale * pre_gain[...]).astype(jnp.bfloat16)
        return 0

    lax.fori_loop(half // 16, rows // 16, own_rows, 0)

    @pl.when(s == 0)
    def _():
        proj[0:PAD, 0:inner] = jnp.zeros((PAD, inner), jnp.bfloat16)
        states[0:PAD, :] = jnp.zeros((PAD, states.shape[1]), jnp.bfloat16)
        state_in[...] = jnp.zeros(state_in.shape, jnp.bfloat16)

    pl.semaphore_wait(barrier, met)

    def row_copy(source, part, side):
        block = rows_all.at[pl.ds(pl.multiple_of(source * rows + part * half, 16), half), :]
        step = 1 if side == 0 else -1
        return remote(
            block, block, g_send.at[side, source, part], g_recv.at[source, part], {"tp": z + step}
        )

    def send_on(source, part):
        @pl.when(jnp.logical_and(source <= z, z < n - 1))
        def _():
            row_copy(source, part, 0).start()

        @pl.when(jnp.logical_and(source >= z, z > 0))
        def _():
            row_copy(source, part, 1).start()

    slice_rows = inner // (2 * shards)
    chunk_rows = slice_rows // 2
    shared_w = spare.shape[1]

    def slice_of(d, q, c):
        first = (d * shards + q) * slice_rows + c * chunk_rows
        return pl.ds(pl.multiple_of(first, chunk_rows), chunk_rows)

    def down_copy(c):
        block = slice_of(part_id, s, c)
        return remote(
            w_out.at[block, pl.ds(0, shared_w)],
            spare.at[block, :],
            wz_send.at[c],
            wz_recv.at[c],
            {"tp": jnp.where(z == 0, 1, n - 2)},
        )

    def y_copy(c):
        block = spare.at[slice_of(part_id, s, c), :]
        return remote(block, block, wy_send.at[c], wy_recv.at[c], {"dp": 1 - part_id})

    def y_taken(c):
        block = spare.at[slice_of(1 - part_id, s, c), :]
        return remote(block, block, wy_send.at[c], wy_recv.at[c], {"dp": 1 - part_id})

    def x_copy(k, c, to):
        d = part_id if k == 0 else 1 - part_id
        block = spare.at[slice_of(d, s if to else across, c), :]
        return remote(block, block, wx_send.at[k, c], wx_recv.at[k, c], {"seq": across})

    def core_copy(j, to):
        d = part_id if j % 2 == 0 else 1 - part_id
        q = s if j < 2 else across
        q = q if to else q + 1 - 2 * lax.rem(q, 2)
        first = (d * shards + q) * slice_rows
        block = spare.at[pl.ds(pl.multiple_of(first, slice_rows), slice_rows), :]
        return remote(block, block, wd_send.at[j], wd_recv.at[j], {"seq": sibling})

    def send_down(c):
        @pl.when(at_end)
        def _():
            down_copy(c).start()

    send_on(z, 1)
    send_down(0)
    lax.fori_loop(0, half // 16, own_rows, 0)
    send_on(z, 0)
    send_down(1)

    def greet_line(side, condition):
        @pl.when(condition)
        def _():
            pl.semaphore_signal(
                line.at[side],
                inc=1,
                device_id={"tp": z + 1 if side == 0 else z - 1},
                device_id_type=MESH,
            )

    greet_line(0, z == 0)
    greet_line(1, z == n - 1)
    for side in range(2):
        edge = 0 if side == 0 else n - 1

        @pl.when(z != edge)
        def _():
            pl.semaphore_wait(line.at[side], 1)

        greet_line(side, jnp.logical_and(z != edge, z != n - 1 - edge))

    @pl.when(s > 0)
    def _():
        pl.semaphore_signal(ahead, inc=1, device_id={"seq": s - 1}, device_id_type=MESH)


    def tap_copy(source, other):
        return remote(
            taps_all.at[source], taps_all.at[source], t_send.at[other], t_recv.at[source], {"tp": other}
        )

    def in_copy(source, chunk, other):
        block = states.at[
            pl.ds(pl.multiple_of(PAD + chunk * rows, 16), rows),
            pl.ds(pl.multiple_of(source * state_w, LANES), STATE),
        ]
        return remote(
            block, block, s_send.at[chunk, other], s_recv.at[source, chunk], {"tp": other}
        )

    def is_edge(i):
        return jnp.logical_or(i == 0, i == n - 1)

    def out_copy(source, other):
        block = states.at[
            pl.ds(PAD, total), pl.ds(pl.multiple_of(source * state_w + STATE, LANES), STATE)
        ]
        return remote(block, block, c_send.at[other], c_recv.at[source], {"tp": other})

    def square_copy(source, other):
        return remote(
            squares.at[source], squares.at[source], q_send.at[other], q_recv.at[source], {"tp": other}
        )

    def each_other(action):
        def one(i, _):
            @pl.when(i != z)
            def _():
                action(i)

            return 0

        lax.fori_loop(0, n, one, 0)

    for load in early[2:]:
        load.wait()
    each_other(lambda i: tap_copy(z, i).start())

    def inner_tail():
        return remote(
            proj.at[pl.ds(total, PAD), pl.ds(0, inner)],
            proj.at[pl.ds(0, PAD), pl.ds(0, inner)],
            ti_send,
            ti_recv,
            {"seq": s + 1, "tp": z},
        )

    def state_tail(source, other):
        columns = pl.ds(pl.multiple_of(source * state_w, LANES), state_w)
        return remote(
            states.at[pl.ds(total, PAD), columns],
            states.at[pl.ds(0, PAD), columns],
            ts_send.at[other],
            ts_recv.at[source],
            {"seq": s + 1, "tp": other},
        )

    for load in loads[:4]:
        load.wait()
    loads[4].start()

    gate_tile = inner // 256

    def project(start, size):
        piece = pl.ds(pl.multiple_of(start, size), size)
        place = pl.ds(pl.multiple_of(PAD + start, 16), size)
        own = pl.ds(pl.multiple_of(z * state_w, LANES), state_w)
        tail = jnp.logical_and(start + size == total, s < shards - 1)
        states[place, own] = bdot(
            rows_all[piece, :], wide[:, 2 * inner : 2 * inner + state_w]
        ).astype(jnp.bfloat16)

        @pl.when(tail)
        def _():
            pl.semaphore_wait(ahead, 1)
            for other in range(n):
                state_tail(z, other).start()

        if size == rows:
            send_in(start // rows)
        else:

            @pl.when(lax.rem(start, rows) == 0)
            def _():
                send_in(start // rows)
                each_other(lambda i: out_copy(z, i).start())

        raw_step[piece, :] = lax.dot_general(
            rows_all[piece, :], step_w[...], NT, preferred_element_type=jnp.float32
        )

        def tile(i, _):
            columns = pl.ds(pl.multiple_of(i * 256, 256), 256)
            proj[place, columns] = bdot(rows_all[piece, :], wide[:, columns]).astype(jnp.bfloat16)
            return 0

        lax.fori_loop(0, gate_tile, tile, 0)

        @pl.when(tail)
        def _():
            inner_tail().start()

    def gate_rows(start, size):
        piece = pl.ds(pl.multiple_of(start, rows), size)
        place = pl.ds(pl.multiple_of(PAD + start, 16), size)

        def tile(i, _):
            columns = pl.ds(pl.multiple_of(inner + i * 256, 256), 256)
            proj[place, columns] = bdot(rows_all[piece, :], wide[:, columns]).astype(jnp.bfloat16)
            return 0

        lax.fori_loop(0, gate_tile, tile, 0)

    def send_in(chunk):
        each_other(lambda i: in_copy(z, chunk, i).start())

    def arrive(distance, _):
        for part in (1, 0):
            for side in range(2):
                source = z - distance if side == 0 else z + distance
                inside = jnp.logical_and(source >= 0, source < n)

                @pl.when(jnp.logical_and(inside, distance > 0))
                def _():
                    row_copy(source, part, side).wait_recv()
                    send_on(source, part)

        @pl.when(jnp.logical_and(beside, distance == 1))
        def _():
            down_copy(0).wait_recv()
            y_copy(0).start()
            x_copy(0, 0, True).start()

        @pl.when(jnp.logical_and(beside, distance == 2))
        def _():
            y_taken(0).wait_recv()
            x_copy(1, 0, True).start()
            down_copy(1).wait_recv()
            y_copy(1).start()
            x_copy(0, 1, True).start()

        def one(side, _):
            source = z - distance + 2 * distance * side
            inside = jnp.logical_and(source >= 0, source < n)

            @pl.when(jnp.logical_and(inside, jnp.logical_or(distance > 0, side == 0)))
            def _():
                project(source * rows, rows)

            return 0

        lax.fori_loop(0, 2, one, 0)
        return 0

    lax.fori_loop(0, n - 1, arrive, 0)

    @pl.when(beside)
    def _():
        y_taken(1).wait_recv()
        x_copy(1, 1, True).start()
        for j in range(2):
            core_copy(j, True).start()

    @pl.when(jnp.logical_not(at_end))
    def _():
        each_other(lambda i: out_copy(z, i).start())
        gate_rows(0, total)

    @pl.when(at_end)
    def _():
        gate_rows(jnp.where(z == 0, 0, rows), total - rows)

        def last_half(i, _):
            part = 1 - i
            for side in range(2):

                @pl.when(z == (n - 1 if side == 0 else 0))
                def _():
                    row_copy(n - 1 - z, part, side).wait_recv()

            project((n - 1 - z) * rows + part * half, half)
            return 0

        lax.fori_loop(0, 2, last_half, 0)

    step = raw_step[...] + step_bias[...]
    step = jnp.maximum(step, 0.0) + jnp.log1p(jnp.exp(-jnp.abs(step)))
    decay = -jnp.exp(log_rate[...]) * step
    place_t = lax.broadcasted_iota(jnp.int32, (total, total), 0)
    place_s = lax.broadcasted_iota(jnp.int32, (total, total), 1)
    tri = (place_t >= place_s).astype(jnp.bfloat16)
    decay_high = decay.astype(jnp.bfloat16)
    rest = decay - decay_high.astype(jnp.float32)
    decay_mid = rest.astype(jnp.bfloat16)
    decay_low = (rest - decay_mid.astype(jnp.float32)).astype(jnp.bfloat16)
    run = bdot(tri, decay_high) + (bdot(tri, decay_mid) + bdot(tri, decay_low))
    run_ref[...] = jnp.zeros(run_ref.shape, jnp.float32)
    run_ref[:, 0:heads] = run
    run_t = run_ref[...].T
    last = run[total - 1 : total, :]
    reach = jnp.exp(last - run) * step
    grown = jnp.exp(run)
    whole = jnp.exp(last)
    lane = lax.broadcasted_iota(jnp.int32, (1, LANES), 1)
    low = lane < HEAD_DIM

    def conv(buffer, columns, taps):
        value = buffer[:, columns].astype(jnp.float32)
        kernel_len = taps.shape[0]
        out_value = jnp.zeros((total, value.shape[1]), jnp.float32)
        for k in range(kernel_len):
            first = PAD - (kernel_len - 1) + k
            out_value = out_value + taps[k : k + 1, :] * value[first : first + total, :]
        return jax.nn.silu(out_value).astype(jnp.bfloat16)

    @pl.when(s > 0)
    def _():
        inner_tail().wait_recv()

    def conv_tile(i, _):
        columns = pl.ds(pl.multiple_of(i * 256, 256), 256)
        x_mix[:, columns] = conv(proj, columns, taps_inner[:, columns])
        return 0

    lax.fori_loop(0, inner // 256, conv_tile, 0)

    def take_states(part, i):
        columns = pl.ds(pl.multiple_of(i * state_w + part * STATE, LANES), STATE)
        taps = taps_all[i][:, part * STATE : (part + 1) * STATE]
        s_mix[:, columns] = conv(states, columns, taps)

    def take_in(i, _):
        @pl.when(i != z)
        def _():
            tap_copy(i, z).wait_recv()
            for chunk in range(n):
                in_copy(i, chunk, z).wait_recv()

        @pl.when(s > 0)
        def _():
            state_tail(i, z).wait_recv()

        take_states(0, i)
        return 0

    def take_out(i, _):
        @pl.when(i != z)
        def _():
            out_copy(i, z).wait_recv()

        take_states(1, i)
        return 0

    lax.fori_loop(0, n, take_in, 0)

    def group_in(g):
        return s_mix[:, g * 2 * STATE : g * 2 * STATE + STATE]

    def group_out(g):
        return s_mix[:, g * 2 * STATE + STATE : (g + 1) * 2 * STATE]

    def pair_of(value, h):
        return jnp.where(low, value[:, h : h + 1], value[:, h + 1 : h + 2])

    pairs = heads // 2
    per_quad = GROUPS // 2
    quads = pairs // per_quad
    quad_w = GROUPS * HEAD_DIM

    def end_copy(c):
        columns = pl.ds(c * quad_w, quad_w)
        return remote(
            state_out.at[:, columns],
            state_in.at[:, columns],
            e_send.at[c],
            e_recv.at[c],
            {"seq": s + 1, "tp": z},
        )

    turned = [group_in(g).T for g in range(GROUPS)]
    for q in range(pairs):
        columns = slice(q * LANES, (q + 1) * LANES)
        h = 2 * q
        scaled = (x_mix[:, columns].astype(jnp.float32) * pair_of(reach, h)).astype(jnp.bfloat16)
        ends[:, columns] = jnp.where(
            low, bdot(turned[h % GROUPS], scaled), bdot(turned[(h + 1) % GROUPS], scaled)
        )
        if q % per_quad == per_quad - 1:
            c = q // per_quad

            @pl.when(jnp.logical_and(s == 0, shards > 1))
            def _():
                columns = slice(c * quad_w, (c + 1) * quad_w)
                state_out[:, columns] = ends[:, columns].astype(jnp.bfloat16)
                end_copy(c).start()

    def hand_on(c, here):
        @pl.when(here)
        def _():
            end_copy(c).wait_recv()

            @pl.when(s < shards - 1)
            def _():
                for q in range(c * per_quad, (c + 1) * per_quad):
                    columns = slice(q * LANES, (q + 1) * LANES)
                    state_out[:, columns] = (
                        ends[:, columns]
                        + pair_of(whole, 2 * q) * state_in[:, columns].astype(jnp.float32)
                    ).astype(jnp.bfloat16)
                end_copy(c).start()

    for c in range(quads):
        hand_on(c, s == 1)

    @pl.when(at_end)
    def _():
        gate_rows((n - 1 - z) * rows, rows)


    @pl.when(beside)
    def _():
        for k in range(2):
            for c in range(2):
                x_copy(k, c, False).wait_recv()
            core_copy(2 + k, True).start()

    for c in range(quads):
        hand_on(c, s == 2)
    lax.fori_loop(0, n, take_out, 0)

    scores = [
        lax.dot_general(group_out(g), group_in(g), NT, preferred_element_type=jnp.float32)
        for g in range(GROUPS)
    ]
    for q in range(pairs):
        columns = slice(q * LANES, (q + 1) * LANES)
        h = 2 * q
        value = x_mix[:, columns].astype(jnp.float32)
        stepped = (value * pair_of(step, h)).astype(jnp.bfloat16)
        direct = value * pair_of(skip_gain[...], h)
        for low_t in range(0, total, BLOCK):
            high_t = low_t + BLOCK
            causal = place_t[low_t:high_t, :high_t] >= place_s[low_t:high_t, :high_t]
            both = []
            for k in (h, h + 1):
                spread = run[low_t:high_t, k : k + 1] - run_t[k : k + 1, :high_t]
                table = jnp.where(causal, jnp.exp(jnp.where(causal, spread, 0.0)), 0.0)
                weights = (scores[k % GROUPS][low_t:high_t, :high_t] * table).astype(jnp.bfloat16)
                both.append(bdot(weights, stepped[:high_t, :]))
            acc[low_t:high_t, columns] = jnp.where(low, both[0], both[1]) + direct[low_t:high_t, :]
    sums = [jnp.zeros((total, LANES), jnp.float32) for _ in range(per_quad)]
    for q in range(pairs):
        columns = slice(q * LANES, (q + 1) * LANES)
        h = 2 * q
        if q % per_quad == 0:
            hand_on(q // per_quad, s > 2)
        came = state_in[:, columns]
        carried = jnp.where(
            low, bdot(group_out(h % GROUPS), came), bdot(group_out((h + 1) % GROUPS), came)
        )
        gate = proj[PAD:, inner + q * LANES : inner + (q + 1) * LANES].astype(jnp.float32)
        gated = (acc[:, columns] + carried * pair_of(grown, h)) * jax.nn.silu(gate)
        acc[:, columns] = gated
        sums[q % per_quad] = sums[q % per_quad] + gated * gated
    pick = lax.broadcasted_iota(jnp.int32, (8, LANES), 0)
    where_lane = lax.broadcasted_iota(jnp.int32, (8, LANES), 1)
    local = jnp.zeros((8, total), jnp.float32)
    for k in range(per_quad):
        chosen = (where_lane // HEAD_DIM + 2 * k == pick).astype(jnp.float32)
        local = local + lax.dot_general(
            chosen, sums[k], NT, precision=highest, preferred_element_type=jnp.float32
        )
    squares[z] = local
    each_other(lambda i: square_copy(z, i).start())

    def mix_copy(target):
        place = pl.ds(pl.multiple_of(target * rows, rows), rows)
        return remote(
            pre.at[place, :],
            far.at[place, :],
            m_send.at[target],
            m_recv.at[target],
            {"tp": jnp.where(z == 0, 1, n - 2)},
        )

    @pl.when(at_end)
    def _():
        for q in range(pairs):
            columns = slice(q * LANES, (q + 1) * LANES)
            pre[:, columns] = (acc[:, columns] * norm_gain[:, columns]).astype(jnp.bfloat16)
        for i in range(n - 1):
            mix_copy(jnp.where(z == 0, n - 1 - i, i)).start()

    loads[4].wait()
    each_other(lambda i: square_copy(i, z).wait_recv())
    sum_all = squares[0]
    for i in range(1, n):
        sum_all = sum_all + squares[i]
    inverse = lax.rsqrt(sum_all / (n * heads // GROUPS * HEAD_DIM) + epsilon)
    inverse = jnp.concatenate([inverse] * (LANES // 8), axis=0).T
    run_ref[...] = inverse
    def mix(target):
        place = pl.ds(pl.multiple_of(target * rows, rows), rows)
        scale = run_ref[place, :]
        for q in range(pairs):
            columns = slice(q * LANES, (q + 1) * LANES)
            mixed[place, columns] = (
                acc[place, columns] * pair_of(scale, (2 * q) % GROUPS) * norm_gain[:, columns]
            ).astype(jnp.bfloat16)

    pieces = r_send.shape[1]
    piece_w = width // pieces

    def partial_of(target, p):
        return bdot(mixed[pl.ds(pl.multiple_of(target * rows, rows), rows), :], wout[:, p])

    def columns_of(p):
        return pl.ds(pl.multiple_of(p * piece_w, LANES), piece_w)

    def sum_copy(target, p, side):
        landing, receive, way = (from_right, rl_recv, -1) if side == 0 else (from_left, rr_recv, 1)
        return remote(
            stage.at[target, p],
            landing.at[target, p],
            r_send.at[target, p],
            receive.at[target, p],
            {"tp": z + way},
        )

    def far_partial(target, p):
        place = pl.ds(pl.multiple_of(target * rows, rows), rows)
        return bdot(far[place, :], spare[:, p])

    def take_far(target):
        place = pl.ds(pl.multiple_of(target * rows, rows), rows)
        mix_copy(target).wait_recv()
        scale = run_ref[place, :]
        for q in range(pairs):
            columns = slice(q * LANES, (q + 1) * LANES)
            far[place, columns] = (
                far[place, columns].astype(jnp.float32) * pair_of(scale, (2 * q) % GROUPS)
            ).astype(jnp.bfloat16)

    @pl.when(beside)
    def _():
        for j in range(4):
            core_copy(j, False).wait_recv()

    items = (n - 1) * pieces
    lag = 3

    def one_sum(t, _):
        for side in range(2):
            i = t - lag * (n - 1 - z) if side == 0 else t - lag * z
            k, p = jnp.maximum(i, 0) // pieces, lax.rem(jnp.maximum(i, 0), pieces)
            target = k if side == 0 else n - 1 - k
            landing = from_right if side == 0 else from_left
            active = target < z if side == 0 else target > z
            more = z < n - 1 if side == 0 else z > 0
            active = jnp.logical_and(active, jnp.logical_and(i >= 0, i < items))

            has_far = z == n - 2 if side == 0 else z == 1
            is_end = z == n - 1 if side == 0 else z == 0
            use_far = jnp.logical_and(has_far, p < shared)
            active = jnp.logical_and(active, jnp.logical_or(p >= shared, jnp.logical_not(is_end)))

            @pl.when(jnp.logical_and(active, p == jnp.where(is_end, shared, 0)))
            def _():
                mix(target)

                @pl.when(has_far)
                def _():
                    take_far(target)

            @pl.when(active)
            def _():
                value = partial_of(target, columns_of(p))

                @pl.when(use_far)
                def _():
                    stage[target, p] = (
                        value + far_partial(target, columns_of(p))
                    ).astype(jnp.bfloat16)

                @pl.when(jnp.logical_and(more, jnp.logical_not(use_far)))
                def _():
                    sum_copy(target, p, side).wait_recv()
                    stage[target, p] = (
                        value + landing[target, p].astype(jnp.float32)
                    ).astype(jnp.bfloat16)

                @pl.when(jnp.logical_not(more))
                def _():
                    stage[target, p] = value.astype(jnp.bfloat16)

                sum_copy(target, p, side).start()

        @pl.when(t == items)
        def _():
            mix(z)

            @pl.when(beside)
            def _():
                take_far(z)

        @pl.when(jnp.logical_and(t >= items, t < items + pieces))
        def _():
            columns = columns_of(t - items)
            own = tokens[:, columns].astype(jnp.float32) + partial_of(z, columns)
            own_sum[:, columns] = own

            @pl.when(jnp.logical_and(beside, t - items < shared))
            def _():
                own_sum[:, columns] = own + far_partial(z, columns)

        return 0

    lax.fori_loop(0, items + max(lag * (n - 1), pieces), one_sum, 0)

    def finish(p, _):
        columns = columns_of(p)
        lands = (
            jnp.logical_and(z < n - 1, jnp.logical_or(z != n - 2, p >= shared)),
            jnp.logical_and(z > 0, jnp.logical_or(z != 1, p >= shared)),
        )
        for side in range(2):

            @pl.when(lands[side])
            def _():
                sum_copy(z, p, side).wait_recv()

        none = jnp.zeros((rows, piece_w), jnp.float32)
        right = jnp.where(lands[0], from_right[z, p].astype(jnp.float32), none)
        left = jnp.where(lands[1], from_left[z, p].astype(jnp.float32), none)
        done[:, columns] = (own_sum[:, columns] + right + left).astype(jnp.bfloat16)
        out_store(p).start()
        return 0

    def out_store(p):
        columns = columns_of(p)
        return pltpu.make_async_copy(done.at[:, columns], out.at[:, columns], o_sem.at[p])

    lax.fori_loop(0, pieces, finish, 0)

    def sent_rows(source, _):
        for part in range(2):

            @pl.when(jnp.logical_and(source <= z, z < n - 1))
            def _():
                row_copy(source, part, 0).wait_send()

            @pl.when(jnp.logical_and(source >= z, z > 0))
            def _():
                row_copy(source, part, 1).wait_send()

        return 0

    lax.fori_loop(0, n, sent_rows, 0)

    def sent_small(i):
        tap_copy(z, i).wait_send()
        square_copy(z, i).wait_send()
        out_copy(z, i).wait_send()
        for chunk in range(n):
            in_copy(z, chunk, i).wait_send()

        def sent_sum(p, _):
            sum_copy(i, p, 0).wait_send()
            return 0

        lax.fori_loop(jnp.where(at_end, shared, 0), pieces, sent_sum, 0)

    each_other(sent_small)

    def stored(p, _):
        out_store(p).wait()
        return 0

    lax.fori_loop(0, pieces, stored, 0)

    @pl.when(s < shards - 1)
    def _():
        inner_tail().wait_send()
        for other in range(n):
            state_tail(z, other).wait_send()
        for c in range(quads):
            end_copy(c).wait_send()

    @pl.when(at_end)
    def _():
        for c in range(2):
            down_copy(c).wait_send()
        for i in range(n - 1):
            mix_copy(jnp.where(z == 0, n - 1 - i, i)).wait_send()

    @pl.when(beside)
    def _():
        for c in range(2):
            y_copy(c).wait_send()
            for k in range(2):
                x_copy(k, c, True).wait_send()
        for j in range(4):
            core_copy(j, True).wait_send()


def body(
    n,
    shards,
    tokens,
    pre_gain,
    proj_inner,
    proj_gate,
    proj_states,
    proj_step,
    step_bias,
    log_rate,
    conv_inner,
    conv_states,
    skip_gain,
    norm_gain,
    proj_output,
):
    rows, width = tokens.shape
    inner, state_w, heads = proj_inner.shape[1], proj_states.shape[1], proj_step.shape[1]
    total = n * rows
    all_states = n * state_w
    quads = heads // GROUPS
    pieces, shared = 8, 4
    bf16, f32 = jnp.bfloat16, jnp.float32
    far = pl.BlockSpec(memory_space=pl.ANY)
    dma = pltpu.SemaphoreType.DMA
    return pl.pallas_call(
        partial(fused_kernel, n, shards, shared),
        out_shape=jax.ShapeDtypeStruct((rows, width), bf16),
        in_specs=[far] * 13,
        out_specs=far,
        scratch_shapes=[
            pltpu.VMEM((rows, width), bf16),
            pltpu.VMEM((1, width), f32),
            pltpu.VMEM((1, heads), f32),
            pltpu.VMEM((1, heads), f32),
            pltpu.VMEM(conv_inner.shape, f32),
            pltpu.VMEM((1, heads), f32),
            pltpu.VMEM((1, inner), f32),
            pltpu.VMEM((width, 2 * inner + state_w), bf16),
            pltpu.VMEM((heads, width), bf16),
            pltpu.VMEM((inner, width), bf16),
            pltpu.VMEM((total, width), bf16),
            pltpu.VMEM((PAD + total, 2 * inner), bf16),
            pltpu.VMEM((PAD + total, all_states), bf16),
            pltpu.VMEM((n,) + conv_states.shape, f32),
            pltpu.VMEM((total, heads), f32),
            pltpu.VMEM((total, LANES), f32),
            pltpu.VMEM((total, inner), bf16),
            pltpu.VMEM((total, all_states), bf16),
            pltpu.VMEM((total, inner), f32),
            pltpu.VMEM((STATE, inner), f32),
            pltpu.VMEM((STATE, inner), bf16),
            pltpu.VMEM((STATE, inner), bf16),
            pltpu.VMEM((n, 8, total), f32),
            pltpu.VMEM((total, inner), bf16),
            pltpu.VMEM((n, pieces, rows, width // pieces), bf16),
            pltpu.VMEM((n, pieces, rows, width // pieces), bf16),
            pltpu.VMEM((n, pieces, rows, width // pieces), bf16),
            pltpu.VMEM((rows, width), f32),
            pltpu.VMEM((inner, width // pieces * shared), bf16),
            pltpu.VMEM((total, inner), bf16),
            pltpu.VMEM((total, inner), bf16),
            pltpu.VMEM((rows, width), bf16),
            dma((13,)),
            dma((pieces,)),
            pltpu.SemaphoreType.REGULAR((2,)),
            pltpu.SemaphoreType.REGULAR,
            dma((2, n, 2)),
            dma((n, 2)),
            dma((n,)),
            dma((n,)),
            dma((n, n)),
            dma((n, n)),
            dma((n,)),
            dma((n,)),
            dma,
            dma,
            dma((n,)),
            dma((n,)),
            dma((quads,)),
            dma((quads,)),
            dma((n,)),
            dma((n,)),
            dma((n, pieces)),
            dma((n, pieces)),
            dma((n, pieces)),
            dma((2,)),
            dma((2,)),
            dma((2,)),
            dma((2,)),
            dma((2, 2)),
            dma((2, 2)),
            dma((4,)),
            dma((4,)),
            dma((n,)),
            dma((n,)),
        ],
        compiler_params=pltpu.CompilerParams(
            collective_id=0, has_side_effects=True, vmem_limit_bytes=62 * 1024 * 1024
        ),
    )(
        tokens,
        pre_gain[None],
        proj_inner,
        proj_gate,
        proj_states,
        proj_step.T,
        step_bias[None],
        log_rate[None],
        conv_inner,
        conv_states,
        skip_gain[None],
        norm_gain[None],
        proj_output,
    )


def solution(mesh):
    n, shards = mesh.shape["tp"], mesh.shape["seq"]
    plain = plain_solution(mesh)

    def run(*arrays):
        tokens, proj_inner, proj_states, proj_step = arrays[0], arrays[2], arrays[4], arrays[5]
        rows = tokens.shape[0] // (mesh.shape["dp"] * shards * n)
        heads, state_w = proj_step.shape[1] // n, proj_states.shape[1] // n
        fits = (
            n == 4
            and shards == 4
            and mesh.shape["dp"] == 2
            and rows % 32 == 0
            and (rows * n) % BLOCK == 0
            and state_w == 2 * STATE
            and heads % GROUPS == 0
            and (proj_inner.shape[1] // n) % 256 == 0
        )
        if not fits:
            return plain(*arrays)
        line = P(("dp", "seq", "tp"), None)
        columns = P(None, "tp")
        placed = (
            (line, P()) + (columns,) * 4 + (P("tp"), P("tp"), columns, columns)
            + (P("tp"), P("tp"), P("tp", None))
        )
        return jax.shard_map(
            partial(body, n, shards), mesh=mesh, in_specs=placed, out_specs=line, check_vma=False
        )(*arrays)

    return run
```

```python
from functools import partial

import jax
import jax.numpy as jnp
from jax import lax
from jax.sharding import PartitionSpec as P
from jax.experimental import pallas as pl
from jax.experimental.pallas import tpu as pltpu

HEAD_DIM = 64
STATE = 128
GROUP_HEADS = 16
BLOCK = 128
GROUPS = 4


epsilon = 1e-05
highest = lax.Precision.HIGHEST


def from_behind(value, axis, steps):
    count = lax.axis_size(axis)
    initial, last = (max(0, -steps), min(count, count - steps))
    return lax.ppermute(value, axis, [(source, source + steps) for source in range(initial, last)])


def causal_conv(values, kernel_taps, before):
    length = values.shape[0]
    padded = jnp.concatenate((before, values), axis=0)
    running_sum = jnp.zeros(values.shape, jnp.float32)
    for offset in range(kernel_taps.shape[0]):
        running_sum = running_sum + kernel_taps[offset] * padded[offset : offset + length]
    return running_sum


def block_step(carry_state, inputs, copies):
    values, step_size, log_decay, in_states, out_states = inputs
    block_len = values.shape[0]
    running = jnp.cumsum(log_decay, axis=0)
    scores = jnp.einsum("tgn,sgn->gts", out_states, in_states, precision=highest)
    scores = jnp.tile(scores, (copies, 1, 1))
    places = jnp.arange(block_len)
    lower_mask = (places[:, None] >= places[None, :])[None]
    spread = running.T[:, :, None] - running.T[:, None, :]
    decay_table = jnp.where(lower_mask, jnp.exp(jnp.where(lower_mask, spread, 0.0)), 0.0)
    weights = scores * decay_table * step_size.T[:, None, :]
    within = jnp.einsum("hts,shp->thp", weights, values, precision=highest)
    out_heads = jnp.tile(out_states, (1, copies, 1))
    in_heads = jnp.tile(in_states, (1, copies, 1))
    carried = (
        jnp.einsum("thn,hpn->thp", out_heads, carry_state, precision=highest)
        * jnp.exp(running)[:, :, None]
    )
    tail_decay = jnp.exp(running[-1][None, :] - running) * step_size
    scaled = values * tail_decay[:, :, None]
    new_state = jnp.exp(running[-1])[:, None, None] * carry_state + jnp.einsum(
        "shp,shn->hpn", scaled, in_heads, precision=highest
    )
    return (new_state, within + carried)


def scan_blocks(
    values, step_size, log_decay, in_states, out_states, carry_state, block_len, copies
):
    row_count, head_count, head_dim = values.shape
    block_count = row_count // block_len

    def split_blocks(source):
        return source.reshape((block_count, block_len) + source.shape[1:])

    final_state, outputs = lax.scan(
        partial(block_step, copies=copies),
        carry_state,
        (
            split_blocks(values),
            split_blocks(step_size),
            split_blocks(log_decay),
            split_blocks(in_states),
            split_blocks(out_states),
        ),
    )
    return (final_state, outputs.reshape(row_count, head_count, head_dim))


def plain_body(
    tokens,
    pre_gain,
    proj_inner,
    proj_gate,
    proj_states,
    proj_step,
    step_bias,
    log_rate,
    conv_inner,
    conv_states,
    skip_gain,
    norm_gain,
    proj_output,
):
    tokens_wide = tokens.astype(jnp.float32)
    normed = (
        tokens_wide
        * lax.rsqrt(jnp.mean(tokens_wide * tokens_wide, axis=1, keepdims=True) + epsilon)
        * pre_gain
    ).astype(jnp.bfloat16)
    inner_width = proj_inner.shape[1]
    state_width = proj_states.shape[1]
    heads_local = proj_step.shape[1]
    copies = heads_local // GROUPS
    row_piece = lax.all_gather(normed, "tp", axis=0, tiled=True)
    projected = jnp.concatenate(
        (
            jnp.dot(row_piece, proj_inner, preferred_element_type=jnp.float32),
            jnp.dot(row_piece, proj_gate, preferred_element_type=jnp.float32),
            jnp.dot(row_piece, proj_states, preferred_element_type=jnp.float32),
            jnp.dot(row_piece, proj_step, preferred_element_type=jnp.float32),
        ),
        axis=1,
    )
    row_count = projected.shape[0]
    inner_proj = projected[:, :inner_width].astype(jnp.bfloat16)
    gate_proj = projected[:, inner_width : 2 * inner_width].astype(jnp.bfloat16)
    state_proj = projected[:, 2 * inner_width : 2 * inner_width + state_width].astype(jnp.bfloat16)
    step_size = jax.nn.softplus(projected[:, 2 * inner_width + state_width :] + step_bias)
    log_decay = -jnp.exp(log_rate) * step_size
    margin = conv_inner.shape[0] - 1
    before_inner, before_states = from_behind(
        (inner_proj[row_count - margin :], state_proj[row_count - margin :]), "seq", 1
    )
    mixed_inner = jax.nn.silu(
        causal_conv(inner_proj.astype(jnp.float32), conv_inner, before_inner.astype(jnp.float32))
    ).astype(jnp.bfloat16)
    mixed_local = jax.nn.silu(
        causal_conv(state_proj.astype(jnp.float32), conv_states, before_states.astype(jnp.float32))
    ).astype(jnp.bfloat16)
    mixed_all = lax.all_gather(mixed_local, "tp", axis=1, tiled=True)
    values = mixed_inner.astype(jnp.float32).reshape(row_count, heads_local, HEAD_DIM)
    paired = mixed_all.astype(jnp.float32).reshape(row_count, GROUPS, 2, STATE)
    in_states = paired[:, :, 0]
    out_states = paired[:, :, 1]
    zero_state = jnp.zeros((heads_local, HEAD_DIM, STATE), jnp.float32)
    final_state, scanned = scan_blocks(
        values, step_size, log_decay, in_states, out_states, zero_state, BLOCK, copies
    )
    decay_sum = jnp.sum(log_decay, axis=0)
    decay_sums, summaries = (
        lax.all_gather(decay_sum[None].astype(jnp.bfloat16), "seq", axis=0, tiled=True).astype(
            jnp.float32
        ),
        lax.all_gather(final_state[None].astype(jnp.bfloat16), "seq", axis=0, tiled=True).astype(
            jnp.float32
        ),
    )
    position = lax.axis_index("seq")
    device_ids = jnp.arange(decay_sums.shape[0])
    earlier_mask = (device_ids < position)[:, None]
    before_me = jnp.sum(jnp.where(earlier_mask, decay_sums, 0.0), axis=0)
    reach_end = jnp.cumsum(decay_sums, axis=0)
    weights = jnp.where(
        earlier_mask, jnp.exp(jnp.where(earlier_mask, before_me[None] - reach_end, 0.0)), 0.0
    )
    incoming = jnp.einsum("jh,jhpn->hpn", weights, summaries, precision=highest)
    running = jnp.cumsum(log_decay, axis=0)
    out_heads = jnp.tile(out_states, (1, copies, 1))
    carried = (
        jnp.einsum("thn,hpn->thp", out_heads, incoming, precision=highest)
        * jnp.exp(running)[:, :, None]
    )
    ssd_out = scanned + carried + skip_gain[None, :, None] * values
    gated_out = ssd_out * jax.nn.silu(gate_proj.astype(jnp.float32)).reshape(
        row_count, heads_local, HEAD_DIM
    )
    head_squares = jnp.sum(gated_out * gated_out, axis=2)
    every_square = lax.all_gather(head_squares, "tp", axis=1, tiled=True)
    group_totals = jnp.sum(
        every_square.reshape(row_count, every_square.shape[1] // GROUPS, GROUPS), axis=1
    )
    mean_square = (group_totals / (GROUP_HEADS * HEAD_DIM))[:, None, :, None]
    grouped = gated_out.reshape(row_count, copies, GROUPS, HEAD_DIM)
    normal_out = grouped * lax.rsqrt(mean_square + epsilon)
    mixed_out = (normal_out.reshape(row_count, inner_width) * norm_gain).astype(jnp.bfloat16)
    summed = lax.psum_scatter(
        jnp.dot(mixed_out, proj_output, preferred_element_type=jnp.float32).astype(jnp.bfloat16),
        "tp",
        scatter_dimension=0,
        tiled=True,
    ).astype(jnp.float32)
    return (tokens_wide + summed).astype(jnp.bfloat16)


def plain_solution(mesh):
    placed = (
        P(("dp", "seq", "tp"), None),
        P(),
        P(None, "tp"),
        P(None, "tp"),
        P(None, "tp"),
        P(None, "tp"),
        P("tp"),
        P("tp"),
        P(None, "tp"),
        P(None, "tp"),
        P("tp"),
        P("tp"),
        P("tp", None),
    )
    return jax.shard_map(
        plain_body, mesh=mesh, in_specs=placed, out_specs=P(("dp", "seq", "tp"), None), check_vma=False
    )


LANES = 128
PAD = 16
MESH = pl.DeviceIdType.MESH
NT = (((1,), (1,)), ((), ()))


def remote(source, target, send, receive, device):
    return pltpu.make_async_remote_copy(
        src_ref=source,
        dst_ref=target,
        send_sem=send,
        recv_sem=receive,
        device_id=device,
        device_id_type=MESH,
    )


def bdot(a, b):
    return jnp.dot(a, b, preferred_element_type=jnp.float32)


def fused_kernel(
    n,
    shards,
    shared,
    tokens_far,
    pre_gain_far,
    w_inner,
    w_gate,
    w_states,
    w_step,
    step_bias_far,
    log_rate_far,
    taps_inner_far,
    taps_states,
    skip_gain_far,
    norm_gain_far,
    w_out,
    out,
    tokens,
    pre_gain,
    step_bias,
    log_rate,
    taps_inner,
    skip_gain,
    norm_gain,
    wide,
    step_w,
    wout,
    rows_all,
    proj,
    states,
    taps_all,
    raw_step,
    run_ref,
    x_mix,
    s_mix,
    acc,
    ends,
    state_out,
    state_in,
    squares,
    mixed,
    stage,
    from_right,
    from_left,
    own_sum,
    spare,
    pre,
    far,
    done,
    load_sem,
    o_sem,
    line,
    ahead,
    g_send,
    g_recv,
    t_send,
    t_recv,
    s_send,
    s_recv,
    c_send,
    c_recv,
    ti_send,
    ti_recv,
    ts_send,
    ts_recv,
    e_send,
    e_recv,
    q_send,
    q_recv,
    r_send,
    rl_recv,
    rr_recv,
    wz_send,
    wz_recv,
    wy_send,
    wy_recv,
    wx_send,
    wx_recv,
    wd_send,
    wd_recv,
    m_send,
    m_recv,
):
    z = lax.axis_index("tp")
    s = lax.axis_index("seq")
    part_id = lax.axis_index("dp")
    rows, width = tokens.shape
    total = n * rows
    inner = w_inner.shape[1]
    state_w = w_states.shape[1]
    heads = w_step.shape[0]
    half = rows // 2
    at_end = jnp.logical_or(z == 0, z == n - 1)
    beside = jnp.logical_or(z == 1, z == n - 2)
    across = lax.rem(s + shards // 2, shards)
    sibling = s + 1 - 2 * lax.rem(s, 2)

    early = [
        pltpu.make_async_copy(source, target, load_sem.at[5 + i])
        for i, (source, target) in enumerate(
            (
                (tokens_far, tokens),
                (pre_gain_far, pre_gain),
                (taps_states, taps_all.at[z]),
                (step_bias_far, step_bias),
                (log_rate_far, log_rate),
                (taps_inner_far, taps_inner),
                (skip_gain_far, skip_gain),
                (norm_gain_far, norm_gain),
            )
        )
    ]
    for load in early:
        load.start()
    barrier = pltpu.get_barrier_semaphore()
    neighbours = (
        (z > 0, {"tp": z - 1}),
        (z < n - 1, {"tp": z + 1}),
        (s > 0, {"seq": s - 1}),
        (s < shards - 1, {"seq": s + 1}),
        (z >= 0, {"seq": across}),
        (z >= 0, {"dp": 1 - part_id}),
    )
    met = jnp.int32(0)
    for there, device in neighbours:
        met = met + there.astype(jnp.int32)

        @pl.when(there)
        def _():
            pl.semaphore_signal(barrier, inc=1, device_id=device, device_id_type=MESH)

    loads = [
        pltpu.make_async_copy(w_states, wide.at[:, pl.ds(2 * inner, state_w)], load_sem.at[0]),
        pltpu.make_async_copy(w_step, step_w, load_sem.at[1]),
        pltpu.make_async_copy(w_inner, wide.at[:, pl.ds(0, inner)], load_sem.at[2]),
        pltpu.make_async_copy(w_gate, wide.at[:, pl.ds(inner, inner)], load_sem.at[3]),
        pltpu.make_async_copy(w_out, wout, load_sem.at[4]),
    ]
    for load in early[:2]:
        load.wait()
    for load in loads[:4]:
        load.start()

    def own_rows(i, _):
        piece = pl.ds(pl.multiple_of(i * 16, 16), 16)
        value = tokens[piece, :].astype(jnp.float32)
        scale = lax.rsqrt(jnp.mean(value * value, axis=1, keepdims=True) + epsilon)
        place = pl.ds(pl.multiple_of(z * rows + i * 16, 16), 16)
        rows_all[place, :] = (value * scale * pre_gain[...]).astype(jnp.bfloat16)
        return 0

    lax.fori_loop(half // 16, rows // 16, own_rows, 0)

    @pl.when(s == 0)
    def _():
        proj[0:PAD, 0:inner] = jnp.zeros((PAD, inner), jnp.bfloat16)
        states[0:PAD, :] = jnp.zeros((PAD, states.shape[1]), jnp.bfloat16)
        state_in[...] = jnp.zeros(state_in.shape, jnp.bfloat16)

    pl.semaphore_wait(barrier, met)

    def row_copy(source, part, side):
        block = rows_all.at[pl.ds(pl.multiple_of(source * rows + part * half, 16), half), :]
        step = 1 if side == 0 else -1
        return remote(
            block, block, g_send.at[side, source, part], g_recv.at[source, part], {"tp": z + step}
        )

    def send_on(source, part):
        @pl.when(jnp.logical_and(source <= z, z < n - 1))
        def _():
            row_copy(source, part, 0).start()

        @pl.when(jnp.logical_and(source >= z, z > 0))
        def _():
            row_copy(source, part, 1).start()

    slice_rows = inner // (2 * shards)
    chunk_rows = slice_rows // 2
    shared_w = spare.shape[1]

    def slice_of(d, q, c):
        first = (d * shards + q) * slice_rows + c * chunk_rows
        return pl.ds(pl.multiple_of(first, chunk_rows), chunk_rows)

    def down_copy(c):
        block = slice_of(part_id, s, c)
        return remote(
            w_out.at[block, pl.ds(0, shared_w)],
            spare.at[block, :],
            wz_send.at[c],
            wz_recv.at[c],
            {"tp": jnp.where(z == 0, 1, n - 2)},
        )

    def y_copy(c):
        block = spare.at[slice_of(part_id, s, c), :]
        return remote(block, block, wy_send.at[c], wy_recv.at[c], {"dp": 1 - part_id})

    def y_taken(c):
        block = spare.at[slice_of(1 - part_id, s, c), :]
        return remote(block, block, wy_send.at[c], wy_recv.at[c], {"dp": 1 - part_id})

    def x_copy(k, c, to):
        d = part_id if k == 0 else 1 - part_id
        block = spare.at[slice_of(d, s if to else across, c), :]
        return remote(block, block, wx_send.at[k, c], wx_recv.at[k, c], {"seq": across})

    def core_copy(j, to):
        d = part_id if j % 2 == 0 else 1 - part_id
        q = s if j < 2 else across
        q = q if to else q + 1 - 2 * lax.rem(q, 2)
        first = (d * shards + q) * slice_rows
        block = spare.at[pl.ds(pl.multiple_of(first, slice_rows), slice_rows), :]
        return remote(block, block, wd_send.at[j], wd_recv.at[j], {"seq": sibling})

    def send_down(c):
        @pl.when(at_end)
        def _():
            down_copy(c).start()

    send_on(z, 1)
    send_down(0)
    lax.fori_loop(0, half // 16, own_rows, 0)
    send_on(z, 0)
    send_down(1)

    def greet_line(side, condition):
        @pl.when(condition)
        def _():
            pl.semaphore_signal(
                line.at[side],
                inc=1,
                device_id={"tp": z + 1 if side == 0 else z - 1},
                device_id_type=MESH,
            )

    greet_line(0, z == 0)
    greet_line(1, z == n - 1)
    for side in range(2):
        edge = 0 if side == 0 else n - 1

        @pl.when(z != edge)
        def _():
            pl.semaphore_wait(line.at[side], 1)

        greet_line(side, jnp.logical_and(z != edge, z != n - 1 - edge))

    @pl.when(s > 0)
    def _():
        pl.semaphore_signal(ahead, inc=1, device_id={"seq": s - 1}, device_id_type=MESH)


    def tap_copy(source, other):
        return remote(
            taps_all.at[source], taps_all.at[source], t_send.at[other], t_recv.at[source], {"tp": other}
        )

    def in_copy(source, chunk, other):
        block = states.at[
            pl.ds(pl.multiple_of(PAD + chunk * rows, 16), rows),
            pl.ds(pl.multiple_of(source * state_w, LANES), STATE),
        ]
        return remote(
            block, block, s_send.at[chunk, other], s_recv.at[source, chunk], {"tp": other}
        )

    def is_edge(i):
        return jnp.logical_or(i == 0, i == n - 1)

    def out_copy(source, other):
        block = states.at[
            pl.ds(PAD, total), pl.ds(pl.multiple_of(source * state_w + STATE, LANES), STATE)
        ]
        return remote(block, block, c_send.at[other], c_recv.at[source], {"tp": other})

    def square_copy(source, other):
        return remote(
            squares.at[source], squares.at[source], q_send.at[other], q_recv.at[source], {"tp": other}
        )

    def each_other(action):
        def one(i, _):
            @pl.when(i != z)
            def _():
                action(i)

            return 0

        lax.fori_loop(0, n, one, 0)

    for load in early[2:]:
        load.wait()
    each_other(lambda i: tap_copy(z, i).start())

    def inner_tail():
        return remote(
            proj.at[pl.ds(total, PAD), pl.ds(0, inner)],
            proj.at[pl.ds(0, PAD), pl.ds(0, inner)],
            ti_send,
            ti_recv,
            {"seq": s + 1, "tp": z},
        )

    def state_tail(source, other):
        columns = pl.ds(pl.multiple_of(source * state_w, LANES), state_w)
        return remote(
            states.at[pl.ds(total, PAD), columns],
            states.at[pl.ds(0, PAD), columns],
            ts_send.at[other],
            ts_recv.at[source],
            {"seq": s + 1, "tp": other},
        )

    for load in loads[:4]:
        load.wait()
    loads[4].start()

    gate_tile = inner // 256

    def project(start, size):
        piece = pl.ds(pl.multiple_of(start, size), size)
        place = pl.ds(pl.multiple_of(PAD + start, 16), size)
        own = pl.ds(pl.multiple_of(z * state_w, LANES), state_w)
        tail = jnp.logical_and(start + size == total, s < shards - 1)
        states[place, own] = bdot(
            rows_all[piece, :], wide[:, 2 * inner : 2 * inner + state_w]
        ).astype(jnp.bfloat16)

        @pl.when(tail)
        def _():
            pl.semaphore_wait(ahead, 1)
            for other in range(n):
                state_tail(z, other).start()

        if size == rows:
            send_in(start // rows)
        else:

            @pl.when(lax.rem(start, rows) == 0)
            def _():
                send_in(start // rows)
                each_other(lambda i: out_copy(z, i).start())

        raw_step[piece, :] = lax.dot_general(
            rows_all[piece, :], step_w[...], NT, preferred_element_type=jnp.float32
        )

        def tile(i, _):
            columns = pl.ds(pl.multiple_of(i * 256, 256), 256)
            proj[place, columns] = bdot(rows_all[piece, :], wide[:, columns]).astype(jnp.bfloat16)
            return 0

        lax.fori_loop(0, gate_tile, tile, 0)

        @pl.when(tail)
        def _():
            inner_tail().start()

    def gate_rows(start, size):
        piece = pl.ds(pl.multiple_of(start, rows), size)
        place = pl.ds(pl.multiple_of(PAD + start, 16), size)

        def tile(i, _):
            columns = pl.ds(pl.multiple_of(inner + i * 256, 256), 256)
            proj[place, columns] = bdot(rows_all[piece, :], wide[:, columns]).astype(jnp.bfloat16)
            return 0

        lax.fori_loop(0, gate_tile, tile, 0)

    def send_in(chunk):
        each_other(lambda i: in_copy(z, chunk, i).start())

    def arrive(distance, _):
        for part in (1, 0):
            for side in range(2):
                source = z - distance if side == 0 else z + distance
                inside = jnp.logical_and(source >= 0, source < n)

                @pl.when(jnp.logical_and(inside, distance > 0))
                def _():
                    row_copy(source, part, side).wait_recv()
                    send_on(source, part)

        @pl.when(jnp.logical_and(beside, distance == 1))
        def _():
            down_copy(0).wait_recv()
            y_copy(0).start()
            x_copy(0, 0, True).start()

        @pl.when(jnp.logical_and(beside, distance == 2))
        def _():
            y_taken(0).wait_recv()
            x_copy(1, 0, True).start()
            down_copy(1).wait_recv()
            y_copy(1).start()
            x_copy(0, 1, True).start()

        def one(side, _):
            source = z - distance + 2 * distance * side
            inside = jnp.logical_and(source >= 0, source < n)

            @pl.when(jnp.logical_and(inside, jnp.logical_or(distance > 0, side == 0)))
            def _():
                project(source * rows, rows)

            return 0

        lax.fori_loop(0, 2, one, 0)
        return 0

    lax.fori_loop(0, n - 1, arrive, 0)

    @pl.when(beside)
    def _():
        y_taken(1).wait_recv()
        x_copy(1, 1, True).start()
        for j in range(2):
            core_copy(j, True).start()

    @pl.when(jnp.logical_not(at_end))
    def _():
        each_other(lambda i: out_copy(z, i).start())
        gate_rows(0, total)

    @pl.when(at_end)
    def _():
        gate_rows(jnp.where(z == 0, 0, rows), total - rows)

        def last_half(i, _):
            part = 1 - i
            for side in range(2):

                @pl.when(z == (n - 1 if side == 0 else 0))
                def _():
                    row_copy(n - 1 - z, part, side).wait_recv()

            project((n - 1 - z) * rows + part * half, half)
            return 0

        lax.fori_loop(0, 2, last_half, 0)

    step = raw_step[...] + step_bias[...]
    step = jnp.maximum(step, 0.0) + jnp.log1p(jnp.exp(-jnp.abs(step)))
    decay = -jnp.exp(log_rate[...]) * step
    place_t = lax.broadcasted_iota(jnp.int32, (total, total), 0)
    place_s = lax.broadcasted_iota(jnp.int32, (total, total), 1)
    tri = (place_t >= place_s).astype(jnp.bfloat16)
    decay_high = decay.astype(jnp.bfloat16)
    rest = decay - decay_high.astype(jnp.float32)
    decay_mid = rest.astype(jnp.bfloat16)
    decay_low = (rest - decay_mid.astype(jnp.float32)).astype(jnp.bfloat16)
    run = bdot(tri, decay_high) + (bdot(tri, decay_mid) + bdot(tri, decay_low))
    run_ref[...] = jnp.zeros(run_ref.shape, jnp.float32)
    run_ref[:, 0:heads] = run
    run_t = run_ref[...].T
    last = run[total - 1 : total, :]
    reach = jnp.exp(last - run) * step
    grown = jnp.exp(run)
    whole = jnp.exp(last)
    lane = lax.broadcasted_iota(jnp.int32, (1, LANES), 1)
    low = lane < HEAD_DIM

    def conv(buffer, columns, taps):
        value = buffer[:, columns].astype(jnp.float32)
        kernel_len = taps.shape[0]
        out_value = jnp.zeros((total, value.shape[1]), jnp.float32)
        for k in range(kernel_len):
            first = PAD - (kernel_len - 1) + k
            out_value = out_value + taps[k : k + 1, :] * value[first : first + total, :]
        return jax.nn.silu(out_value).astype(jnp.bfloat16)

    @pl.when(s > 0)
    def _():
        inner_tail().wait_recv()

    def conv_tile(i, _):
        columns = pl.ds(pl.multiple_of(i * 256, 256), 256)
        x_mix[:, columns] = conv(proj, columns, taps_inner[:, columns])
        return 0

    lax.fori_loop(0, inner // 256, conv_tile, 0)

    def take_states(part, i):
        columns = pl.ds(pl.multiple_of(i * state_w + part * STATE, LANES), STATE)
        taps = taps_all[i][:, part * STATE : (part + 1) * STATE]
        s_mix[:, columns] = conv(states, columns, taps)

    def take_in(i, _):
        @pl.when(i != z)
        def _():
            tap_copy(i, z).wait_recv()
            for chunk in range(n):
                in_copy(i, chunk, z).wait_recv()

        @pl.when(s > 0)
        def _():
            state_tail(i, z).wait_recv()

        take_states(0, i)
        return 0

    def take_out(i, _):
        @pl.when(i != z)
        def _():
            out_copy(i, z).wait_recv()

        take_states(1, i)
        return 0

    lax.fori_loop(0, n, take_in, 0)

    def group_in(g):
        return s_mix[:, g * 2 * STATE : g * 2 * STATE + STATE]

    def group_out(g):
        return s_mix[:, g * 2 * STATE + STATE : (g + 1) * 2 * STATE]

    def pair_of(value, h):
        return jnp.where(low, value[:, h : h + 1], value[:, h + 1 : h + 2])

    pairs = heads // 2
    per_quad = GROUPS // 2
    quads = pairs // per_quad
    quad_w = GROUPS * HEAD_DIM

    def end_copy(c):
        columns = pl.ds(c * quad_w, quad_w)
        return remote(
            state_out.at[:, columns],
            state_in.at[:, columns],
            e_send.at[c],
            e_recv.at[c],
            {"seq": s + 1, "tp": z},
        )

    turned = [
        jnp.concatenate((group_in(g).T, group_in(g + 1).T), axis=0) for g in range(0, GROUPS, 2)
    ]
    for q in range(pairs):
        columns = slice(q * LANES, (q + 1) * LANES)
        h = 2 * q
        scaled = (x_mix[:, columns].astype(jnp.float32) * pair_of(reach, h)).astype(jnp.bfloat16)
        both = bdot(turned[h % GROUPS // 2], scaled)
        ends[:, columns] = jnp.where(low, both[:STATE], both[STATE:])
        if q % per_quad == per_quad - 1:
            c = q // per_quad

            @pl.when(jnp.logical_and(s == 0, shards > 1))
            def _():
                columns = slice(c * quad_w, (c + 1) * quad_w)
                state_out[:, columns] = ends[:, columns].astype(jnp.bfloat16)
                end_copy(c).start()

    def hand_on(c, here):
        @pl.when(here)
        def _():
            end_copy(c).wait_recv()

            @pl.when(s < shards - 1)
            def _():
                for q in range(c * per_quad, (c + 1) * per_quad):
                    columns = slice(q * LANES, (q + 1) * LANES)
                    state_out[:, columns] = (
                        ends[:, columns]
                        + pair_of(whole, 2 * q) * state_in[:, columns].astype(jnp.float32)
                    ).astype(jnp.bfloat16)
                end_copy(c).start()

    for c in range(quads):
        hand_on(c, s == 1)

    @pl.when(at_end)
    def _():
        gate_rows((n - 1 - z) * rows, rows)


    for c in range(quads):
        hand_on(c, s == 2)
    lax.fori_loop(0, n, take_out, 0)

    scores = [
        lax.dot_general(group_out(g), group_in(g), NT, preferred_element_type=jnp.float32)
        for g in range(GROUPS)
    ]
    for q in range(pairs):
        columns = slice(q * LANES, (q + 1) * LANES)
        h = 2 * q
        value = x_mix[:, columns].astype(jnp.float32)
        stepped = (value * pair_of(step, h)).astype(jnp.bfloat16)
        direct = value * pair_of(skip_gain[...], h)
        for low_t in range(0, total, BLOCK):
            high_t = low_t + BLOCK
            causal = place_t[low_t:high_t, :high_t] >= place_s[low_t:high_t, :high_t]
            both = []
            for k in (h, h + 1):
                spread = run[low_t:high_t, k : k + 1] - run_t[k : k + 1, :high_t]
                table = jnp.where(causal, jnp.exp(jnp.where(causal, spread, 0.0)), 0.0)
                weights = (scores[k % GROUPS][low_t:high_t, :high_t] * table).astype(jnp.bfloat16)
                both.append(bdot(weights, stepped[:high_t, :]))
            acc[low_t:high_t, columns] = jnp.where(low, both[0], both[1]) + direct[low_t:high_t, :]
    @pl.when(beside)
    def _():
        for k in range(2):
            for c in range(2):
                x_copy(k, c, False).wait_recv()
            core_copy(2 + k, True).start()

    sums = [jnp.zeros((total, LANES), jnp.float32) for _ in range(per_quad)]
    for q in range(pairs):
        columns = slice(q * LANES, (q + 1) * LANES)
        h = 2 * q
        if q % per_quad == 0:
            hand_on(q // per_quad, s > 2)
        came = state_in[:, columns]
        carried = jnp.where(
            low, bdot(group_out(h % GROUPS), came), bdot(group_out((h + 1) % GROUPS), came)
        )
        gate = proj[PAD:, inner + q * LANES : inner + (q + 1) * LANES].astype(jnp.float32)
        gated = (acc[:, columns] + carried * pair_of(grown, h)) * jax.nn.silu(gate)
        acc[:, columns] = gated
        sums[q % per_quad] = sums[q % per_quad] + gated * gated
    pick = lax.broadcasted_iota(jnp.int32, (8, LANES), 0)
    where_lane = lax.broadcasted_iota(jnp.int32, (8, LANES), 1)
    local = jnp.zeros((8, total), jnp.float32)
    for k in range(per_quad):
        chosen = (where_lane // HEAD_DIM + 2 * k == pick).astype(jnp.float32)
        local = local + lax.dot_general(
            chosen, sums[k], NT, precision=highest, preferred_element_type=jnp.float32
        )
    squares[z] = local
    each_other(lambda i: square_copy(z, i).start())

    def mix_copy(target):
        place = pl.ds(pl.multiple_of(target * rows, rows), rows)
        return remote(
            pre.at[place, :],
            far.at[place, :],
            m_send.at[target],
            m_recv.at[target],
            {"tp": jnp.where(z == 0, 1, n - 2)},
        )

    @pl.when(at_end)
    def _():
        for q in range(pairs):
            columns = slice(q * LANES, (q + 1) * LANES)
            pre[:, columns] = (acc[:, columns] * norm_gain[:, columns]).astype(jnp.bfloat16)
        for i in range(n - 1):
            mix_copy(jnp.where(z == 0, n - 1 - i, i)).start()

    loads[4].wait()
    each_other(lambda i: square_copy(i, z).wait_recv())
    sum_all = squares[0]
    for i in range(1, n):
        sum_all = sum_all + squares[i]
    inverse = lax.rsqrt(sum_all / (n * heads // GROUPS * HEAD_DIM) + epsilon)
    inverse = jnp.concatenate([inverse] * (LANES // 8), axis=0).T
    run_ref[...] = inverse
    def mix(target):
        place = pl.ds(pl.multiple_of(target * rows, rows), rows)
        scale = run_ref[place, :]
        for q in range(pairs):
            columns = slice(q * LANES, (q + 1) * LANES)
            mixed[place, columns] = (
                acc[place, columns] * pair_of(scale, (2 * q) % GROUPS) * norm_gain[:, columns]
            ).astype(jnp.bfloat16)

    pieces = r_send.shape[1]
    piece_w = width // pieces

    def partial_of(target, p):
        return bdot(mixed[pl.ds(pl.multiple_of(target * rows, rows), rows), :], wout[:, p])

    def columns_of(p):
        return pl.ds(pl.multiple_of(p * piece_w, LANES), piece_w)

    def sum_copy(target, p, side):
        landing, receive, way = (from_right, rl_recv, -1) if side == 0 else (from_left, rr_recv, 1)
        return remote(
            stage.at[target, p],
            landing.at[target, p],
            r_send.at[target, p],
            receive.at[target, p],
            {"tp": z + way},
        )

    def far_partial(target, p):
        place = pl.ds(pl.multiple_of(target * rows, rows), rows)
        return bdot(far[place, :], spare[:, p])

    def take_far(target):
        place = pl.ds(pl.multiple_of(target * rows, rows), rows)
        mix_copy(target).wait_recv()
        scale = run_ref[place, :]
        for q in range(pairs):
            columns = slice(q * LANES, (q + 1) * LANES)
            far[place, columns] = (
                far[place, columns].astype(jnp.float32) * pair_of(scale, (2 * q) % GROUPS)
            ).astype(jnp.bfloat16)

    @pl.when(beside)
    def _():
        for j in range(4):
            core_copy(j, False).wait_recv()

    items = (n - 1) * pieces
    lag = 3

    def one_sum(t, _):
        for side in range(2):
            i = t - lag * (n - 1 - z) if side == 0 else t - lag * z
            k, p = jnp.maximum(i, 0) // pieces, lax.rem(jnp.maximum(i, 0), pieces)
            target = k if side == 0 else n - 1 - k
            landing = from_right if side == 0 else from_left
            active = target < z if side == 0 else target > z
            more = z < n - 1 if side == 0 else z > 0
            active = jnp.logical_and(active, jnp.logical_and(i >= 0, i < items))

            has_far = z == n - 2 if side == 0 else z == 1
            is_end = z == n - 1 if side == 0 else z == 0
            use_far = jnp.logical_and(has_far, p < shared)
            active = jnp.logical_and(active, jnp.logical_or(p >= shared, jnp.logical_not(is_end)))

            @pl.when(jnp.logical_and(active, p == jnp.where(is_end, shared, 0)))
            def _():
                mix(target)

                @pl.when(has_far)
                def _():
                    take_far(target)

            @pl.when(active)
            def _():
                value = partial_of(target, columns_of(p))

                @pl.when(use_far)
                def _():
                    stage[target, p] = (
                        value + far_partial(target, columns_of(p))
                    ).astype(jnp.bfloat16)

                @pl.when(jnp.logical_and(more, jnp.logical_not(use_far)))
                def _():
                    sum_copy(target, p, side).wait_recv()
                    stage[target, p] = (
                        value + landing[target, p].astype(jnp.float32)
                    ).astype(jnp.bfloat16)

                @pl.when(jnp.logical_not(more))
                def _():
                    stage[target, p] = value.astype(jnp.bfloat16)

                sum_copy(target, p, side).start()

        @pl.when(t == items)
        def _():
            mix(z)

            @pl.when(beside)
            def _():
                take_far(z)

        @pl.when(jnp.logical_and(t >= items, t < items + pieces))
        def _():
            columns = columns_of(t - items)
            own = tokens[:, columns].astype(jnp.float32) + partial_of(z, columns)
            own_sum[:, columns] = own

            @pl.when(jnp.logical_and(beside, t - items < shared))
            def _():
                own_sum[:, columns] = own + far_partial(z, columns)

        return 0

    lax.fori_loop(0, items + max(lag * (n - 1), pieces), one_sum, 0)

    def finish(p, _):
        columns = columns_of(p)
        lands = (
            jnp.logical_and(z < n - 1, jnp.logical_or(z != n - 2, p >= shared)),
            jnp.logical_and(z > 0, jnp.logical_or(z != 1, p >= shared)),
        )
        for side in range(2):

            @pl.when(lands[side])
            def _():
                sum_copy(z, p, side).wait_recv()

        none = jnp.zeros((rows, piece_w), jnp.float32)
        right = jnp.where(lands[0], from_right[z, p].astype(jnp.float32), none)
        left = jnp.where(lands[1], from_left[z, p].astype(jnp.float32), none)
        done[:, columns] = (own_sum[:, columns] + right + left).astype(jnp.bfloat16)
        out_store(p).start()
        return 0

    def out_store(p):
        columns = columns_of(p)
        return pltpu.make_async_copy(done.at[:, columns], out.at[:, columns], o_sem.at[p])

    lax.fori_loop(0, pieces, finish, 0)

    def sent_rows(source, _):
        for part in range(2):

            @pl.when(jnp.logical_and(source <= z, z < n - 1))
            def _():
                row_copy(source, part, 0).wait_send()

            @pl.when(jnp.logical_and(source >= z, z > 0))
            def _():
                row_copy(source, part, 1).wait_send()

        return 0

    lax.fori_loop(0, n, sent_rows, 0)

    def sent_small(i):
        tap_copy(z, i).wait_send()
        square_copy(z, i).wait_send()
        out_copy(z, i).wait_send()
        for chunk in range(n):
            in_copy(z, chunk, i).wait_send()

        def sent_sum(p, _):
            sum_copy(i, p, 0).wait_send()
            return 0

        lax.fori_loop(jnp.where(at_end, shared, 0), pieces, sent_sum, 0)

    each_other(sent_small)

    def stored(p, _):
        out_store(p).wait()
        return 0

    lax.fori_loop(0, pieces, stored, 0)

    @pl.when(s < shards - 1)
    def _():
        inner_tail().wait_send()
        for other in range(n):
            state_tail(z, other).wait_send()
        for c in range(quads):
            end_copy(c).wait_send()

    @pl.when(at_end)
    def _():
        for c in range(2):
            down_copy(c).wait_send()
        for i in range(n - 1):
            mix_copy(jnp.where(z == 0, n - 1 - i, i)).wait_send()

    @pl.when(beside)
    def _():
        for c in range(2):
            y_copy(c).wait_send()
            for k in range(2):
                x_copy(k, c, True).wait_send()
        for j in range(4):
            core_copy(j, True).wait_send()


def body(
    n,
    shards,
    tokens,
    pre_gain,
    proj_inner,
    proj_gate,
    proj_states,
    proj_step,
    step_bias,
    log_rate,
    conv_inner,
    conv_states,
    skip_gain,
    norm_gain,
    proj_output,
):
    rows, width = tokens.shape
    inner, state_w, heads = proj_inner.shape[1], proj_states.shape[1], proj_step.shape[1]
    total = n * rows
    all_states = n * state_w
    quads = heads // GROUPS
    pieces, shared = 8, 4
    bf16, f32 = jnp.bfloat16, jnp.float32
    far = pl.BlockSpec(memory_space=pl.ANY)
    dma = pltpu.SemaphoreType.DMA
    return pl.pallas_call(
        partial(fused_kernel, n, shards, shared),
        out_shape=jax.ShapeDtypeStruct((rows, width), bf16),
        in_specs=[far] * 13,
        out_specs=far,
        scratch_shapes=[
            pltpu.VMEM((rows, width), bf16),
            pltpu.VMEM((1, width), f32),
            pltpu.VMEM((1, heads), f32),
            pltpu.VMEM((1, heads), f32),
            pltpu.VMEM(conv_inner.shape, f32),
            pltpu.VMEM((1, heads), f32),
            pltpu.VMEM((1, inner), f32),
            pltpu.VMEM((width, 2 * inner + state_w), bf16),
            pltpu.VMEM((heads, width), bf16),
            pltpu.VMEM((inner, width), bf16),
            pltpu.VMEM((total, width), bf16),
            pltpu.VMEM((PAD + total, 2 * inner), bf16),
            pltpu.VMEM((PAD + total, all_states), bf16),
            pltpu.VMEM((n,) + conv_states.shape, f32),
            pltpu.VMEM((total, heads), f32),
            pltpu.VMEM((total, LANES), f32),
            pltpu.VMEM((total, inner), bf16),
            pltpu.VMEM((total, all_states), bf16),
            pltpu.VMEM((total, inner), f32),
            pltpu.VMEM((STATE, inner), f32),
            pltpu.VMEM((STATE, inner), bf16),
            pltpu.VMEM((STATE, inner), bf16),
            pltpu.VMEM((n, 8, total), f32),
            pltpu.VMEM((total, inner), bf16),
            pltpu.VMEM((n, pieces, rows, width // pieces), bf16),
            pltpu.VMEM((n, pieces, rows, width // pieces), bf16),
            pltpu.VMEM((n, pieces, rows, width // pieces), bf16),
            pltpu.VMEM((rows, width), f32),
            pltpu.VMEM((inner, width // pieces * shared), bf16),
            pltpu.VMEM((total, inner), bf16),
            pltpu.VMEM((total, inner), bf16),
            pltpu.VMEM((rows, width), bf16),
            dma((13,)),
            dma((pieces,)),
            pltpu.SemaphoreType.REGULAR((2,)),
            pltpu.SemaphoreType.REGULAR,
            dma((2, n, 2)),
            dma((n, 2)),
            dma((n,)),
            dma((n,)),
            dma((n, n)),
            dma((n, n)),
            dma((n,)),
            dma((n,)),
            dma,
            dma,
            dma((n,)),
            dma((n,)),
            dma((quads,)),
            dma((quads,)),
            dma((n,)),
            dma((n,)),
            dma((n, pieces)),
            dma((n, pieces)),
            dma((n, pieces)),
            dma((2,)),
            dma((2,)),
            dma((2,)),
            dma((2,)),
            dma((2, 2)),
            dma((2, 2)),
            dma((4,)),
            dma((4,)),
            dma((n,)),
            dma((n,)),
        ],
        compiler_params=pltpu.CompilerParams(
            collective_id=0, has_side_effects=True, vmem_limit_bytes=62 * 1024 * 1024
        ),
    )(
        tokens,
        pre_gain[None],
        proj_inner,
        proj_gate,
        proj_states,
        proj_step.T,
        step_bias[None],
        log_rate[None],
        conv_inner,
        conv_states,
        skip_gain[None],
        norm_gain[None],
        proj_output,
    )


def solution(mesh):
    n, shards = mesh.shape["tp"], mesh.shape["seq"]
    plain = plain_solution(mesh)

    def run(*arrays):
        tokens, proj_inner, proj_states, proj_step = arrays[0], arrays[2], arrays[4], arrays[5]
        rows = tokens.shape[0] // (mesh.shape["dp"] * shards * n)
        heads, state_w = proj_step.shape[1] // n, proj_states.shape[1] // n
        fits = (
            n == 4
            and shards == 4
            and mesh.shape["dp"] == 2
            and rows % 32 == 0
            and (rows * n) % BLOCK == 0
            and state_w == 2 * STATE
            and heads % GROUPS == 0
            and (proj_inner.shape[1] // n) % 256 == 0
        )
        if not fits:
            return plain(*arrays)
        line = P(("dp", "seq", "tp"), None)
        columns = P(None, "tp")
        placed = (
            (line, P()) + (columns,) * 4 + (P("tp"), P("tp"), columns, columns)
            + (P("tp"), P("tp"), P("tp", None))
        )
        return jax.shard_map(
            partial(body, n, shards), mesh=mesh, in_specs=placed, out_specs=line, check_vma=False
        )(*arrays)

    return run
```
